32 devices in a mesh: grp: 2 (over y), mem: 16 (over z, x, core).
Axes of the slice: x: 2, y: 2, z: 4, core: 2. Of those that a mesh axis runs over, the one named last changes fastest.
Arguments:
- tokens: bfloat16 [4096, 1024], P(('grp', 'mem')), may hold values from -6 to 6
- cotangent: bfloat16 [4096, 1024], P(('grp', 'mem')), may hold values from -6 to 6
- path: int32 [32, 3], P(('grp', 'mem')), may hold values from 0 to 63, as said below
- coarse_weights: bfloat16 [4, 1024, 512], P(None, 'mem'), may hold values from -0.1875 to 0.1875
- middle_weights: bfloat16 [64, 1024, 256], P(None, 'mem'), may hold values from -0.1875 to 0.1875
- fine_weights: bfloat16 [64, 1024, 128], P('grp', 'mem'), may hold values from -0.1875 to 0.1875
Outputs:
- tokens_grad: bfloat16 [4096, 1024], P(('grp', 'mem'))
- coarse_grad: bfloat16 [4, 1024, 512], P(None, 'mem')
- middle_grad: bfloat16 [64, 1024, 256], P(None, 'mem')
- fine_grad: bfloat16 [64, 1024, 128], P('grp', 'mem')
The draws below stay inside these ranges and needn't reach their ends.
Inputs may be any that keep to these rules, and one draw needn't show every extreme that they name: Row d is the path of document d: column 0 its coarse block, column 1 its middle block, column 2 its fine block, with middle = fine * 1 and coarse = middle * 4 // 64. Some fine blocks are chosen by many documents.
All inputs are finite; a program needn't handle non-finite values.
Results may differ from the reference program's by a relative error of at most 0.005.
Values may be sent and summed in bfloat16 or wider, within the bound.
A program may use at most 64 MiB of HBM per device.

```python
from functools import partial
import jax
import jax.numpy as jnp
from jax import lax

D = 1024
HC = 256
HM = 128
HF = 64
COARSE = 4
MIDDLE = 64
TOK_DEV = 128
FINE = 64
DOCS = 32
TOKENS = 4096


def draw_path(key, part):
    first, second, third, fourth = jax.random.split(key, 4)
    fine_ids = jax.random.randint(first, (DOCS,), 0, FINE)
    popular = jax.random.randint(second, (8,), 0, FINE)
    chooser = jax.random.randint(third, (DOCS,), 0, 32)
    fine_ids = jnp.where(chooser < 8, popular[chooser % 8], fine_ids)
    places = jax.random.permutation(fourth, DOCS)
    fine_ids = fine_ids.at[places[0]].set(0).at[places[1]].set(FINE - 1)
    middle_ids = fine_ids * MIDDLE // FINE
    coarse_ids = middle_ids * COARSE // MIDDLE
    return jnp.stack([coarse_ids, middle_ids, fine_ids], axis=1).astype(jnp.int32)


def steps_of(stream_key, dims, shards, smallest, top_value):
    def one(dim, shards_of):
        draws = jax.random.uniform(jax.random.fold_in(jax.random.fold_in(stream_key, 6), dim), (shards_of,), jnp.float32, smallest / len(shards), top_value / len(shards))
        return jnp.repeat(jnp.exp(draws), dims[dim] // shards_of).reshape((-1,) + (1,) * (len(dims) - dim - 1))

    loudness = one(*shards[0])
    for cut in shards[1:]:
        loudness = loudness * one(*cut)
    return loudness


def bell_draw(stream_key, dims, width, most, cuts=(), kind=jnp.bfloat16):
    entries = width * jax.random.normal(stream_key, dims, jnp.float32)
    if cuts:
        entries = entries * steps_of(stream_key, dims, cuts, -0.22, 0.18)
    return jnp.clip(entries, -most, most).astype(kind)


def setup_inputs(seed: int = 0) -> dict:
    streams_of = jax.random.split(jax.random.key(seed), 7)
    tokens = bell_draw(streams_of[0], (TOKENS, D), 1.0, 6.0, ((0, 32),))
    cotangent = bell_draw(streams_of[1], (TOKENS, D), 1.0, 6.0, ((0, 32),))
    path = draw_path(jax.random.fold_in(streams_of[6], 71), 0)
    coarse_weights = bell_draw(streams_of[3], (COARSE, D, 2 * HC), D ** -0.5, 0.1875, ((1, 16),))
    middle_weights = bell_draw(streams_of[4], (MIDDLE, D, 2 * HM), D ** -0.5, 0.1875, ((1, 16),))
    fine_weights = bell_draw(streams_of[5], (FINE, D, 2 * HF), D ** -0.5, 0.1875, ((0, 2), (1, 16)))
    return dict(tokens=tokens, cotangent=cotangent, path=path, coarse_weights=coarse_weights, middle_weights=middle_weights, fine_weights=fine_weights)


def contract_rows(left, right):
    return lax.dot_general(left, right, (((0,), (0,)), ((), ())), preferred_element_type=jnp.float32)

def level_terms(inputs, upstream, weights):
    hidden_width = weights.shape[1] // 2
    up_half = weights[:, :hidden_width]
    down_half = weights[:, hidden_width:]
    before = jnp.dot(inputs, up_half, preferred_element_type=jnp.float32)
    hidden, pullback = jax.vjp(partial(jax.nn.gelu, approximate=True), before)
    hidden_low = hidden.astype(jnp.bfloat16)
    hidden_grad = jnp.dot(upstream, down_half, preferred_element_type=jnp.float32)
    before_grad = pullback(hidden_grad)[0].astype(jnp.bfloat16)
    up_grad = contract_rows(inputs, before_grad)
    down_grad = contract_rows(upstream, hidden_low)
    input_part = lax.dot_general(before_grad, up_half, (((1,), (1,)), ((), ())), preferred_element_type=jnp.float32)
    return (jnp.concatenate([up_grad, down_grad], axis=1), input_part)

def reference(tokens, cotangent, path, coarse_weights, middle_weights, fine_weights):
    documents = path.shape[0]
    token_blocks = tokens.reshape(documents, TOK_DEV, D)
    upstream_blocks = cotangent.reshape(documents, TOK_DEV, D)
    start = (jnp.zeros(coarse_weights.shape, jnp.float32), jnp.zeros(middle_weights.shape, jnp.float32), jnp.zeros(fine_weights.shape, jnp.float32))

    def advance(carry, item):
        inputs, upstream, route = item
        coarse_sum, middle_sum, fine_sum = carry
        coarse_term, coarse_back = level_terms(inputs, upstream, coarse_weights[route[0]])
        middle_term, middle_back = level_terms(inputs, upstream, middle_weights[route[1]])
        fine_term, fine_back = level_terms(inputs, upstream, fine_weights[route[2]])
        coarse_sum = coarse_sum.at[route[0]].add(coarse_term)
        middle_sum = middle_sum.at[route[1]].add(middle_term)
        fine_sum = fine_sum.at[route[2]].add(fine_term)
        summed = (coarse_back + middle_back + fine_back).astype(jnp.bfloat16)
        return ((coarse_sum, middle_sum, fine_sum), summed)
    totals, input_grads = lax.scan(advance, start, (token_blocks, upstream_blocks, path))
    return (input_grads.reshape(documents * TOK_DEV, D), totals[0].astype(jnp.bfloat16), totals[1].astype(jnp.bfloat16), totals[2].astype(jnp.bfloat16))
```

```python
import functools
import math

import jax
import jax.numpy as jnp
from jax import lax
from jax.experimental import pallas as pl
from jax.experimental.pallas import tpu as pltpu
from jax.sharding import PartitionSpec as P

MESH = pl.DeviceIdType.MESH
LANES = 128
F32 = jnp.float32
BF16 = jnp.bfloat16


def gelu_parts(before, hidden_grad):
    scale = math.sqrt(2.0 / math.pi)
    square = before * before
    tanh = jnp.tanh(scale * (before + 0.044715 * (square * before)))
    half = 0.5 * (1.0 + tanh)
    hidden = before * half
    slope = half + 0.5 * before * (1.0 - tanh * tanh) * (scale * (1.0 + 3 * 0.044715 * square))
    return hidden.astype(BF16), (hidden_grad * slope).astype(BF16)


def dot(left, right):
    return jnp.dot(left, right, preferred_element_type=F32)


def dot_transposed(left, right):
    return lax.dot_general(left, right, (((1,), (1,)), ((), ())), preferred_element_type=F32)


def level(weights, x, g, xt, gt):
    width = weights.shape[1]
    half = width // 2
    if half % LANES == 0:
        up = weights[:, :half]
        down = weights[:, half:]
        hidden, grad = gelu_parts(dot(x, up), dot(g, down))
        term = jnp.concatenate(
            [dot(xt, grad).astype(BF16), dot(gt, hidden).astype(BF16)], axis=1
        )
        return term, dot_transposed(grad, up)
    before = dot(x, weights)
    hidden_grad = pltpu.roll(dot(g, weights), half, 1)
    hidden, grad = gelu_parts(before, hidden_grad)
    first = lax.broadcasted_iota(jnp.int32, grad.shape, 1) < half
    grad = jnp.where(first, grad.astype(F32), 0.0).astype(BF16)
    hidden = jnp.where(first, hidden.astype(F32), 0.0)
    hidden = pltpu.roll(hidden, half, 1).astype(BF16)
    term = (dot(xt, grad) + dot(gt, hidden)).astype(BF16)
    return term, dot_transposed(grad, weights)


def plan(groups, members, blocks_width):
    inner = max(k for k in range(1, math.isqrt(members) + 1) if members % k == 0)
    cores = 2 if inner % 2 == 0 else 1
    return members // inner, inner // cores, cores


def bits_of(outer):
    bits = []
    while outer > 1:
        outer //= 2
        bits.append(outer)
    return bits


def main_kernel(
    groups,
    members,
    path_row,
    tokens_hbm,
    cotangent_hbm,
    coarse_hbm,
    middle_hbm,
    fine_hbm,
    all_paths,
    tokens_grad,
    middle_parts,
    fine_parts,
    coarse_parts,
    path,
    both,
    other_doc,
    coarse_w,
    middle_w,
    fine_w,
    middle_send,
    fine_out,
    fine_in,
    fine_send,
    middle_block,
    fine_block,
    middle_term,
    fine_term,
    sums,
    from_core,
    from_side,
    from_line,
    coarse_total,
    flipped,
    pair_t,
    total,
    pre_give,
    pre_take,
    act_give,
    act_take,
    back_give,
    back_take,
    path_send,
    path_recv,
    mem_send,
    mem_recv,
    grp_send,
    grp_recv,
    pair_send,
    pair_recv,
    gather_send,
    gather_recv,
    side_send,
    side_recv,
    core_send,
    core_recv,
    fold_send,
    fold_recv,
    local_sem,
    load_sem,
    middle_send_on,
    middle_recv_on,
    fine_send_on,
    fine_recv_on,
):
    group = lax.axis_index("grp")
    me = lax.axis_index("mem")
    count = groups * members
    device = group * members + me
    owned = fine_w.shape[0]
    blocks, outer, sides, cores, rows, columns = coarse_w.shape
    inner = sides * cores
    bits = bits_of(outer)
    line = me // inner
    place = lax.rem(me, inner)
    side = place // cores
    core = lax.rem(place, cores)
    slot = lax.rem(group, 2)
    mirror = group + 1 - 2 * slot
    token_count, width = tokens_grad.shape

    def loop(start, stop, body):
        def wrapped(step, carry):
            body(step)
            return carry

        lax.fori_loop(start, stop, wrapped, 0)

    def flip(r):
        there = line
        for bit in bits:
            if r & bit:
                there = there + bit * (1 - 2 * lax.rem(there // bit, 2))
        return there

    def at_line(r, s, c):
        return flip(r) * inner + s * cores + c

    def to_member(source, target, send, recv, p):
        return pltpu.make_async_remote_copy(
            src_ref=source,
            dst_ref=target,
            send_sem=send,
            recv_sem=recv,
            device_id={"mem": p},
            device_id_type=MESH,
        )

    half = pl.ds(pl.multiple_of(slot * columns, LANES), columns)
    loads = [
        pltpu.make_async_copy(source, target, load_sem.at[index])
        for index, (source, target) in enumerate(
            (
                (tokens_hbm, both.at[0]),
                (cotangent_hbm, both.at[1]),
                (coarse_hbm.at[:, :, half], coarse_w.at[:, line, side, core]),
                (fine_hbm, fine_w),
                (middle_hbm, middle_w),
            )
        )
    ]
    for load in loads:
        load.start()
    barrier = pltpu.get_barrier_semaphore()

    def anyone(step):
        other = lax.rem(device + step, count)
        return other, (other // members, lax.rem(other, members))

    def greet(step):
        _, where = anyone(step)
        pl.semaphore_signal(barrier, inc=1, device_id=where, device_id_type=MESH)

    loop(1, count, greet)
    for load in loads[:3]:
        load.wait()
    pl.semaphore_wait(barrier, count - 1)

    def path_copy(step):
        _, where = anyone(step)
        return pltpu.make_async_remote_copy(
            src_ref=path_row,
            dst_ref=all_paths.at[device],
            send_sem=path_send,
            recv_sem=path_recv,
            device_id=where,
            device_id_type=MESH,
        )

    loop(1, count, lambda step: path_copy(step).start())
    all_paths[device] = path_row[...]

    def pair_copy(index, source, target):
        return pltpu.make_async_remote_copy(
            src_ref=source,
            dst_ref=target,
            send_sem=pair_send.at[index],
            recv_sem=pair_recv.at[index],
            device_id={"grp": mirror},
            device_id_type=MESH,
        )

    def gather_copy(r, bit):
        piece = coarse_w.at[:, flip(r), side, core]
        return to_member(
            piece,
            piece,
            gather_send.at[r, bits.index(bit)],
            gather_recv.at[r ^ bit],
            at_line(bit, side, core),
        )

    def gather_wait(r):
        piece = coarse_w.at[:, flip(r), side, core]
        bit = r & -r
        to_member(
            piece, piece, gather_send.at[0, 0], gather_recv.at[r], at_line(bit, side, core)
        ).wait_recv()

    def gather_on(r):
        return [bit for bit in bits if r == 0 or bit < (r & -r)]

    def side_copy(r, step, landing_own):
        there = lax.rem(side + step, sides)
        landing = side if landing_own else lax.rem(side + sides - step, sides)
        piece = coarse_w.at[:, flip(r), landing, core]
        return to_member(
            piece, piece, side_send.at[0, r, step], side_recv.at[0, r, step], at_line(0, there, core)
        )

    def core_copy(r, landing_own):
        piece = coarse_w.at[:, flip(r), :, core if landing_own else 1 - core]
        return to_member(
            piece, piece, core_send.at[0, r], core_recv.at[0, r], at_line(0, side, 1 - core)
        )

    tokens_pair = pair_copy(0, both.at[1 - slot], other_doc)

    def pass_on(r):
        for bit in gather_on(r):
            gather_copy(r, bit).start()
        for step in range(1, sides):
            side_copy(r, step, True).start()

    def share(r):
        for step in range(1, sides):
            side_copy(r, step, False).wait_recv()
        if cores > 1:
            core_copy(r, True).start()

    pass_on(0)
    tokens_pair.start()
    for which in range(2):
        for start in range(0, width, LANES):
            part = slice(start, start + LANES)
            flipped[which, part, :] = both[which, :, part].T
    for load in loads[3:]:
        load.wait()
    pair_t[:, :token_count] = flipped[slot]

    others = all_paths.at[pl.ds(0, count - 1)]
    pltpu.make_async_copy(others, others, path_recv).wait()
    scalars = pltpu.make_async_copy(all_paths, path, local_sem.at[0])
    scalars.start()
    scalars.wait()

    def route(document, column):
        return path[document, 0, column]

    def member_copy(index, source, target, p, landing_own):
        landing = me if landing_own else p
        return to_member(
            source.at[p],
            target.at[landing],
            mem_send.at[index, p],
            mem_recv.at[index, landing],
            p,
        )

    def spread(index, source, target):
        loop(
            1,
            members,
            lambda step: member_copy(
                index, source, target, lax.rem(me + step, members), True
            ).start(),
        )

    def arrive(index, source, target):
        loop(
            1,
            members,
            lambda step: member_copy(
                index, source, target, lax.rem(me + members - step, members), False
            ).wait_recv(),
        )

    def left(index, source, target):
        loop(
            1,
            members,
            lambda step: member_copy(
                index, source, target, lax.rem(me + step, members), False
            ).wait_send(),
        )

    def group_copy(index, source, target, step, landing_own):
        other = lax.rem(group + step, groups)
        landing = group if landing_own else other
        return pltpu.make_async_remote_copy(
            src_ref=source(other),
            dst_ref=target.at[landing],
            send_sem=grp_send.at[index, other],
            recv_sem=grp_recv.at[index, landing],
            device_id={"grp": other},
            device_id_type=MESH,
        )

    def group_spread(*what):
        loop(1, groups, lambda step: group_copy(*what, step, True).start())

    def group_arrive(*what):
        loop(1, groups, lambda step: group_copy(*what, step, False).wait_recv())

    def group_left(*what):
        loop(1, groups, lambda step: group_copy(*what, step, False).wait_send())

    def pick_fine(index):
        held = jnp.clip(route(index, 2) - group * owned, 0, owned - 1)
        fine_out[index // members, lax.rem(index, members)] = fine_w[held]

    def pick_middle(p):
        middle_send[p] = middle_w[route(group * members + p, 1)]

    loop(0, count, pick_fine)
    fine_trade = (0, lambda other: fine_out.at[other], fine_in)
    group_spread(*fine_trade)
    loop(0, members, pick_middle)
    spread(0, middle_send, middle_block)
    fine_in[group] = fine_out[group]
    middle_block[me] = middle_send[me]

    share(0)
    for r in (r for r in range(1, outer) if r % 2):
        if r == 1:
            gather_wait(r)
            pass_on(r)
    for r in range(2, outer, 2):
        gather_wait(r)
        pass_on(r)
    tokens_pair.wait_recv()
    for start in range(0, width, LANES):
        pair_t[start : start + LANES, token_count:] = other_doc[:, start : start + LANES].T

    def merge_fine(p):
        owner = route(group * members + p, 2) // owned
        fine_send[p] = fine_in[owner, p]

    group_arrive(*fine_trade)
    loop(0, members, merge_fine)
    spread(1, fine_send, fine_block)
    fine_block[me] = fine_send[me]

    if outer > 1:
        share(1)
    for r in range(2, outer, 2):
        share(r)
    for r in range(3, outer, 2):
        gather_wait(r)
        pass_on(r)
    for r in range(3, outer, 2):
        share(r)
    if cores > 1:
        for r in range(outer):
            core_copy(r, False).wait_recv()

    own_block = route(device, 0)
    other_block = route(mirror * members + me, 0)

    def coarse_of(k):
        return coarse_w[k].reshape(width, columns)

    first = slot == 0
    pre_give[...] = dot(other_doc[...], coarse_of(other_block))
    pre_pair = pair_copy(1, pre_give, pre_take)
    pre_pair.start()
    pre_own = dot(both[slot], coarse_of(own_block))

    def compute(block, term):
        weights = block[...].reshape(width, block.shape[-1])
        value, part = level(weights, both[0], both[1], flipped[0], flipped[1])
        term[...] = value.reshape(term.shape)
        return part

    middle_own = middle_parts.at[group]
    fine_own = fine_parts.at[group]

    arrive(0, middle_send, middle_block)
    total[...] = compute(middle_block, middle_term)
    spread(2, middle_term, middle_own)
    middle_parts[group, me] = middle_term[me]

    pre_pair.wait_recv()
    pre_other = pre_take[...]
    hidden, before_grad = gelu_parts(
        jnp.where(first, pre_own, pre_other), jnp.where(first, pre_other, pre_own)
    )
    hidden, before_grad = hidden.astype(F32), before_grad.astype(F32)
    act_give[...] = jnp.where(first, hidden, before_grad).astype(BF16)
    act_own = jnp.where(first, before_grad, hidden).astype(BF16)
    act_pair = pair_copy(2, act_give, act_take)
    act_pair.start()

    @pl.when(first)
    def _():
        total[...] += dot_transposed(act_own, coarse_of(own_block))

    act_pair.wait_recv()
    act_other = act_take[...]
    back = pair_copy(3, back_give, back_take)

    for k in range(blocks):
        mine = jnp.where(own_block == k, act_own.astype(F32), 0.0).astype(BF16)
        theirs = jnp.where(other_block == k, act_other.astype(F32), 0.0).astype(BF16)
        value = dot(pair_t[...], jnp.concatenate([mine, theirs], axis=0))
        sums[:, :, :, k] = value.astype(BF16).reshape(outer, sides, cores, rows, columns)

    order = [r for r in range(outer - 1, -1, -1)]

    def fold_core(r):
        return to_member(
            sums.at[flip(r), :, 1 - core],
            from_core.at[r],
            core_send.at[1, r],
            core_recv.at[1, r],
            at_line(0, side, 1 - core),
        )

    def fold_side(r, step):
        there = lax.rem(side + step, sides)
        return to_member(
            sums.at[flip(r), there, core],
            from_side.at[r, step],
            side_send.at[1, r, step],
            side_recv.at[1, r, step],
            at_line(0, there, core),
        )

    def fold_line(r, bit):
        return to_member(
            sums.at[flip(r), side, core],
            from_line.at[r ^ bit, bits.index(bit)],
            fold_send.at[r],
            fold_recv.at[r ^ bit, bits.index(bit)],
            at_line(bit, side, core),
        )

    def fold_line_wait(r, bit):
        to_member(
            sums.at[flip(r), side, core],
            from_line.at[r, bits.index(bit)],
            fold_send.at[r],
            fold_recv.at[r, bits.index(bit)],
            at_line(bit, side, core),
        ).wait_recv()

    def lower(r):
        return [bit for bit in reversed(bits) if r == 0 or bit < (r & -r)]

    if cores > 1:
        for r in order:
            fold_core(r).start()

    @pl.when(first)
    def _():
        back_give[...] = dot_transposed(act_other, coarse_of(other_block)).astype(BF16)
        back.start()

    for r in order:
        if cores > 1:
            fold_core(r).wait_recv()
            for step in range(1, sides):
                there = lax.rem(side + step, sides)
                sums[flip(r), there, core] = (
                    sums[flip(r), there, core].astype(F32) + from_core[r, there].astype(F32)
                ).astype(BF16)
        for step in range(1, sides):
            fold_side(r, step).start()

    arrive(1, fine_send, fine_block)
    total[...] += compute(fine_block, fine_term)
    spread(3, fine_term, fine_own)
    fine_parts[group, me] = fine_term[me]

    def hand_on(target, send_on, recv_on, p, step, landing_own):
        other = lax.rem(group + step, groups)
        landing = group if landing_own else other
        return pltpu.make_async_remote_copy(
            src_ref=target.at[group, p],
            dst_ref=target.at[landing, p],
            send_sem=send_on.at[other, p],
            recv_sem=recv_on.at[landing, p],
            device_id={"grp": other},
            device_id_type=MESH,
        )

    def relay(index, source, target, send_on, recv_on):
        own = target.at[group]

        def start(p):
            loop(1, groups, lambda step: hand_on(target, send_on, recv_on, p, step, True).start())

        def body(step):
            p = lax.rem(me + members - step, members)
            member_copy(index, source, own, p, False).wait_recv()
            start(p)

        start(me)
        loop(1, members, body)

    def relay_done(target, send_on, recv_on):
        def body(index):
            p = index // (groups - 1)
            step = lax.rem(index, groups - 1) + 1
            done = hand_on(target, send_on, recv_on, p, step, False)
            done.wait_recv()
            done.wait_send()

        if groups > 1:
            loop(0, members * (groups - 1), body)

    relay(2, middle_term, middle_parts, middle_send_on, middle_recv_on)

    def folded(r):
        value = sums[flip(r), side, core].astype(F32)
        if cores > 1:
            value = value + from_core[r, side].astype(F32)
        for step in range(1, sides):
            value = value + from_side[r, step].astype(F32)
        for bit in lower(r):
            value = value + from_line[r, bits.index(bit)].astype(F32)
        return value

    for r in order:
        for step in range(1, sides):
            fold_side(r, step).wait_recv()
        for bit in lower(r):
            fold_line_wait(r, bit)
        if r:
            sums[flip(r), side, core] = folded(r).astype(BF16)
            fold_line(r, r & -r).start()
        else:
            coarse_total[...] = folded(0).astype(BF16)

    coarse_trade = (1, lambda other: coarse_total, coarse_parts)
    group_spread(*coarse_trade)
    coarse_parts[group] = coarse_total[...]
    relay(3, fine_term, fine_parts, fine_send_on, fine_recv_on)

    @pl.when(first)
    def _():
        tokens_grad[...] = total[...].astype(BF16)
        back.wait_send()

    @pl.when(slot == 1)
    def _():
        back.wait_recv()
        tokens_grad[...] = (total[...] + back_take[...].astype(F32)).astype(BF16)

    pltpu.make_async_copy(others, others, path_send).wait()
    for copy in (tokens_pair, pre_pair, act_pair):
        copy.wait_send()
    for r in range(outer):
        for bit in gather_on(r):
            gather_copy(r, bit).wait_send()
        for step in range(1, sides):
            side_copy(r, step, True).wait_send()
            fold_side(r, step).wait_send()
        if cores > 1:
            core_copy(r, True).wait_send()
            fold_core(r).wait_send()
        if r:
            fold_line(r, r & -r).wait_send()
    left(0, middle_send, middle_block)
    left(1, fine_send, fine_block)
    group_left(*fine_trade)
    left(2, middle_term, middle_own)
    left(3, fine_term, fine_own)
    group_arrive(*coarse_trade)
    group_left(*coarse_trade)
    relay_done(middle_parts, middle_send_on, middle_recv_on)
    relay_done(fine_parts, fine_send_on, fine_recv_on)


def exchange(path, tokens, cotangent, coarse_w, middle_w, fine_w, groups, members):
    blocks, rows, wide = coarse_w.shape
    medium, narrow = middle_w.shape[2], fine_w.shape[2]
    token_count, width = tokens.shape
    count = groups * members
    outer, sides, cores = plan(groups, members, wide)
    steps = max(len(bits_of(outer)), 1)
    columns = wide // 2

    def stack(*shape):
        return pltpu.VMEM(shape, BF16)

    def sems(*shape):
        return pltpu.SemaphoreType.DMA(shape)

    vmem = pl.BlockSpec(memory_space=pltpu.VMEM)
    return pl.pallas_call(
        functools.partial(main_kernel, groups, members),
        out_shape=(
            jax.ShapeDtypeStruct((count,) + path.shape, jnp.int32),
            jax.ShapeDtypeStruct(tokens.shape, BF16),
            jax.ShapeDtypeStruct((groups, members, rows, medium), BF16),
            jax.ShapeDtypeStruct((groups, members, rows, narrow), BF16),
            jax.ShapeDtypeStruct((groups, blocks, rows, columns), BF16),
        ),
        in_specs=[vmem] + [pl.BlockSpec(memory_space=pl.ANY)] * 5,
        out_specs=(vmem,) * 5,
        scratch_shapes=[
            pltpu.SMEM((count,) + path.shape, jnp.int32),
            stack(2, *tokens.shape),
            stack(*tokens.shape),
            stack(blocks, outer, sides, cores, rows, columns),
            stack(*middle_w.shape),
            stack(*fine_w.shape),
            stack(members, rows, medium),
            stack(groups, members, rows, narrow),
            stack(groups, members, rows, narrow),
            stack(members, rows, narrow),
            stack(members, rows, medium),
            stack(members, rows, narrow),
            stack(members, rows, medium),
            stack(members, rows, narrow),
            stack(outer, sides, cores, blocks, rows, columns),
            stack(outer, sides, blocks, rows, columns),
            stack(outer, sides, blocks, rows, columns),
            stack(outer, steps, blocks, rows, columns),
            stack(blocks, rows, columns),
            stack(2, width, token_count),
            stack(width, 2 * token_count),
            pltpu.VMEM((token_count, width), F32),
            pltpu.VMEM((token_count, columns), F32),
            pltpu.VMEM((token_count, columns), F32),
            stack(token_count, columns),
            stack(token_count, columns),
            stack(token_count, width),
            stack(token_count, width),
            pltpu.SemaphoreType.DMA,
            pltpu.SemaphoreType.DMA,
            sems(4, members),
            sems(4, members),
            sems(2, groups),
            sems(2, groups),
            sems(4),
            sems(4),
            sems(outer, steps),
            sems(outer),
            sems(2, outer, sides),
            sems(2, outer, sides),
            sems(2, outer),
            sems(2, outer),
            sems(outer),
            sems(outer, steps),
            sems(1),
            sems(5),
            sems(groups, members),
            sems(groups, members),
            sems(groups, members),
            sems(groups, members),
        ],
        compiler_params=pltpu.CompilerParams(
            collective_id=0, has_side_effects=True, vmem_limit_bytes=60 * 2**20
        ),
        name="exchange",
    )(path, tokens, cotangent, coarse_w, middle_w, fine_w)


def collect_kernel(
    path,
    first_owned,
    tokens_in,
    middle_hbm,
    fine_hbm,
    coarse_parts,
    tokens_grad,
    coarse_grad,
    middle_grad,
    fine_grad,
    middle_parts,
    fine_parts,
    middle_sum,
    fine_sum,
    middle_last,
    fine_last,
    load_sem,
):
    count = middle_parts.shape[0]
    owned = fine_grad.shape[0]
    loads = (
        pltpu.make_async_copy(middle_hbm, middle_parts, load_sem.at[0]),
        pltpu.make_async_copy(fine_hbm, fine_parts, load_sem.at[1]),
    )
    for load in loads:
        load.start()
    middle_grad[...] = jnp.zeros_like(middle_grad)
    fine_grad[...] = jnp.zeros_like(fine_grad)
    middle_sum[count] = jnp.zeros(middle_sum.shape[1:], F32)
    fine_sum[count] = jnp.zeros(fine_sum.shape[1:], F32)
    for last in (middle_last, fine_last):

        def clear(k, carry, last=last):
            last[k] = count
            return carry

        lax.fori_loop(0, last.shape[0], clear, 0)
    tokens_grad[...] = tokens_in[...]
    groups, _, _, columns = coarse_parts.shape
    team = coarse_grad.shape[2] // columns
    for s in range(team):
        value = coarse_parts[s].astype(F32)
        for other in range(s + team, groups, team):
            value = value + coarse_parts[other].astype(F32)
        coarse_grad[:, :, s * columns : (s + 1) * columns] = value.astype(BF16)
    for load in loads:
        load.wait()

    def add(document, carry):
        k = path[document, 0, 1]
        value = middle_parts[document].astype(F32) + middle_sum[middle_last[k]]
        middle_sum[document] = value
        middle_grad[k] = value.astype(BF16)
        middle_last[k] = document
        place = path[document, 0, 2] - first_owned[0]

        @pl.when((place >= 0) & (place < owned))
        def _():
            piece = fine_parts[document].astype(F32) + fine_sum[fine_last[place]]
            fine_sum[document] = piece
            fine_grad[place] = piece.astype(BF16)
            fine_last[place] = document

        return carry

    lax.fori_loop(0, count, add, 0)


def collect(paths, first_owned, tokens_grad, middle_parts, fine_parts, coarse_parts, shapes):
    vmem = pl.BlockSpec(memory_space=pltpu.VMEM)
    smem = pl.BlockSpec(memory_space=pltpu.SMEM)
    hbm = pl.BlockSpec(memory_space=pl.ANY)
    count, rows, medium = middle_parts.shape
    narrow = fine_parts.shape[2]
    return pl.pallas_call(
        collect_kernel,
        out_shape=tuple(
            jax.ShapeDtypeStruct(shape, BF16) for shape in (tokens_grad.shape,) + shapes
        ),
        in_specs=[smem, smem, vmem, hbm, hbm, vmem],
        out_specs=(vmem,) * 4,
        scratch_shapes=[
            pltpu.VMEM(middle_parts.shape, BF16),
            pltpu.VMEM(fine_parts.shape, BF16),
            pltpu.VMEM((count + 1, rows, medium), F32),
            pltpu.VMEM((count + 1, rows, narrow), F32),
            pltpu.SMEM((shapes[1][0],), jnp.int32),
            pltpu.SMEM((shapes[2][0],), jnp.int32),
            pltpu.SemaphoreType.DMA((2,)),
        ],
        compiler_params=pltpu.CompilerParams(vmem_limit_bytes=60 * 2**20),
        name="collect",
    )(paths, first_owned, tokens_grad, middle_parts, fine_parts, coarse_parts)


def on_device(tokens, cotangent, path, coarse_weights, middle_weights, fine_weights):
    members = lax.axis_size("mem")
    groups = lax.axis_size("grp")
    paths, tokens_grad, middle_parts, fine_parts, coarse_parts = exchange(
        path, tokens, cotangent, coarse_weights, middle_weights, fine_weights, groups, members
    )
    first_owned = (lax.axis_index("grp") * fine_weights.shape[0]).astype(jnp.int32).reshape(1)
    flat = lambda parts: parts.reshape((groups * members,) + parts.shape[2:])
    return collect(
        paths,
        first_owned,
        tokens_grad,
        flat(middle_parts),
        flat(fine_parts),
        coarse_parts,
        (coarse_weights.shape, middle_weights.shape, fine_weights.shape),
    )


def solution(mesh):
    return jax.shard_map(
        on_device,
        mesh=mesh,
        in_specs=(
            P(("grp", "mem"), None),
            P(("grp", "mem"), None),
            P(("grp", "mem"), None),
            P(None, "mem", None),
            P(None, "mem", None),
            P("grp", "mem", None),
        ),
        out_specs=(
            P(("grp", "mem"), None),
            P(None, "mem", None),
            P(None, "mem", None),
            P("grp", "mem", None),
        ),
        check_vma=False,
    )
```

```python
import functools
import math

import jax
import jax.numpy as jnp
from jax import lax
from jax.experimental import pallas as pl
from jax.experimental.pallas import tpu as pltpu
from jax.sharding import PartitionSpec as P

MESH = pl.DeviceIdType.MESH
LANES = 128
F32 = jnp.float32
BF16 = jnp.bfloat16


def gelu_parts(before, hidden_grad):
    scale = math.sqrt(2.0 / math.pi)
    square = before * before
    tanh = jnp.tanh(scale * (before + 0.044715 * (square * before)))
    half = 0.5 * (1.0 + tanh)
    hidden = before * half
    slope = half + 0.5 * before * (1.0 - tanh * tanh) * (scale * (1.0 + 3 * 0.044715 * square))
    return hidden.astype(BF16), (hidden_grad * slope).astype(BF16)


def dot(left, right):
    return jnp.dot(left, right, preferred_element_type=F32)


def dot_transposed(left, right):
    return lax.dot_general(left, right, (((1,), (1,)), ((), ())), preferred_element_type=F32)


def level(weights, x, g, xt, gt):
    width = weights.shape[1]
    half = width // 2
    if half % LANES == 0:
        up = weights[:, :half]
        down = weights[:, half:]
        hidden, grad = gelu_parts(dot(x, up), dot(g, down))
        term = jnp.concatenate(
            [dot(xt, grad).astype(BF16), dot(gt, hidden).astype(BF16)], axis=1
        )
        return term, dot_transposed(grad, up)
    before = dot(x, weights)
    hidden_grad = pltpu.roll(dot(g, weights), half, 1)
    hidden, grad = gelu_parts(before, hidden_grad)
    first = lax.broadcasted_iota(jnp.int32, grad.shape, 1) < half
    grad = jnp.where(first, grad.astype(F32), 0.0).astype(BF16)
    hidden = jnp.where(first, hidden.astype(F32), 0.0)
    hidden = pltpu.roll(hidden, half, 1).astype(BF16)
    term = (dot(xt, grad) + dot(gt, hidden)).astype(BF16)
    return term, dot_transposed(grad, weights)


def plan(groups, members, blocks_width):
    inner = max(k for k in range(1, math.isqrt(members) + 1) if members % k == 0)
    cores = 2 if inner % 2 == 0 else 1
    return members // inner, inner // cores, cores


def bits_of(outer):
    bits = []
    while outer > 1:
        outer //= 2
        bits.append(outer)
    return bits


def main_kernel(
    groups,
    members,
    path_row,
    tokens_hbm,
    cotangent_hbm,
    coarse_hbm,
    middle_hbm,
    fine_hbm,
    paths_out,
    tokens_out,
    middle_out,
    fine_parts_out,
    coarse_out,
    all_paths,
    tokens_grad,
    middle_parts,
    fine_parts,
    coarse_parts,
    path,
    both,
    other_doc,
    coarse_w,
    middle_w,
    fine_w,
    middle_send,
    fine_out,
    fine_in,
    fine_send,
    middle_block,
    fine_block,
    middle_term,
    fine_term,
    sums,
    from_core,
    from_side,
    from_line,
    coarse_total,
    flipped,
    pair_t,
    total,
    pre_give,
    pre_take,
    act_give,
    act_take,
    back_give,
    back_take,
    path_send,
    path_recv,
    mem_send,
    mem_recv,
    weight_recv,
    grp_send,
    grp_recv,
    pair_send,
    pair_recv,
    gather_send,
    gather_recv,
    side_send,
    side_recv,
    core_send,
    core_recv,
    fold_send,
    fold_recv,
    local_sem,
    load_sem,
    out_sem,
    middle_send_on,
    middle_recv_on,
    fine_send_on,
    fine_recv_on,
):
    group = lax.axis_index("grp")
    me = lax.axis_index("mem")
    count = groups * members
    device = group * members + me
    owned = fine_w.shape[0]
    blocks, outer, sides, cores, rows, columns = coarse_w.shape
    inner = sides * cores
    bits = bits_of(outer)
    line = me // inner
    place = lax.rem(me, inner)
    side = place // cores
    core = lax.rem(place, cores)
    slot = lax.rem(group, 2)
    mirror = group + 1 - 2 * slot
    token_count, width = tokens_grad.shape

    def loop(start, stop, body):
        def wrapped(step, carry):
            body(step)
            return carry

        lax.fori_loop(start, stop, wrapped, 0)

    def flip(r):
        there = line
        for bit in bits:
            if r & bit:
                there = there + bit * (1 - 2 * lax.rem(there // bit, 2))
        return there

    def at_line(r, s, c):
        return flip(r) * inner + s * cores + c

    def to_member(source, target, send, recv, p):
        return pltpu.make_async_remote_copy(
            src_ref=source,
            dst_ref=target,
            send_sem=send,
            recv_sem=recv,
            device_id={"mem": p},
            device_id_type=MESH,
        )

    half = pl.ds(pl.multiple_of(slot * columns, LANES), columns)
    loads = [
        pltpu.make_async_copy(source, target, load_sem.at[index])
        for index, (source, target) in enumerate(
            (
                (tokens_hbm, both.at[0]),
                (cotangent_hbm, both.at[1]),
                (coarse_hbm.at[:, :, half], coarse_w.at[:, line, side, core]),
                (fine_hbm, fine_w),
                (middle_hbm, middle_w),
            )
        )
    ]
    for load in loads:
        load.start()
    outs = [
        pltpu.make_async_copy(source, target, out_sem.at[index])
        for index, (source, target) in enumerate(
            (
                (all_paths, paths_out),
                (tokens_grad, tokens_out),
                (middle_parts, middle_out),
                (fine_parts, fine_parts_out),
                (coarse_parts, coarse_out),
            )
        )
    ]
    barrier = pltpu.get_barrier_semaphore()

    def anyone(step):
        other = lax.rem(device + step, count)
        return other, (other // members, lax.rem(other, members))

    def greet(step):
        _, where = anyone(step)
        pl.semaphore_signal(barrier, inc=1, device_id=where, device_id_type=MESH)

    loop(1, count, greet)
    for load in loads[:3]:
        load.wait()
    pl.semaphore_wait(barrier, count - 1)

    def path_copy(step):
        _, where = anyone(step)
        return pltpu.make_async_remote_copy(
            src_ref=path_row,
            dst_ref=all_paths.at[device],
            send_sem=path_send,
            recv_sem=path_recv,
            device_id=where,
            device_id_type=MESH,
        )

    loop(1, count, lambda step: path_copy(step).start())
    all_paths[device] = path_row[...]

    def pair_copy(index, source, target):
        return pltpu.make_async_remote_copy(
            src_ref=source,
            dst_ref=target,
            send_sem=pair_send.at[index],
            recv_sem=pair_recv.at[index],
            device_id={"grp": mirror},
            device_id_type=MESH,
        )

    def gather_copy(r, bit):
        piece = coarse_w.at[:, flip(r), side, core]
        return to_member(
            piece,
            piece,
            gather_send.at[r, bits.index(bit)],
            gather_recv.at[r ^ bit],
            at_line(bit, side, core),
        )

    def gather_wait(r):
        piece = coarse_w.at[:, flip(r), side, core]
        bit = r & -r
        to_member(
            piece, piece, gather_send.at[0, 0], gather_recv.at[r], at_line(bit, side, core)
        ).wait_recv()

    def gather_on(r):
        return [bit for bit in bits if r == 0 or bit < (r & -r)]

    def side_copy(r, step, landing_own):
        there = lax.rem(side + step, sides)
        landing = side if landing_own else lax.rem(side + sides - step, sides)
        piece = coarse_w.at[:, flip(r), landing, core]
        return to_member(
            piece, piece, side_send.at[0, r, step], side_recv.at[0, r, step], at_line(0, there, core)
        )

    def core_copy(r, landing_own):
        piece = coarse_w.at[:, flip(r), :, core if landing_own else 1 - core]
        return to_member(
            piece, piece, core_send.at[0, r], core_recv.at[0, r], at_line(0, side, 1 - core)
        )

    tokens_pair = pair_copy(0, both.at[1 - slot], other_doc)

    def pass_on(r):
        for bit in gather_on(r):
            gather_copy(r, bit).start()
        for step in range(1, sides):
            side_copy(r, step, True).start()

    def share(r):
        for step in range(1, sides):
            side_copy(r, step, False).wait_recv()
        if cores > 1:
            core_copy(r, True).start()

    pass_on(0)
    tokens_pair.start()
    for which in range(2):
        for start in range(0, width, LANES):
            part = slice(start, start + LANES)
            flipped[which, part, :] = both[which, :, part].T
    for load in loads[3:]:
        load.wait()
    pair_t[:, :token_count] = flipped[slot]
    if outer > 1:
        gather_wait(1)
        pass_on(1)
    share(0)

    others = all_paths.at[pl.ds(0, count - 1)]
    pltpu.make_async_copy(others, others, path_recv).wait()
    scalars = pltpu.make_async_copy(all_paths, path, local_sem.at[0])
    scalars.start()
    scalars.wait()
    outs[0].start()

    def route(document, column):
        return path[document, 0, column]

    def member_copy(index, source, target, p, landing_own):
        landing = me if landing_own else p
        arrived = weight_recv.at[index] if index < 2 else mem_recv.at[index - 2, landing]
        return to_member(source.at[p], target.at[landing], mem_send.at[index], arrived, p)

    def all_of(ref, number, sem):
        some = ref.at[pl.ds(0, number)]
        return pltpu.make_async_copy(some, some, sem)

    near = outer * cores

    def partner(step):
        there = lax.rem(side + step // near, sides)
        rest = lax.rem(step, near)
        return (
            lax.rem(line + rest // cores, outer) * inner
            + there * cores
            + lax.rem(core + lax.rem(rest, cores), cores)
        )

    def spread(index, source, target, start=1, stop=members):
        loop(
            start,
            stop,
            lambda step: member_copy(index, source, target, partner(step), True).start(),
        )

    def arrive(index, target):
        if members > 1:
            all_of(target, members - 1, weight_recv.at[index]).wait()

    def left(index, source):
        if members > 1:
            all_of(source, members - 1, mem_send.at[index]).wait()

    def group_copy(index, source, target, step, landing_own):
        other = lax.rem(group + step, groups)
        landing = group if landing_own else other
        return pltpu.make_async_remote_copy(
            src_ref=source(other),
            dst_ref=target.at[landing],
            send_sem=grp_send.at[index, other],
            recv_sem=grp_recv.at[index, landing],
            device_id={"grp": other},
            device_id_type=MESH,
        )

    def group_spread(*what):
        loop(1, groups, lambda step: group_copy(*what, step, True).start())

    def group_arrive(*what):
        loop(1, groups, lambda step: group_copy(*what, step, False).wait_recv())

    def group_left(*what):
        loop(1, groups, lambda step: group_copy(*what, step, False).wait_send())

    def pick_fine(index):
        held = jnp.clip(route(index, 2) - group * owned, 0, owned - 1)
        fine_out[index // members, lax.rem(index, members)] = fine_w[held]

    def pick_middle(p):
        middle_send[p] = middle_w[route(group * members + p, 1)]

    loop(0, count, pick_fine)
    fine_trade = (0, lambda other: fine_out.at[other], fine_in)
    group_spread(*fine_trade)
    loop(0, members, pick_middle)
    spread(0, middle_send, middle_block, 1, near)
    fine_in[group] = fine_out[group]
    middle_block[me] = middle_send[me]

    for r in range(2, outer, 2):
        gather_wait(r)
        pass_on(r)
    if outer > 1:
        share(1)
    for r in range(3, outer, 2):
        gather_wait(r)
        pass_on(r)
    spread(0, middle_send, middle_block, near, members)
    tokens_pair.wait_recv()
    for start in range(0, width, LANES):
        pair_t[start : start + LANES, token_count:] = other_doc[:, start : start + LANES].T
    for r in range(2, outer, 2):
        share(r)

    def merge_fine(p):
        owner = route(group * members + p, 2) // owned
        fine_send[p] = fine_in[owner, p]

    group_arrive(*fine_trade)
    loop(0, members, merge_fine)
    spread(1, fine_send, fine_block)
    fine_block[me] = fine_send[me]

    for r in range(3, outer, 2):
        share(r)
    if cores > 1:
        for r in range(outer):
            core_copy(r, False).wait_recv()

    own_block = route(device, 0)
    other_block = route(mirror * members + me, 0)

    def coarse_of(k):
        return coarse_w[k].reshape(width, columns)

    first = slot == 0
    pre_give[...] = dot(other_doc[...], coarse_of(other_block))
    pre_pair = pair_copy(1, pre_give, pre_take)
    pre_pair.start()
    pre_own = dot(both[slot], coarse_of(own_block))

    def compute(block, term):
        weights = block[...].reshape(width, block.shape[-1])
        value, part = level(weights, both[0], both[1], flipped[0], flipped[1])
        term[...] = value.reshape(term.shape)
        return part

    middle_own = middle_parts.at[group]
    fine_own = fine_parts.at[group]

    arrive(0, middle_block)
    total[...] = compute(middle_block, middle_term)
    spread(2, middle_term, middle_own)
    middle_parts[group, me] = middle_term[me]

    pre_pair.wait_recv()
    pre_other = pre_take[...]
    hidden, before_grad = gelu_parts(
        jnp.where(first, pre_own, pre_other), jnp.where(first, pre_other, pre_own)
    )
    hidden, before_grad = hidden.astype(F32), before_grad.astype(F32)
    act_give[...] = jnp.where(first, hidden, before_grad).astype(BF16)
    act_own = jnp.where(first, before_grad, hidden).astype(BF16)
    act_pair = pair_copy(2, act_give, act_take)
    act_pair.start()

    @pl.when(first)
    def _():
        total[...] += dot_transposed(act_own, coarse_of(own_block))

    act_pair.wait_recv()
    act_other = act_take[...]
    back = pair_copy(3, back_give, back_take)

    for k in range(blocks):
        mine = jnp.where(own_block == k, act_own.astype(F32), 0.0).astype(BF16)
        theirs = jnp.where(other_block == k, act_other.astype(F32), 0.0).astype(BF16)
        value = dot(pair_t[...], jnp.concatenate([mine, theirs], axis=0))
        sums[:, :, :, k] = value.astype(BF16).reshape(outer, sides, cores, rows, columns)

    order = list(range(outer - 1, 0, -2)) + list(range(outer - 2, 0, -2)) + [0]

    def fold_core(r):
        return to_member(
            sums.at[flip(r), :, 1 - core],
            from_core.at[r],
            core_send.at[1, r],
            core_recv.at[1, r],
            at_line(0, side, 1 - core),
        )

    def fold_side(r, step):
        there = lax.rem(side + step, sides)
        return to_member(
            sums.at[flip(r), there, core],
            from_side.at[r, step],
            side_send.at[1, r, step],
            side_recv.at[1, r, step],
            at_line(0, there, core),
        )

    def fold_line(r, bit):
        return to_member(
            sums.at[flip(r), side, core],
            from_line.at[r ^ bit, bits.index(bit)],
            fold_send.at[r],
            fold_recv.at[r ^ bit, bits.index(bit)],
            at_line(bit, side, core),
        )

    def fold_line_wait(r, bit):
        to_member(
            sums.at[flip(r), side, core],
            from_line.at[r, bits.index(bit)],
            fold_send.at[r],
            fold_recv.at[r, bits.index(bit)],
            at_line(bit, side, core),
        ).wait_recv()

    def lower(r):
        return [bit for bit in reversed(bits) if r == 0 or bit < (r & -r)]

    if cores > 1:
        for r in order:
            fold_core(r).start()

    @pl.when(first)
    def _():
        back_give[...] = dot_transposed(act_other, coarse_of(other_block)).astype(BF16)
        back.start()

    for r in order:
        if cores > 1:
            fold_core(r).wait_recv()
            for step in range(1, sides):
                there = lax.rem(side + step, sides)
                sums[flip(r), there, core] = (
                    sums[flip(r), there, core].astype(F32) + from_core[r, there].astype(F32)
                ).astype(BF16)
        for step in range(1, sides):
            fold_side(r, step).start()

    arrive(1, fine_block)
    total[...] += compute(fine_block, fine_term)
    spread(3, fine_term, fine_own)
    fine_parts[group, me] = fine_term[me]

    def hand_on(target, send_on, recv_on, p, step, landing_own):
        other = lax.rem(group + step, groups)
        landing = group if landing_own else other
        return pltpu.make_async_remote_copy(
            src_ref=target.at[group, p],
            dst_ref=target.at[landing, p],
            send_sem=send_on,
            recv_sem=recv_on,
            device_id={"grp": other},
            device_id_type=MESH,
        )

    def relay(index, source, target, send_on, recv_on):
        own = target.at[group]

        def start(p):
            loop(1, groups, lambda step: hand_on(target, send_on, recv_on, p, step, True).start())

        def body(step):
            p = lax.rem(me + members - step, members)
            member_copy(index, source, own, p, False).wait_recv()
            start(p)

        start(me)
        loop(1, members, body)

    def relay_done(target, send_on, recv_on):
        if groups > 1:
            all_of(target, groups - 1, recv_on).wait()
            all_of(target, groups - 1, send_on).wait()

    relay(2, middle_term, middle_parts, middle_send_on, middle_recv_on)

    def folded(r):
        value = sums[flip(r), side, core].astype(F32)
        if cores > 1:
            value = value + from_core[r, side].astype(F32)
        for step in range(1, sides):
            value = value + from_side[r, step].astype(F32)
        for bit in lower(r):
            value = value + from_line[r, bits.index(bit)].astype(F32)
        return value

    for r in order:
        for step in range(1, sides):
            fold_side(r, step).wait_recv()
        for bit in lower(r):
            fold_line_wait(r, bit)
        if r:
            sums[flip(r), side, core] = folded(r).astype(BF16)
            fold_line(r, r & -r).start()
            if r == order[-2]:
                relay(3, fine_term, fine_parts, fine_send_on, fine_recv_on)
        else:
            coarse_total[...] = folded(0).astype(BF16)

    coarse_trade = (1, lambda other: coarse_total, coarse_parts)
    group_spread(*coarse_trade)
    coarse_parts[group] = coarse_total[...]

    @pl.when(first)
    def _():
        tokens_grad[...] = total[...].astype(BF16)
        back.wait_send()

    @pl.when(slot == 1)
    def _():
        back.wait_recv()
        tokens_grad[...] = (total[...] + back_take[...].astype(F32)).astype(BF16)

    outs[1].start()
    pltpu.make_async_copy(others, others, path_send).wait()
    for copy in (tokens_pair, pre_pair, act_pair):
        copy.wait_send()
    for r in range(outer):
        for bit in gather_on(r):
            gather_copy(r, bit).wait_send()
        for step in range(1, sides):
            side_copy(r, step, True).wait_send()
            fold_side(r, step).wait_send()
        if cores > 1:
            core_copy(r, True).wait_send()
            fold_core(r).wait_send()
        if r:
            fold_line(r, r & -r).wait_send()
    left(0, middle_send)
    left(1, fine_send)
    group_left(*fine_trade)
    left(2, middle_term)
    left(3, fine_term)
    relay_done(middle_parts, middle_send_on, middle_recv_on)
    outs[2].start()
    relay_done(fine_parts, fine_send_on, fine_recv_on)
    outs[3].start()
    group_arrive(*coarse_trade)
    outs[4].start()
    group_left(*coarse_trade)
    for out in outs:
        out.wait()


def exchange(path, tokens, cotangent, coarse_w, middle_w, fine_w, groups, members):
    blocks, rows, wide = coarse_w.shape
    medium, narrow = middle_w.shape[2], fine_w.shape[2]
    token_count, width = tokens.shape
    count = groups * members
    outer, sides, cores = plan(groups, members, wide)
    steps = max(len(bits_of(outer)), 1)
    columns = wide // 2

    def stack(*shape):
        return pltpu.VMEM(shape, BF16)

    def sems(*shape):
        return pltpu.SemaphoreType.DMA(shape)

    vmem = pl.BlockSpec(memory_space=pltpu.VMEM)
    return pl.pallas_call(
        functools.partial(main_kernel, groups, members),
        out_shape=(
            jax.ShapeDtypeStruct((count,) + path.shape, jnp.int32),
            jax.ShapeDtypeStruct(tokens.shape, BF16),
            jax.ShapeDtypeStruct((groups, members, rows, medium), BF16),
            jax.ShapeDtypeStruct((groups, members, rows, narrow), BF16),
            jax.ShapeDtypeStruct((groups, blocks, rows, columns), BF16),
        ),
        in_specs=[vmem] + [pl.BlockSpec(memory_space=pl.ANY)] * 5,
        out_specs=(pl.BlockSpec(memory_space=pl.ANY),) * 5,
        scratch_shapes=[
            pltpu.VMEM((count,) + path.shape, jnp.int32),
            stack(*tokens.shape),
            stack(groups, members, rows, medium),
            stack(groups, members, rows, narrow),
            stack(groups, blocks, rows, columns),
            pltpu.SMEM((count,) + path.shape, jnp.int32),
            stack(2, *tokens.shape),
            stack(*tokens.shape),
            stack(blocks, outer, sides, cores, rows, columns),
            stack(*middle_w.shape),
            stack(*fine_w.shape),
            stack(members, rows, medium),
            stack(groups, members, rows, narrow),
            stack(groups, members, rows, narrow),
            stack(members, rows, narrow),
            stack(members, rows, medium),
            stack(members, rows, narrow),
            stack(members, rows, medium),
            stack(members, rows, narrow),
            stack(outer, sides, cores, blocks, rows, columns),
            stack(outer, sides, blocks, rows, columns),
            stack(outer, sides, blocks, rows, columns),
            stack(outer, steps, blocks, rows, columns),
            stack(blocks, rows, columns),
            stack(2, width, token_count),
            stack(width, 2 * token_count),
            pltpu.VMEM((token_count, width), F32),
            pltpu.VMEM((token_count, columns), F32),
            pltpu.VMEM((token_count, columns), F32),
            stack(token_count, columns),
            stack(token_count, columns),
            stack(token_count, width),
            stack(token_count, width),
            pltpu.SemaphoreType.DMA,
            pltpu.SemaphoreType.DMA,
            sems(4),
            sems(2, members),
            sems(2),
            sems(2, groups),
            sems(2, groups),
            sems(4),
            sems(4),
            sems(outer, steps),
            sems(outer),
            sems(2, outer, sides),
            sems(2, outer, sides),
            sems(2, outer),
            sems(2, outer),
            sems(outer),
            sems(outer, steps),
            sems(1),
            sems(5),
            sems(5),
            pltpu.SemaphoreType.DMA,
            pltpu.SemaphoreType.DMA,
            pltpu.SemaphoreType.DMA,
            pltpu.SemaphoreType.DMA,
        ],
        compiler_params=pltpu.CompilerParams(
            collective_id=0, has_side_effects=True, vmem_limit_bytes=60 * 2**20
        ),
        name="exchange",
    )(path, tokens, cotangent, coarse_w, middle_w, fine_w)


def collect_kernel(
    path,
    first_owned,
    tokens_in,
    middle_hbm,
    fine_hbm,
    coarse_parts,
    tokens_grad,
    coarse_grad,
    middle_grad,
    fine_grad,
    middle_parts,
    fine_parts,
    middle_sum,
    fine_sum,
    middle_last,
    fine_last,
    load_sem,
):
    count = middle_parts.shape[0]
    owned = fine_grad.shape[0]
    loads = (
        pltpu.make_async_copy(middle_hbm, middle_parts, load_sem.at[0]),
        pltpu.make_async_copy(fine_hbm, fine_parts, load_sem.at[1]),
    )
    for load in loads:
        load.start()
    middle_grad[...] = jnp.zeros_like(middle_grad)
    fine_grad[...] = jnp.zeros_like(fine_grad)
    middle_sum[count] = jnp.zeros(middle_sum.shape[1:], F32)
    fine_sum[count] = jnp.zeros(fine_sum.shape[1:], F32)
    for last in (middle_last, fine_last):

        def clear(k, carry, last=last):
            last[k] = count
            return carry

        lax.fori_loop(0, last.shape[0], clear, 0)
    tokens_grad[...] = tokens_in[...]
    groups, _, _, columns = coarse_parts.shape
    team = coarse_grad.shape[2] // columns
    for s in range(team):
        value = coarse_parts[s].astype(F32)
        for other in range(s + team, groups, team):
            value = value + coarse_parts[other].astype(F32)
        coarse_grad[:, :, s * columns : (s + 1) * columns] = value.astype(BF16)
    for load in loads:
        load.wait()

    def add(document, carry):
        k = path[document, 0, 1]
        value = middle_parts[document].astype(F32) + middle_sum[middle_last[k]]
        middle_sum[document] = value
        middle_grad[k] = value.astype(BF16)
        middle_last[k] = document
        place = path[document, 0, 2] - first_owned[0]

        @pl.when((place >= 0) & (place < owned))
        def _():
            piece = fine_parts[document].astype(F32) + fine_sum[fine_last[place]]
            fine_sum[document] = piece
            fine_grad[place] = piece.astype(BF16)
            fine_last[place] = document

        return carry

    lax.fori_loop(0, count, add, 0)


def collect(paths, first_owned, tokens_grad, middle_parts, fine_parts, coarse_parts, shapes):
    vmem = pl.BlockSpec(memory_space=pltpu.VMEM)
    smem = pl.BlockSpec(memory_space=pltpu.SMEM)
    hbm = pl.BlockSpec(memory_space=pl.ANY)
    count, rows, medium = middle_parts.shape
    narrow = fine_parts.shape[2]
    return pl.pallas_call(
        collect_kernel,
        out_shape=tuple(
            jax.ShapeDtypeStruct(shape, BF16) for shape in (tokens_grad.shape,) + shapes
        ),
        in_specs=[smem, smem, vmem, hbm, hbm, vmem],
        out_specs=(vmem,) * 4,
        scratch_shapes=[
            pltpu.VMEM(middle_parts.shape, BF16),
            pltpu.VMEM(fine_parts.shape, BF16),
            pltpu.VMEM((count + 1, rows, medium), F32),
            pltpu.VMEM((count + 1, rows, narrow), F32),
            pltpu.SMEM((shapes[1][0],), jnp.int32),
            pltpu.SMEM((shapes[2][0],), jnp.int32),
            pltpu.SemaphoreType.DMA((2,)),
        ],
        compiler_params=pltpu.CompilerParams(vmem_limit_bytes=60 * 2**20),
        name="collect",
    )(paths, first_owned, tokens_grad, middle_parts, fine_parts, coarse_parts)


def on_device(tokens, cotangent, path, coarse_weights, middle_weights, fine_weights):
    members = lax.axis_size("mem")
    groups = lax.axis_size("grp")
    paths, tokens_grad, middle_parts, fine_parts, coarse_parts = exchange(
        path, tokens, cotangent, coarse_weights, middle_weights, fine_weights, groups, members
    )
    first_owned = (lax.axis_index("grp") * fine_weights.shape[0]).astype(jnp.int32).reshape(1)
    flat = lambda parts: parts.reshape((groups * members,) + parts.shape[2:])
    return collect(
        paths,
        first_owned,
        tokens_grad,
        flat(middle_parts),
        flat(fine_parts),
        coarse_parts,
        (coarse_weights.shape, middle_weights.shape, fine_weights.shape),
    )


def solution(mesh):
    return jax.shard_map(
        on_device,
        mesh=mesh,
        in_specs=(
            P(("grp", "mem"), None),
            P(("grp", "mem"), None),
            P(("grp", "mem"), None),
            P(None, "mem", None),
            P(None, "mem", None),
            P("grp", "mem", None),
        ),
        out_specs=(
            P(("grp", "mem"), None),
            P(None, "mem", None),
            P(None, "mem", None),
            P("grp", "mem", None),
        ),
        check_vma=False,
    )
```

```python
import functools
import math

import jax
import jax.numpy as jnp
from jax import lax
from jax.experimental import pallas as pl
from jax.experimental.pallas import tpu as pltpu
from jax.sharding import PartitionSpec as P

MESH = pl.DeviceIdType.MESH
LANES = 128
F32 = jnp.float32
BF16 = jnp.bfloat16


def gelu_parts(before, hidden_grad):
    scale = math.sqrt(2.0 / math.pi)
    square = before * before
    tanh = jnp.tanh(scale * (before + 0.044715 * (square * before)))
    half = 0.5 * (1.0 + tanh)
    hidden = before * half
    slope = half + 0.5 * before * (1.0 - tanh * tanh) * (scale * (1.0 + 3 * 0.044715 * square))
    return hidden.astype(BF16), (hidden_grad * slope).astype(BF16)


def dot(left, right):
    return jnp.dot(left, right, preferred_element_type=F32)


def dot_transposed(left, right):
    return lax.dot_general(left, right, (((1,), (1,)), ((), ())), preferred_element_type=F32)


def level(weights, x, g, xt, gt):
    width = weights.shape[1]
    half = width // 2
    if half % LANES == 0:
        up = weights[:, :half]
        down = weights[:, half:]
        hidden, grad = gelu_parts(dot(x, up), dot(g, down))
        term = jnp.concatenate(
            [dot(xt, grad).astype(BF16), dot(gt, hidden).astype(BF16)], axis=1
        )
        return term, dot_transposed(grad, up)
    before = dot(x, weights)
    hidden_grad = pltpu.roll(dot(g, weights), half, 1)
    hidden, grad = gelu_parts(before, hidden_grad)
    first = lax.broadcasted_iota(jnp.int32, grad.shape, 1) < half
    grad = jnp.where(first, grad.astype(F32), 0.0).astype(BF16)
    hidden = jnp.where(first, hidden.astype(F32), 0.0)
    hidden = pltpu.roll(hidden, half, 1).astype(BF16)
    term = (dot(xt, grad) + dot(gt, hidden)).astype(BF16)
    return term, dot_transposed(grad, weights)


def plan(members, rows):
    inner = max(k for k in range(1, math.isqrt(members) + 1) if members % k == 0)
    cores = next(
        k for k in range(1, inner + 1) if inner % k == 0 and (k * rows % LANES == 0 or k == inner)
    )
    return members // inner, inner // cores, cores


def bits_of(outer):
    bits = []
    while outer > 1:
        outer //= 2
        bits.append(outer)
    return bits


def main_kernel(
    groups,
    members,
    path_row,
    tokens_hbm,
    cotangent_hbm,
    coarse_hbm,
    middle_hbm,
    fine_hbm,
    paths_out,
    tokens_out,
    middle_out,
    fine_parts_out,
    coarse_out,
    all_paths,
    tokens_grad,
    middle_parts,
    fine_parts,
    coarse_parts,
    path,
    both,
    docs,
    coarse_w,
    middle_w,
    fine_w,
    middle_send,
    fine_out,
    fine_in,
    fine_send,
    middle_block,
    fine_block,
    middle_term,
    fine_term,
    sums,
    from_core,
    from_line,
    coarse_total,
    flipped,
    quad_t,
    total,
    pre_give,
    pre_take,
    act_keep,
    act_give,
    act_take,
    back_give,
    back_take,
    path_send,
    path_recv,
    mem_send,
    mem_recv,
    weight_recv,
    grp_send,
    grp_recv,
    quad_send,
    quad_recv,
    gather_send,
    gather_recv,
    core_send,
    core_recv,
    fold_send,
    fold_recv,
    local_sem,
    load_sem,
    token_sem,
    out_sem,
    middle_send_on,
    middle_recv_on,
    fine_send_on,
    fine_recv_on,
):
    group = lax.axis_index("grp")
    me = lax.axis_index("mem")
    count = groups * members
    device = group * members + me
    owned = fine_w.shape[0]
    blocks, outer, cores, rows, columns = coarse_w.shape
    _, _, sides, token_count, span = both.shape
    inner = sides * cores
    depth = outer * span
    bits = bits_of(outer)
    line = me // inner
    place = lax.rem(me, inner)
    side = place // cores
    core = lax.rem(place, cores)
    slot = lax.rem(group, 2)
    mirror = group + 1 - 2 * slot
    width = tokens_grad.shape[1]

    def loop(start, stop, body):
        def wrapped(step, carry):
            body(step)
            return carry

        lax.fori_loop(start, stop, wrapped, 0)

    def flip(r):
        there = line
        for bit in bits:
            if r & bit:
                there = there + bit * (1 - 2 * lax.rem(there // bit, 2))
        return there

    def at_line(r, s, c):
        return flip(r) * inner + s * cores + c

    def to_member(source, target, send, recv, p):
        return pltpu.make_async_remote_copy(
            src_ref=source,
            dst_ref=target,
            send_sem=send,
            recv_sem=recv,
            device_id={"mem": p},
            device_id_type=MESH,
        )

    half = pl.ds(pl.multiple_of(slot * columns, LANES), columns)
    loads = [
        pltpu.make_async_copy(source, target, load_sem.at[index])
        for index, (source, target) in enumerate(
            (
                (coarse_hbm.at[:, :, half], coarse_w.at[:, line, core]),
                (fine_hbm, fine_w),
                (middle_hbm, middle_w),
            )
        )
    ]
    places = [(o, a) for o in range(outer) for a in range(sides)]
    token_loads = [
        pltpu.make_async_copy(
            source.at[:, pl.ds(index * span, span)],
            both.at[which, o, a],
            token_sem.at[which, index],
        )
        for which, source in enumerate((tokens_hbm, cotangent_hbm))
        for index, (o, a) in enumerate(places)
    ]
    loads[0].start()
    for load in token_loads:
        load.start()
    for load in loads[1:]:
        load.start()
    outs = [
        pltpu.make_async_copy(source, target, out_sem.at[index])
        for index, (source, target) in enumerate(
            (
                (all_paths, paths_out),
                (tokens_grad, tokens_out),
                (middle_parts, middle_out),
                (fine_parts, fine_parts_out),
                (coarse_parts, coarse_out),
            )
        )
    ]
    barrier = pltpu.get_barrier_semaphore()

    def anyone(step):
        other = lax.rem(device + step, count)
        return other, (other // members, lax.rem(other, members))

    def greet(step):
        _, where = anyone(step)
        pl.semaphore_signal(barrier, inc=1, device_id=where, device_id_type=MESH)

    loop(1, count, greet)
    loads[0].wait()
    pl.semaphore_wait(barrier, count - 1)

    def path_copy(step):
        _, where = anyone(step)
        return pltpu.make_async_remote_copy(
            src_ref=path_row,
            dst_ref=all_paths.at[device],
            send_sem=path_send,
            recv_sem=path_recv,
            device_id=where,
            device_id_type=MESH,
        )

    loop(1, count, lambda step: path_copy(step).start())
    all_paths[device] = path_row[...]

    quad = [(dy, da) for dy in range(2) for da in range(sides)]
    peers = quad[1:]

    def quad_side(da):
        return lax.rem(side + da, sides)

    def quad_copy(stage, source, target, dy, da):
        back_da = (sides - da) % sides
        return pltpu.make_async_remote_copy(
            src_ref=source,
            dst_ref=target.at[dy, back_da],
            send_sem=quad_send.at[stage, dy, da],
            recv_sem=quad_recv.at[stage, dy, back_da],
            device_id=(mirror if dy else group, at_line(0, quad_side(da), core)),
            device_id_type=MESH,
        )

    def quad_wait(stage, source, target, dy, da):
        quad_copy(stage, source, target, dy, (sides - da) % sides).wait_recv()

    def gather_copy(r, bit):
        piece = coarse_w.at[:, flip(r), core]
        return to_member(
            piece,
            piece,
            gather_send.at[r, bits.index(bit)],
            gather_recv.at[r ^ bit],
            at_line(bit, side, core),
        )

    def gather_wait(r):
        piece = coarse_w.at[:, flip(r), core]
        bit = r & -r
        to_member(
            piece, piece, gather_send.at[0, 0], gather_recv.at[r], at_line(bit, side, core)
        ).wait_recv()

    def gather_on(r):
        return [bit for bit in bits if r == 0 or bit < (r & -r)]

    def core_copy(r, step, landing_own):
        there = lax.rem(core + step, cores)
        landing = core if landing_own else lax.rem(core + cores - step, cores)
        piece = coarse_w.at[:, flip(r), landing]
        return to_member(
            piece, piece, core_send.at[0, r, step], core_recv.at[0, r, step], at_line(0, side, there)
        )

    def pass_on(r):
        for bit in gather_on(r):
            gather_copy(r, bit).start()
        for step in range(1, cores):
            core_copy(r, step, True).start()

    def doc_copy(dy, da):
        which = 1 - slot if dy else slot
        return quad_copy(0, both.at[which, :, quad_side(da)], docs, dy, da)

    pass_on(0)
    for load in token_loads:
        load.wait()
    for dy, da in peers:
        doc_copy(dy, da).start()
    for which in range(2):
        for index, (o, a) in enumerate(places):
            flipped[which, index * span : (index + 1) * span, :] = both[which, o, a].T
    docs[0, 0] = both[slot, :, side]
    for load in loads[1:]:
        load.wait()
    if outer > 1:
        gather_wait(1)
        pass_on(1)

    def turn(dy, da):
        q = dy * sides + da
        for o in range(outer):
            quad_t[o * span : (o + 1) * span, q * token_count : (q + 1) * token_count] = docs[
                dy, da, o
            ].T

    turn(0, 0)
    others = all_paths.at[pl.ds(0, count - 1)]
    pltpu.make_async_copy(others, others, path_recv).wait()
    scalars = pltpu.make_async_copy(all_paths, path, local_sem.at[0])
    scalars.start()
    scalars.wait()
    outs[0].start()

    def route(document, column):
        return path[document, 0, column]

    def member_copy(index, source, target, p, landing_own):
        landing = me if landing_own else p
        arrived = weight_recv.at[index] if index < 2 else mem_recv.at[index - 2, landing]
        return to_member(source.at[p], target.at[landing], mem_send.at[index], arrived, p)

    def all_of(ref, number, sem):
        some = ref.at[pl.ds(0, number)]
        return pltpu.make_async_copy(some, some, sem)

    near = outer * cores

    def partner(step):
        there = lax.rem(side + step // near, sides)
        rest = lax.rem(step, near)
        return (
            lax.rem(line + rest // cores, outer) * inner
            + there * cores
            + lax.rem(core + lax.rem(rest, cores), cores)
        )

    def spread(index, source, target, start=1, stop=members):
        loop(
            start,
            stop,
            lambda step: member_copy(index, source, target, partner(step), True).start(),
        )

    def arrive(index, target):
        if members > 1:
            all_of(target, members - 1, weight_recv.at[index]).wait()

    def left(index, source):
        if members > 1:
            all_of(source, members - 1, mem_send.at[index]).wait()

    def group_copy(index, source, target, step, landing_own):
        other = lax.rem(group + step, groups)
        landing = group if landing_own else other
        return pltpu.make_async_remote_copy(
            src_ref=source(other),
            dst_ref=target.at[landing],
            send_sem=grp_send.at[index, other],
            recv_sem=grp_recv.at[index, landing],
            device_id={"grp": other},
            device_id_type=MESH,
        )

    def group_spread(*what):
        loop(1, groups, lambda step: group_copy(*what, step, True).start())

    def group_arrive(*what):
        loop(1, groups, lambda step: group_copy(*what, step, False).wait_recv())

    def group_left(*what):
        loop(1, groups, lambda step: group_copy(*what, step, False).wait_send())

    def pick_fine(index):
        held = jnp.clip(route(index, 2) - group * owned, 0, owned - 1)
        fine_out[index // members, lax.rem(index, members)] = fine_w[held]

    def pick_middle(p):
        middle_send[p] = middle_w[route(group * members + p, 1)]

    loop(0, count, pick_fine)
    fine_trade = (0, lambda other: fine_out.at[other], fine_in)
    group_spread(*fine_trade)
    loop(0, members, pick_middle)
    spread(0, middle_send, middle_block)
    fine_in[group] = fine_out[group]
    middle_block[me] = middle_send[me]

    for r in range(2, outer, 2):
        gather_wait(r)
        pass_on(r)
    for dy, da in peers:
        quad_wait(0, both.at[0, :, 0], docs, dy, da)
        turn(dy, da)

    def merge_fine(p):
        owner = route(group * members + p, 2) // owned
        fine_send[p] = fine_in[owner, p]

    group_arrive(*fine_trade)
    loop(0, members, merge_fine)
    spread(1, fine_send, fine_block)
    fine_block[me] = fine_send[me]

    for r in range(3, outer, 2):
        gather_wait(r)
        pass_on(r)
    for r in range(outer):
        for step in range(1, cores):
            core_copy(r, step, False).wait_recv()

    def block_of(dy, da):
        who = (mirror if dy else group) * members + at_line(0, quad_side(da), core)
        return route(who, 0)

    def coarse_of(k):
        return coarse_w[k].reshape(depth, columns)

    def wide_of(dy, da):
        return jnp.concatenate([docs[dy, da, o] for o in range(outer)], axis=1)

    first = slot == 0
    for dy, da in peers:
        pre_give[dy, da] = dot(wide_of(dy, da), coarse_of(block_of(dy, da))).astype(BF16)
        quad_copy(1, pre_give.at[dy, da], pre_take, dy, da).start()
    pre_own = dot(wide_of(0, 0), coarse_of(block_of(0, 0)))
    pre_other = jnp.zeros_like(pre_own)

    def whole(which):
        return jnp.concatenate([both[which, o, a] for o, a in places], axis=1)

    def compute(block, term):
        weights = block[...].reshape(width, block.shape[-1])
        value, part = level(weights, whole(0), whole(1), flipped[0], flipped[1])
        term[...] = value.reshape(term.shape)
        return part

    middle_own = middle_parts.at[group]
    fine_own = fine_parts.at[group]

    for dy, da in peers:
        quad_wait(1, pre_give.at[0, 0], pre_take, dy, da)
    for dy, da in peers:
        if dy:
            pre_other = pre_other + pre_take[dy, da].astype(F32)
        else:
            pre_own = pre_own + pre_take[dy, da].astype(F32)
    hidden, before_grad = gelu_parts(
        jnp.where(first, pre_own, pre_other), jnp.where(first, pre_other, pre_own)
    )
    hidden, before_grad = hidden.astype(F32), before_grad.astype(F32)
    act_give[...] = jnp.where(first, hidden, before_grad).astype(BF16)
    act_keep[...] = jnp.where(first, before_grad, hidden).astype(BF16)
    act_take[0, 0] = act_keep[...]
    for dy, da in peers:
        quad_copy(2, act_give if dy else act_keep, act_take, dy, da).start()

    arrive(0, middle_block)
    total[...] = compute(middle_block, middle_term)
    spread(2, middle_term, middle_own)
    middle_parts[group, me] = middle_term[me]

    arrive(1, fine_block)
    total[...] += compute(fine_block, fine_term)
    spread(3, fine_term, fine_own)
    fine_parts[group, me] = fine_term[me]

    for dy, da in peers:
        quad_wait(2, act_keep, act_take, dy, da)

    for k in range(blocks):
        acts = [
            jnp.where(block_of(dy, da) == k, act_take[dy, da].astype(F32), 0.0).astype(BF16)
            for dy, da in quad
        ]
        value = dot(quad_t[...], jnp.concatenate(acts, axis=0))
        sums[:, :, k] = value.astype(BF16).reshape(outer, cores, rows, columns)

    order = list(range(outer - 1, 0, -2)) + list(range(outer - 2, 0, -2)) + [0]

    def fold_core(r, step):
        there = lax.rem(core + step, cores)
        return to_member(
            sums.at[flip(r), there],
            from_core.at[r, step],
            core_send.at[1, r, step],
            core_recv.at[1, r, step],
            at_line(0, side, there),
        )

    def fold_line(r, bit):
        return to_member(
            sums.at[flip(r), core],
            from_line.at[r ^ bit, bits.index(bit)],
            fold_send.at[r],
            fold_recv.at[r ^ bit, bits.index(bit)],
            at_line(bit, side, core),
        )

    def fold_line_wait(r, bit):
        to_member(
            sums.at[flip(r), core],
            from_line.at[r, bits.index(bit)],
            fold_send.at[r],
            fold_recv.at[r, bits.index(bit)],
            at_line(bit, side, core),
        ).wait_recv()

    def lower(r):
        return [bit for bit in reversed(bits) if r == 0 or bit < (r & -r)]

    for r in order:
        for step in range(1, cores):
            fold_core(r, step).start()

    def back_copy(dy, da):
        return quad_copy(3, back_give.at[dy, da], back_take, dy, da)

    @pl.when(first)
    def _():
        for dy, da in peers:
            back_give[dy, da] = dot_transposed(
                act_take[dy, da], coarse_of(block_of(dy, da))
            ).astype(BF16)
            back_copy(dy, da).start()

    def hand_on(target, send_on, recv_on, p, step, landing_own):
        other = lax.rem(group + step, groups)
        landing = group if landing_own else other
        return pltpu.make_async_remote_copy(
            src_ref=target.at[group, p],
            dst_ref=target.at[landing, p],
            send_sem=send_on,
            recv_sem=recv_on,
            device_id={"grp": other},
            device_id_type=MESH,
        )

    def relay(index, source, target, send_on, recv_on):
        own = target.at[group]

        def start(p):
            loop(1, groups, lambda step: hand_on(target, send_on, recv_on, p, step, True).start())

        def body(step):
            p = lax.rem(me + members - step, members)
            member_copy(index, source, own, p, False).wait_recv()
            start(p)

        start(me)
        loop(1, members, body)

    def relay_done(target, send_on, recv_on):
        if groups > 1:
            all_of(target, groups - 1, recv_on).wait()
            all_of(target, groups - 1, send_on).wait()

    def folded(r):
        value = sums[flip(r), core].astype(F32)
        for step in range(1, cores):
            value = value + from_core[r, step].astype(F32)
        for bit in lower(r):
            value = value + from_line[r, bits.index(bit)].astype(F32)
        return value

    for r in order:
        for step in range(1, cores):
            fold_core(r, step).wait_recv()
        for bit in lower(r):
            fold_line_wait(r, bit)
        if r:
            sums[flip(r), core] = folded(r).astype(BF16)
            fold_line(r, r & -r).start()
            if r == order[-2]:
                relay(2, middle_term, middle_parts, middle_send_on, middle_recv_on)
                relay(3, fine_term, fine_parts, fine_send_on, fine_recv_on)
        else:
            coarse_total[...] = folded(0).astype(BF16)

    coarse_trade = (1, lambda other: coarse_total, coarse_parts)
    group_spread(*coarse_trade)
    coarse_parts[group] = coarse_total[...]

    def add_back(dy, da, piece):
        for o in range(outer):
            columns_of = pl.ds(pl.multiple_of((o * sides + quad_side(da)) * span, span), span)
            total[:, columns_of] += piece[:, o * span : (o + 1) * span]

    @pl.when(first)
    def _():
        add_back(0, 0, dot_transposed(act_take[0, 0], coarse_of(block_of(0, 0))))
        for dy, da in peers:
            if dy == 0:
                quad_wait(3, back_give.at[0, 0], back_take, dy, da)
                add_back(dy, da, back_take[dy, da].astype(F32))
        for dy, da in peers:
            back_copy(dy, da).wait_send()

    @pl.when(slot == 1)
    def _():
        for dy, da in peers:
            if dy:
                quad_wait(3, back_give.at[0, 0], back_take, dy, da)
                add_back(dy, da, back_take[dy, da].astype(F32))

    tokens_grad[...] = total[...].astype(BF16)
    outs[1].start()
    pltpu.make_async_copy(others, others, path_send).wait()
    for dy, da in peers:
        doc_copy(dy, da).wait_send()
        quad_copy(1, pre_give.at[dy, da], pre_take, dy, da).wait_send()
        quad_copy(2, act_give if dy else act_keep, act_take, dy, da).wait_send()
    for r in range(outer):
        for bit in gather_on(r):
            gather_copy(r, bit).wait_send()
        for step in range(1, cores):
            core_copy(r, step, True).wait_send()
            fold_core(r, step).wait_send()
        if r:
            fold_line(r, r & -r).wait_send()
    left(0, middle_send)
    left(1, fine_send)
    group_left(*fine_trade)
    left(2, middle_term)
    left(3, fine_term)
    relay_done(middle_parts, middle_send_on, middle_recv_on)
    outs[2].start()
    relay_done(fine_parts, fine_send_on, fine_recv_on)
    outs[3].start()
    group_arrive(*coarse_trade)
    outs[4].start()
    group_left(*coarse_trade)
    for out in outs:
        out.wait()


def exchange(path, tokens, cotangent, coarse_w, middle_w, fine_w, groups, members):
    blocks, rows, wide = coarse_w.shape
    medium, narrow = middle_w.shape[2], fine_w.shape[2]
    token_count, width = tokens.shape
    count = groups * members
    outer, sides, cores = plan(members, rows)
    span = cores * rows
    depth = outer * span
    steps = max(len(bits_of(outer)), 1)
    columns = wide // 2

    def stack(*shape):
        return pltpu.VMEM(shape, BF16)

    def sems(*shape):
        return pltpu.SemaphoreType.DMA(shape)

    vmem = pl.BlockSpec(memory_space=pltpu.VMEM)
    return pl.pallas_call(
        functools.partial(main_kernel, groups, members),
        out_shape=(
            jax.ShapeDtypeStruct((count,) + path.shape, jnp.int32),
            jax.ShapeDtypeStruct(tokens.shape, BF16),
            jax.ShapeDtypeStruct((groups, members, rows, medium), BF16),
            jax.ShapeDtypeStruct((groups, members, rows, narrow), BF16),
            jax.ShapeDtypeStruct((groups, blocks, rows, columns), BF16),
        ),
        in_specs=[vmem] + [pl.BlockSpec(memory_space=pl.ANY)] * 5,
        out_specs=(pl.BlockSpec(memory_space=pl.ANY),) * 5,
        scratch_shapes=[
            pltpu.VMEM((count,) + path.shape, jnp.int32),
            stack(*tokens.shape),
            stack(groups, members, rows, medium),
            stack(groups, members, rows, narrow),
            stack(groups, blocks, rows, columns),
            pltpu.SMEM((count,) + path.shape, jnp.int32),
            stack(2, outer, sides, token_count, span),
            stack(2, sides, outer, token_count, span),
            stack(blocks, outer, cores, rows, columns),
            stack(*middle_w.shape),
            stack(*fine_w.shape),
            stack(members, rows, medium),
            stack(groups, members, rows, narrow),
            stack(groups, members, rows, narrow),
            stack(members, rows, narrow),
            stack(members, rows, medium),
            stack(members, rows, narrow),
            stack(members, rows, medium),
            stack(members, rows, narrow),
            stack(outer, cores, blocks, rows, columns),
            stack(outer, cores, blocks, rows, columns),
            stack(outer, steps, blocks, rows, columns),
            stack(blocks, rows, columns),
            stack(2, width, token_count),
            stack(depth, 2 * sides * token_count),
            pltpu.VMEM((token_count, width), F32),
            stack(2, sides, token_count, columns),
            stack(2, sides, token_count, columns),
            stack(token_count, columns),
            stack(token_count, columns),
            stack(2, sides, token_count, columns),
            stack(2, sides, token_count, depth),
            stack(2, sides, token_count, depth),
            pltpu.SemaphoreType.DMA,
            pltpu.SemaphoreType.DMA,
            sems(4),
            sems(2, members),
            sems(2),
            sems(2, groups),
            sems(2, groups),
            sems(4, 2, sides),
            sems(4, 2, sides),
            sems(outer, steps),
            sems(outer),
            sems(2, outer, cores),
            sems(2, outer, cores),
            sems(outer),
            sems(outer, steps),
            sems(1),
            sems(3),
            sems(2, outer * sides),
            sems(5),
            pltpu.SemaphoreType.DMA,
            pltpu.SemaphoreType.DMA,
            pltpu.SemaphoreType.DMA,
            pltpu.SemaphoreType.DMA,
        ],
        compiler_params=pltpu.CompilerParams(
            collective_id=0, has_side_effects=True, vmem_limit_bytes=60 * 2**20
        ),
        name="exchange",
    )(path, tokens, cotangent, coarse_w, middle_w, fine_w)


def collect_kernel(
    path,
    first_owned,
    tokens_in,
    middle_hbm,
    fine_hbm,
    coarse_parts,
    tokens_grad,
    coarse_grad,
    middle_grad,
    fine_grad,
    middle_parts,
    fine_parts,
    middle_sum,
    fine_sum,
    middle_last,
    fine_last,
    load_sem,
):
    count = middle_parts.shape[0]
    owned = fine_grad.shape[0]
    loads = (
        pltpu.make_async_copy(middle_hbm, middle_parts, load_sem.at[0]),
        pltpu.make_async_copy(fine_hbm, fine_parts, load_sem.at[1]),
    )
    for load in loads:
        load.start()
    middle_grad[...] = jnp.zeros_like(middle_grad)
    fine_grad[...] = jnp.zeros_like(fine_grad)
    middle_sum[count] = jnp.zeros(middle_sum.shape[1:], F32)
    fine_sum[count] = jnp.zeros(fine_sum.shape[1:], F32)
    for last in (middle_last, fine_last):

        def clear(k, carry, last=last):
            last[k] = count
            return carry

        lax.fori_loop(0, last.shape[0], clear, 0)
    tokens_grad[...] = tokens_in[...]
    groups, _, _, columns = coarse_parts.shape
    team = coarse_grad.shape[2] // columns
    for s in range(team):
        value = coarse_parts[s].astype(F32)
        for other in range(s + team, groups, team):
            value = value + coarse_parts[other].astype(F32)
        coarse_grad[:, :, s * columns : (s + 1) * columns] = value.astype(BF16)
    for load in loads:
        load.wait()

    def add(document, carry):
        k = path[document, 0, 1]
        value = middle_parts[document].astype(F32) + middle_sum[middle_last[k]]
        middle_sum[document] = value
        middle_grad[k] = value.astype(BF16)
        middle_last[k] = document
        place = path[document, 0, 2] - first_owned[0]

        @pl.when((place >= 0) & (place < owned))
        def _():
            piece = fine_parts[document].astype(F32) + fine_sum[fine_last[place]]
            fine_sum[document] = piece
            fine_grad[place] = piece.astype(BF16)
            fine_last[place] = document

        return carry

    lax.fori_loop(0, count, add, 0)


def collect(paths, first_owned, tokens_grad, middle_parts, fine_parts, coarse_parts, shapes):
    vmem = pl.BlockSpec(memory_space=pltpu.VMEM)
    smem = pl.BlockSpec(memory_space=pltpu.SMEM)
    hbm = pl.BlockSpec(memory_space=pl.ANY)
    count, rows, medium = middle_parts.shape
    narrow = fine_parts.shape[2]
    return pl.pallas_call(
        collect_kernel,
        out_shape=tuple(
            jax.ShapeDtypeStruct(shape, BF16) for shape in (tokens_grad.shape,) + shapes
        ),
        in_specs=[smem, smem, vmem, hbm, hbm, vmem],
        out_specs=(vmem,) * 4,
        scratch_shapes=[
            pltpu.VMEM(middle_parts.shape, BF16),
            pltpu.VMEM(fine_parts.shape, BF16),
            pltpu.VMEM((count + 1, rows, medium), F32),
            pltpu.VMEM((count + 1, rows, narrow), F32),
            pltpu.SMEM((shapes[1][0],), jnp.int32),
            pltpu.SMEM((shapes[2][0],), jnp.int32),
            pltpu.SemaphoreType.DMA((2,)),
        ],
        compiler_params=pltpu.CompilerParams(vmem_limit_bytes=60 * 2**20),
        name="collect",
    )(paths, first_owned, tokens_grad, middle_parts, fine_parts, coarse_parts)


def on_device(tokens, cotangent, path, coarse_weights, middle_weights, fine_weights):
    members = lax.axis_size("mem")
    groups = lax.axis_size("grp")
    paths, tokens_grad, middle_parts, fine_parts, coarse_parts = exchange(
        path, tokens, cotangent, coarse_weights, middle_weights, fine_weights, groups, members
    )
    first_owned = (lax.axis_index("grp") * fine_weights.shape[0]).astype(jnp.int32).reshape(1)
    flat = lambda parts: parts.reshape((groups * members,) + parts.shape[2:])
    return collect(
        paths,
        first_owned,
        tokens_grad,
        flat(middle_parts),
        flat(fine_parts),
        coarse_parts,
        (coarse_weights.shape, middle_weights.shape, fine_weights.shape),
    )


def solution(mesh):
    return jax.shard_map(
        on_device,
        mesh=mesh,
        in_specs=(
            P(("grp", "mem"), None),
            P(("grp", "mem"), None),
            P(("grp", "mem"), None),
            P(None, "mem", None),
            P(None, "mem", None),
            P("grp", "mem", None),
        ),
        out_specs=(
            P(("grp", "mem"), None),
            P(None, "mem", None),
            P(None, "mem", None),
            P("grp", "mem", None),
        ),
        check_vma=False,
    )
```

```python
import functools
import math

import jax
import jax.numpy as jnp
from jax import lax
from jax.experimental import pallas as pl
from jax.experimental.pallas import tpu as pltpu
from jax.sharding import PartitionSpec as P

MESH = pl.DeviceIdType.MESH
LANES = 128
F32 = jnp.float32
BF16 = jnp.bfloat16


def gelu_parts(before, hidden_grad):
    scale = math.sqrt(2.0 / math.pi)
    square = before * before
    tanh = jnp.tanh(scale * (before + 0.044715 * (square * before)))
    half = 0.5 * (1.0 + tanh)
    hidden = before * half
    slope = half + 0.5 * before * (1.0 - tanh * tanh) * (scale * (1.0 + 3 * 0.044715 * square))
    return hidden.astype(BF16), (hidden_grad * slope).astype(BF16)


def dot(left, right):
    return jnp.dot(left, right, preferred_element_type=F32)


def dot_transposed(left, right):
    return lax.dot_general(left, right, (((1,), (1,)), ((), ())), preferred_element_type=F32)


def level(weights, x, g, xt, gt):
    width = weights.shape[1]
    half = width // 2
    if half % LANES == 0:
        up = weights[:, :half]
        down = weights[:, half:]
        hidden, grad = gelu_parts(dot(x, up), dot(g, down))
        term = jnp.concatenate(
            [dot(xt, grad).astype(BF16), dot(gt, hidden).astype(BF16)], axis=1
        )
        return term, dot_transposed(grad, up)
    before = dot(x, weights)
    hidden_grad = pltpu.roll(dot(g, weights), half, 1)
    hidden, grad = gelu_parts(before, hidden_grad)
    first = lax.broadcasted_iota(jnp.int32, grad.shape, 1) < half
    grad = jnp.where(first, grad.astype(F32), 0.0).astype(BF16)
    hidden = jnp.where(first, hidden.astype(F32), 0.0)
    hidden = pltpu.roll(hidden, half, 1).astype(BF16)
    term = (dot(xt, grad) + dot(gt, hidden)).astype(BF16)
    return term, dot_transposed(grad, weights)


def plan(groups, members, blocks_width):
    inner = max(k for k in range(1, math.isqrt(members) + 1) if members % k == 0)
    cores = 2 if inner % 2 == 0 else 1
    return members // inner, inner // cores, cores


def bits_of(outer):
    bits = []
    while outer > 1:
        outer //= 2
        bits.append(outer)
    return bits


def main_kernel(
    groups,
    members,
    path_row,
    tokens_hbm,
    cotangent_hbm,
    coarse_hbm,
    middle_hbm,
    fine_hbm,
    paths_out,
    tokens_out,
    middle_out,
    fine_parts_out,
    coarse_out,
    all_paths,
    tokens_grad,
    middle_parts,
    fine_parts,
    coarse_parts,
    path,
    both,
    other_doc,
    coarse_w,
    middle_w,
    fine_w,
    middle_send,
    fine_out,
    fine_in,
    fine_send,
    middle_block,
    fine_block,
    middle_term,
    fine_term,
    sums,
    from_core,
    from_side,
    from_line,
    coarse_total,
    flipped,
    pair_t,
    total,
    pre_give,
    pre_take,
    act_give,
    act_take,
    back_give,
    back_take,
    path_send,
    path_recv,
    mem_send,
    mem_recv,
    weight_recv,
    grp_send,
    grp_recv,
    pair_send,
    pair_recv,
    gather_send,
    gather_recv,
    side_send,
    side_recv,
    core_send,
    core_recv,
    fold_send,
    fold_recv,
    local_sem,
    load_sem,
    out_sem,
    middle_send_on,
    middle_recv_on,
    fine_send_on,
    fine_recv_on,
):
    group = lax.axis_index("grp")
    me = lax.axis_index("mem")
    count = groups * members
    device = group * members + me
    owned = fine_w.shape[0]
    blocks, outer, sides, cores, rows, columns = coarse_w.shape
    inner = sides * cores
    bits = bits_of(outer)
    line = me // inner
    place = lax.rem(me, inner)
    side = place // cores
    core = lax.rem(place, cores)
    slot = lax.rem(group, 2)
    mirror = group + 1 - 2 * slot
    token_count, width = tokens_grad.shape

    def loop(start, stop, body):
        def wrapped(step, carry):
            body(step)
            return carry

        lax.fori_loop(start, stop, wrapped, 0)

    def flip(r):
        there = line
        for bit in bits:
            if r & bit:
                there = there + bit * (1 - 2 * lax.rem(there // bit, 2))
        return there

    def at_line(r, s, c):
        return flip(r) * inner + s * cores + c

    def to_member(source, target, send, recv, p):
        return pltpu.make_async_remote_copy(
            src_ref=source,
            dst_ref=target,
            send_sem=send,
            recv_sem=recv,
            device_id={"mem": p},
            device_id_type=MESH,
        )

    half = pl.ds(pl.multiple_of(slot * columns, LANES), columns)
    loads = [
        pltpu.make_async_copy(source, target, load_sem.at[index])
        for index, (source, target) in enumerate(
            (
                (coarse_hbm.at[:, :, half], coarse_w.at[:, line, side, core]),
                (tokens_hbm, both.at[0]),
                (cotangent_hbm, both.at[1]),
                (fine_hbm, fine_w),
                (middle_hbm, middle_w),
            )
        )
    ]
    for load in loads:
        load.start()
    outs = [
        pltpu.make_async_copy(source, target, out_sem.at[index])
        for index, (source, target) in enumerate(
            (
                (all_paths, paths_out),
                (tokens_grad, tokens_out),
                (middle_parts, middle_out),
                (fine_parts, fine_parts_out),
                (coarse_parts, coarse_out),
            )
        )
    ]
    barrier = pltpu.get_barrier_semaphore()

    def anyone(step):
        other = lax.rem(device + step, count)
        return other, (other // members, lax.rem(other, members))

    def greet(step):
        _, where = anyone(step)
        pl.semaphore_signal(barrier, inc=1, device_id=where, device_id_type=MESH)

    loop(1, count, greet)
    loads[0].wait()
    pl.semaphore_wait(barrier, count - 1)

    def path_copy(step):
        _, where = anyone(step)
        return pltpu.make_async_remote_copy(
            src_ref=path_row,
            dst_ref=all_paths.at[device],
            send_sem=path_send,
            recv_sem=path_recv,
            device_id=where,
            device_id_type=MESH,
        )

    loop(1, count, lambda step: path_copy(step).start())
    all_paths[device] = path_row[...]

    def pair_copy(index, source, target):
        return pltpu.make_async_remote_copy(
            src_ref=source,
            dst_ref=target,
            send_sem=pair_send.at[index],
            recv_sem=pair_recv.at[index],
            device_id={"grp": mirror},
            device_id_type=MESH,
        )

    def gather_copy(r, bit):
        piece = coarse_w.at[:, flip(r), side, core]
        return to_member(
            piece,
            piece,
            gather_send.at[r, bits.index(bit)],
            gather_recv.at[r ^ bit],
            at_line(bit, side, core),
        )

    def gather_wait(r):
        piece = coarse_w.at[:, flip(r), side, core]
        bit = r & -r
        to_member(
            piece, piece, gather_send.at[0, 0], gather_recv.at[r], at_line(bit, side, core)
        ).wait_recv()

    def gather_on(r):
        return [bit for bit in bits if r == 0 or bit < (r & -r)]

    def side_copy(r, step, landing_own):
        there = lax.rem(side + step, sides)
        landing = side if landing_own else lax.rem(side + sides - step, sides)
        piece = coarse_w.at[:, flip(r), landing, core]
        return to_member(
            piece, piece, side_send.at[0, r, step], side_recv.at[0, r, step], at_line(0, there, core)
        )

    def core_copy(r, landing_own):
        piece = coarse_w.at[:, flip(r), :, core if landing_own else 1 - core]
        return to_member(
            piece, piece, core_send.at[0, r], core_recv.at[0, r], at_line(0, side, 1 - core)
        )

    tokens_pair = pair_copy(0, both.at[1 - slot], other_doc)

    def pass_on(r):
        for bit in gather_on(r):
            gather_copy(r, bit).start()
        for step in range(1, sides):
            side_copy(r, step, True).start()

    def share(r):
        for step in range(1, sides):
            side_copy(r, step, False).wait_recv()
        if cores > 1:
            core_copy(r, True).start()

    pass_on(0)
    for load in loads[1:3]:
        load.wait()
    tokens_pair.start()
    for which in range(2):
        for start in range(0, width, LANES):
            part = slice(start, start + LANES)
            flipped[which, part, :] = both[which, :, part].T
    for load in loads[3:]:
        load.wait()
    pair_t[:, :token_count] = flipped[slot]
    if outer > 1:
        gather_wait(1)
        pass_on(1)
    share(0)

    others = all_paths.at[pl.ds(0, count - 1)]
    pltpu.make_async_copy(others, others, path_recv).wait()
    scalars = pltpu.make_async_copy(all_paths, path, local_sem.at[0])
    scalars.start()
    scalars.wait()
    outs[0].start()

    def route(document, column):
        return path[document, 0, column]

    def member_copy(index, source, target, p, landing_own):
        landing = me if landing_own else p
        arrived = weight_recv.at[index] if index < 2 else mem_recv.at[index - 2, landing]
        return to_member(source.at[p], target.at[landing], mem_send.at[index], arrived, p)

    def all_of(ref, number, sem):
        some = ref.at[pl.ds(0, number)]
        return pltpu.make_async_copy(some, some, sem)

    near = outer * cores

    def partner(step):
        there = lax.rem(side + step // near, sides)
        rest = lax.rem(step, near)
        return (
            lax.rem(line + rest // cores, outer) * inner
            + there * cores
            + lax.rem(core + lax.rem(rest, cores), cores)
        )

    def spread(index, source, target, start=1, stop=members):
        loop(
            start,
            stop,
            lambda step: member_copy(index, source, target, partner(step), True).start(),
        )

    def arrive(index, target):
        if members > 1:
            all_of(target, members - 1, weight_recv.at[index]).wait()

    def left(index, source):
        if members > 1:
            all_of(source, members - 1, mem_send.at[index]).wait()

    def group_copy(index, source, target, step, landing_own):
        other = lax.rem(group + step, groups)
        landing = group if landing_own else other
        return pltpu.make_async_remote_copy(
            src_ref=source(other),
            dst_ref=target.at[landing],
            send_sem=grp_send.at[index, other],
            recv_sem=grp_recv.at[index, landing],
            device_id={"grp": other},
            device_id_type=MESH,
        )

    def group_spread(*what):
        loop(1, groups, lambda step: group_copy(*what, step, True).start())

    def group_arrive(*what):
        loop(1, groups, lambda step: group_copy(*what, step, False).wait_recv())

    def group_left(*what):
        loop(1, groups, lambda step: group_copy(*what, step, False).wait_send())

    def pick_fine(index):
        held = jnp.clip(route(index, 2) - group * owned, 0, owned - 1)
        fine_out[index // members, lax.rem(index, members)] = fine_w[held]

    def pick_middle(p):
        middle_send[p] = middle_w[route(group * members + p, 1)]

    loop(0, count, pick_fine)
    fine_trade = (0, lambda other: fine_out.at[other], fine_in)
    group_spread(*fine_trade)
    loop(0, members, pick_middle)
    spread(0, middle_send, middle_block, 1, near)
    fine_in[group] = fine_out[group]
    middle_block[me] = middle_send[me]

    for r in range(2, outer, 2):
        gather_wait(r)
        pass_on(r)
    if outer > 1:
        share(1)
    for r in range(3, outer, 2):
        gather_wait(r)
        pass_on(r)
    spread(0, middle_send, middle_block, near, members)
    tokens_pair.wait_recv()
    for start in range(0, width, LANES):
        pair_t[start : start + LANES, token_count:] = other_doc[:, start : start + LANES].T
    for r in range(2, outer, 2):
        share(r)

    def merge_fine(p):
        owner = route(group * members + p, 2) // owned
        fine_send[p] = fine_in[owner, p]

    group_arrive(*fine_trade)
    loop(0, members, merge_fine)
    spread(1, fine_send, fine_block)
    fine_block[me] = fine_send[me]

    for r in range(3, outer, 2):
        share(r)
    if cores > 1:
        for r in range(outer):
            core_copy(r, False).wait_recv()

    own_block = route(device, 0)
    other_block = route(mirror * members + me, 0)

    def coarse_of(k):
        return coarse_w[k].reshape(width, columns)

    first = slot == 0
    pre_give[...] = dot(other_doc[...], coarse_of(other_block)).astype(BF16)
    pre_pair = pair_copy(1, pre_give, pre_take)
    pre_pair.start()
    pre_own = dot(both[slot], coarse_of(own_block))

    def compute(block, term):
        weights = block[...].reshape(width, block.shape[-1])
        value, part = level(weights, both[0], both[1], flipped[0], flipped[1])
        term[...] = value.reshape(term.shape)
        return part

    middle_own = middle_parts.at[group]
    fine_own = fine_parts.at[group]

    arrive(0, middle_block)
    total[...] = compute(middle_block, middle_term)
    spread(2, middle_term, middle_own)
    middle_parts[group, me] = middle_term[me]

    pre_pair.wait_recv()
    pre_other = pre_take[...].astype(F32)
    hidden, before_grad = gelu_parts(
        jnp.where(first, pre_own, pre_other), jnp.where(first, pre_other, pre_own)
    )
    hidden, before_grad = hidden.astype(F32), before_grad.astype(F32)
    act_give[...] = jnp.where(first, hidden, before_grad).astype(BF16)
    act_own = jnp.where(first, before_grad, hidden).astype(BF16)
    act_pair = pair_copy(2, act_give, act_take)
    act_pair.start()

    @pl.when(first)
    def _():
        total[...] += dot_transposed(act_own, coarse_of(own_block))

    arrive(1, fine_block)
    total[...] += compute(fine_block, fine_term)
    spread(3, fine_term, fine_own)
    fine_parts[group, me] = fine_term[me]

    act_pair.wait_recv()
    act_other = act_take[...]
    back = pair_copy(3, back_give, back_take)

    for k in range(blocks):
        mine = jnp.where(own_block == k, act_own.astype(F32), 0.0).astype(BF16)
        theirs = jnp.where(other_block == k, act_other.astype(F32), 0.0).astype(BF16)
        value = dot(pair_t[...], jnp.concatenate([mine, theirs], axis=0))
        sums[:, :, :, k] = value.astype(BF16).reshape(outer, sides, cores, rows, columns)

    order = list(range(outer - 1, -1, -1))

    def fold_core(r):
        return to_member(
            sums.at[flip(r), :, 1 - core],
            from_core.at[r],
            core_send.at[1, r],
            core_recv.at[1, r],
            at_line(0, side, 1 - core),
        )

    def fold_side(r, step):
        there = lax.rem(side + step, sides)
        return to_member(
            sums.at[flip(r), there, core],
            from_side.at[r, step],
            side_send.at[1, r, step],
            side_recv.at[1, r, step],
            at_line(0, there, core),
        )

    def fold_line(r, bit):
        return to_member(
            sums.at[flip(r), side, core],
            from_line.at[r ^ bit, bits.index(bit)],
            fold_send.at[r],
            fold_recv.at[r ^ bit, bits.index(bit)],
            at_line(bit, side, core),
        )

    def fold_line_wait(r, bit):
        to_member(
            sums.at[flip(r), side, core],
            from_line.at[r, bits.index(bit)],
            fold_send.at[r],
            fold_recv.at[r, bits.index(bit)],
            at_line(bit, side, core),
        ).wait_recv()

    def lower(r):
        return [bit for bit in reversed(bits) if r == 0 or bit < (r & -r)]

    if cores > 1:
        for r in order:
            fold_core(r).start()

    @pl.when(first)
    def _():
        back_give[...] = dot_transposed(act_other, coarse_of(other_block)).astype(BF16)
        back.start()

    for r in order:
        if cores > 1:
            fold_core(r).wait_recv()
            for step in range(1, sides):
                there = lax.rem(side + step, sides)
                sums[flip(r), there, core] = (
                    sums[flip(r), there, core].astype(F32) + from_core[r, there].astype(F32)
                ).astype(BF16)
        for step in range(1, sides):
            fold_side(r, step).start()

    def hand_on(target, send_on, recv_on, p, step, landing_own):
        other = lax.rem(group + step, groups)
        landing = group if landing_own else other
        return pltpu.make_async_remote_copy(
            src_ref=target.at[group, p],
            dst_ref=target.at[landing, p],
            send_sem=send_on,
            recv_sem=recv_on,
            device_id={"grp": other},
            device_id_type=MESH,
        )

    def relay(index, source, target, send_on, recv_on):
        own = target.at[group]

        def start(p):
            loop(1, groups, lambda step: hand_on(target, send_on, recv_on, p, step, True).start())

        def body(step):
            p = lax.rem(me + members - step, members)
            member_copy(index, source, own, p, False).wait_recv()
            start(p)

        start(me)
        loop(1, members, body)

    def relay_done(target, send_on, recv_on):
        if groups > 1:
            all_of(target, groups - 1, recv_on).wait()
            all_of(target, groups - 1, send_on).wait()

    relay(2, middle_term, middle_parts, middle_send_on, middle_recv_on)

    def folded(r):
        value = sums[flip(r), side, core].astype(F32)
        if cores > 1:
            value = value + from_core[r, side].astype(F32)
        for step in range(1, sides):
            value = value + from_side[r, step].astype(F32)
        for bit in lower(r):
            value = value + from_line[r, bits.index(bit)].astype(F32)
        return value

    for r in order:
        for step in range(1, sides):
            fold_side(r, step).wait_recv()
        for bit in lower(r):
            fold_line_wait(r, bit)
        if r:
            sums[flip(r), side, core] = folded(r).astype(BF16)
            fold_line(r, r & -r).start()
            if r == order[-2]:
                relay(3, fine_term, fine_parts, fine_send_on, fine_recv_on)
        else:
            coarse_total[...] = folded(0).astype(BF16)

    coarse_trade = (1, lambda other: coarse_total, coarse_parts)
    group_spread(*coarse_trade)
    coarse_parts[group] = coarse_total[...]

    @pl.when(first)
    def _():
        tokens_grad[...] = total[...].astype(BF16)
        back.wait_send()

    @pl.when(slot == 1)
    def _():
        back.wait_recv()
        tokens_grad[...] = (total[...] + back_take[...].astype(F32)).astype(BF16)

    outs[1].start()
    pltpu.make_async_copy(others, others, path_send).wait()
    for copy in (tokens_pair, pre_pair, act_pair):
        copy.wait_send()
    for r in range(outer):
        for bit in gather_on(r):
            gather_copy(r, bit).wait_send()
        for step in range(1, sides):
            side_copy(r, step, True).wait_send()
            fold_side(r, step).wait_send()
        if cores > 1:
            core_copy(r, True).wait_send()
            fold_core(r).wait_send()
        if r:
            fold_line(r, r & -r).wait_send()
    left(0, middle_send)
    left(1, fine_send)
    group_left(*fine_trade)
    left(2, middle_term)
    left(3, fine_term)
    relay_done(middle_parts, middle_send_on, middle_recv_on)
    outs[2].start()
    relay_done(fine_parts, fine_send_on, fine_recv_on)
    outs[3].start()
    group_arrive(*coarse_trade)
    outs[4].start()
    group_left(*coarse_trade)
    for out in outs:
        out.wait()


def exchange(path, tokens, cotangent, coarse_w, middle_w, fine_w, groups, members):
    blocks, rows, wide = coarse_w.shape
    medium, narrow = middle_w.shape[2], fine_w.shape[2]
    token_count, width = tokens.shape
    count = groups * members
    outer, sides, cores = plan(groups, members, wide)
    steps = max(len(bits_of(outer)), 1)
    columns = wide // 2

    def stack(*shape):
        return pltpu.VMEM(shape, BF16)

    def sems(*shape):
        return pltpu.SemaphoreType.DMA(shape)

    vmem = pl.BlockSpec(memory_space=pltpu.VMEM)
    return pl.pallas_call(
        functools.partial(main_kernel, groups, members),
        out_shape=(
            jax.ShapeDtypeStruct((count,) + path.shape, jnp.int32),
            jax.ShapeDtypeStruct(tokens.shape, BF16),
            jax.ShapeDtypeStruct((groups, members, rows, medium), BF16),
            jax.ShapeDtypeStruct((groups, members, rows, narrow), BF16),
            jax.ShapeDtypeStruct((groups, blocks, rows, columns), BF16),
        ),
        in_specs=[vmem] + [pl.BlockSpec(memory_space=pl.ANY)] * 5,
        out_specs=(pl.BlockSpec(memory_space=pl.ANY),) * 5,
        scratch_shapes=[
            pltpu.VMEM((count,) + path.shape, jnp.int32),
            stack(*tokens.shape),
            stack(groups, members, rows, medium),
            stack(groups, members, rows, narrow),
            stack(groups, blocks, rows, columns),
            pltpu.SMEM((count,) + path.shape, jnp.int32),
            stack(2, *tokens.shape),
            stack(*tokens.shape),
            stack(blocks, outer, sides, cores, rows, columns),
            stack(*middle_w.shape),
            stack(*fine_w.shape),
            stack(members, rows, medium),
            stack(groups, members, rows, narrow),
            stack(groups, members, rows, narrow),
            stack(members, rows, narrow),
            stack(members, rows, medium),
            stack(members, rows, narrow),
            stack(members, rows, medium),
            stack(members, rows, narrow),
            stack(outer, sides, cores, blocks, rows, columns),
            stack(outer, sides, blocks, rows, columns),
            stack(outer, sides, blocks, rows, columns),
            stack(outer, steps, blocks, rows, columns),
            stack(blocks, rows, columns),
            stack(2, width, token_count),
            stack(width, 2 * token_count),
            pltpu.VMEM((token_count, width), F32),
            stack(token_count, columns),
            stack(token_count, columns),
            stack(token_count, columns),
            stack(token_count, columns),
            stack(token_count, width),
            stack(token_count, width),
            pltpu.SemaphoreType.DMA,
            pltpu.SemaphoreType.DMA,
            sems(4),
            sems(2, members),
            sems(2),
            sems(2, groups),
            sems(2, groups),
            sems(4),
            sems(4),
            sems(outer, steps),
            sems(outer),
            sems(2, outer, sides),
            sems(2, outer, sides),
            sems(2, outer),
            sems(2, outer),
            sems(outer),
            sems(outer, steps),
            sems(1),
            sems(5),
            sems(5),
            pltpu.SemaphoreType.DMA,
            pltpu.SemaphoreType.DMA,
            pltpu.SemaphoreType.DMA,
            pltpu.SemaphoreType.DMA,
        ],
        compiler_params=pltpu.CompilerParams(
            collective_id=0, has_side_effects=True, vmem_limit_bytes=60 * 2**20
        ),
        name="exchange",
    )(path, tokens, cotangent, coarse_w, middle_w, fine_w)


def collect_kernel(
    path_hbm,
    tokens_hbm,
    middle_hbm,
    fine_hbm,
    coarse_hbm,
    tokens_out,
    coarse_out,
    middle_out,
    fine_out,
    path,
    tokens_grad,
    coarse_grad,
    middle_grad,
    fine_grad,
    coarse_parts,
    middle_parts,
    fine_parts,
    middle_sum,
    fine_sum,
    middle_last,
    fine_last,
    load_sem,
    out_sem,
):
    count = middle_parts.shape[0]
    owned = fine_grad.shape[0]
    first_owned = lax.axis_index("grp") * owned
    loads = [
        pltpu.make_async_copy(source, target, load_sem.at[index])
        for index, (source, target) in enumerate(
            (
                (path_hbm, path),
                (middle_hbm, middle_parts),
                (fine_hbm, fine_parts),
                (coarse_hbm, coarse_parts),
                (tokens_hbm, tokens_grad),
            )
        )
    ]
    outs = [
        pltpu.make_async_copy(source, target, out_sem.at[index])
        for index, (source, target) in enumerate(
            (
                (tokens_grad, tokens_out),
                (coarse_grad, coarse_out),
                (middle_grad, middle_out),
                (fine_grad, fine_out),
            )
        )
    ]
    for load in loads:
        load.start()
    for last in (middle_last, fine_last):
        for k in range(last.shape[0]):
            last[k] = count
    middle_grad[...] = jnp.zeros_like(middle_grad)
    middle_sum[count] = jnp.zeros(middle_sum.shape[1:], F32)
    fine_sum[count] = jnp.zeros(fine_sum.shape[1:], F32)
    loads[0].wait()
    loads[1].wait()

    def add_middle(document, carry):
        k = path[document, 0, 1]
        value = middle_parts[document].astype(F32) + middle_sum[middle_last[k]]
        middle_sum[document] = value
        middle_grad[k] = value.astype(BF16)
        middle_last[k] = document
        return carry

    lax.fori_loop(0, count, add_middle, 0)
    outs[2].start()
    fine_grad[...] = jnp.zeros_like(fine_grad)
    loads[2].wait()

    def add_fine(document, carry):
        place = path[document, 0, 2] - first_owned

        @pl.when((place >= 0) & (place < owned))
        def _():
            piece = fine_parts[document].astype(F32) + fine_sum[fine_last[place]]
            fine_sum[document] = piece
            fine_grad[place] = piece.astype(BF16)
            fine_last[place] = document

        return carry

    lax.fori_loop(0, count, add_fine, 0)
    outs[3].start()
    loads[3].wait()
    groups, _, _, columns = coarse_parts.shape
    team = coarse_grad.shape[2] // columns
    for s in range(team):
        value = coarse_parts[s].astype(F32)
        for other in range(s + team, groups, team):
            value = value + coarse_parts[other].astype(F32)
        coarse_grad[:, :, s * columns : (s + 1) * columns] = value.astype(BF16)
    outs[1].start()
    loads[4].wait()
    outs[0].start()
    for out in outs:
        out.wait()


def collect(paths, tokens_grad, middle_parts, fine_parts, coarse_parts, shapes):
    hbm = pl.BlockSpec(memory_space=pl.ANY)
    count, rows, medium = middle_parts.shape
    narrow = fine_parts.shape[2]
    outs = (tokens_grad.shape,) + shapes
    return pl.pallas_call(
        collect_kernel,
        out_shape=tuple(jax.ShapeDtypeStruct(shape, BF16) for shape in outs),
        in_specs=[hbm] * 5,
        out_specs=(hbm,) * 4,
        scratch_shapes=[pltpu.SMEM(paths.shape, jnp.int32)]
        + [pltpu.VMEM(shape, BF16) for shape in outs]
        + [
            pltpu.VMEM(coarse_parts.shape, BF16),
            pltpu.VMEM(middle_parts.shape, BF16),
            pltpu.VMEM(fine_parts.shape, BF16),
            pltpu.VMEM((count + 1, rows, medium), F32),
            pltpu.VMEM((count + 1, rows, narrow), F32),
            pltpu.SMEM((shapes[1][0],), jnp.int32),
            pltpu.SMEM((shapes[2][0],), jnp.int32),
            pltpu.SemaphoreType.DMA((5,)),
            pltpu.SemaphoreType.DMA((4,)),
        ],
        compiler_params=pltpu.CompilerParams(vmem_limit_bytes=60 * 2**20),
        name="collect",
    )(paths, tokens_grad, middle_parts, fine_parts, coarse_parts)


def on_device(tokens, cotangent, path, coarse_weights, middle_weights, fine_weights):
    members = lax.axis_size("mem")
    groups = lax.axis_size("grp")
    paths, tokens_grad, middle_parts, fine_parts, coarse_parts = exchange(
        path, tokens, cotangent, coarse_weights, middle_weights, fine_weights, groups, members
    )
    flat = lambda parts: parts.reshape((groups * members,) + parts.shape[2:])
    return collect(
        paths,
        tokens_grad,
        flat(middle_parts),
        flat(fine_parts),
        coarse_parts,
        (coarse_weights.shape, middle_weights.shape, fine_weights.shape),
    )


def solution(mesh):
    return jax.shard_map(
        on_device,
        mesh=mesh,
        in_specs=(
            P(("grp", "mem"), None),
            P(("grp", "mem"), None),
            P(("grp", "mem"), None),
            P(None, "mem", None),
            P(None, "mem", None),
            P("grp", "mem", None),
        ),
        out_specs=(
            P(("grp", "mem"), None),
            P(None, "mem", None),
            P(None, "mem", None),
            P("grp", "mem", None),
        ),
        check_vma=False,
    )
```

```python
import functools
import math

import jax
import jax.numpy as jnp
from jax import lax
from jax.experimental import pallas as pl
from jax.experimental.pallas import tpu as pltpu
from jax.sharding import PartitionSpec as P

MESH = pl.DeviceIdType.MESH
LANES = 128
F32 = jnp.float32
BF16 = jnp.bfloat16


def gelu_parts(before, hidden_grad):
    scale = math.sqrt(2.0 / math.pi)
    square = before * before
    tanh = jnp.tanh(scale * (before + 0.044715 * (square * before)))
    half = 0.5 * (1.0 + tanh)
    hidden = before * half
    slope = half + 0.5 * before * (1.0 - tanh * tanh) * (scale * (1.0 + 3 * 0.044715 * square))
    return hidden.astype(BF16), (hidden_grad * slope).astype(BF16)


def dot(left, right):
    return jnp.dot(left, right, preferred_element_type=F32)


def dot_transposed(left, right):
    return lax.dot_general(left, right, (((1,), (1,)), ((), ())), preferred_element_type=F32)


def level(weights, x, g, xt, gt):
    width = weights.shape[1]
    half = width // 2
    if half % LANES == 0:
        up = weights[:, :half]
        down = weights[:, half:]
        hidden, grad = gelu_parts(dot(x, up), dot(g, down))
        term = jnp.concatenate(
            [dot(xt, grad).astype(BF16), dot(gt, hidden).astype(BF16)], axis=1
        )
        return term, dot_transposed(grad, up)
    before = dot(x, weights)
    hidden_grad = pltpu.roll(dot(g, weights), half, 1)
    hidden, grad = gelu_parts(before, hidden_grad)
    first = lax.broadcasted_iota(jnp.int32, grad.shape, 1) < half
    grad = jnp.where(first, grad.astype(F32), 0.0).astype(BF16)
    hidden = jnp.where(first, hidden.astype(F32), 0.0)
    hidden = pltpu.roll(hidden, half, 1).astype(BF16)
    term = (dot(xt, grad) + dot(gt, hidden)).astype(BF16)
    return term, dot_transposed(grad, weights)


def plan(members, rows):
    inner = max(k for k in range(1, math.isqrt(members) + 1) if members % k == 0)
    cores = next(
        k for k in range(1, inner + 1) if inner % k == 0 and (k * rows % LANES == 0 or k == inner)
    )
    return members // inner, inner // cores, cores


def bits_of(outer):
    bits = []
    while outer > 1:
        outer //= 2
        bits.append(outer)
    return bits


def main_kernel(
    groups,
    members,
    path_row,
    tokens_hbm,
    cotangent_hbm,
    coarse_hbm,
    middle_hbm,
    fine_hbm,
    paths_out,
    tokens_out,
    middle_out,
    fine_parts_out,
    coarse_out,
    all_paths,
    tokens_grad,
    middle_parts,
    fine_parts,
    coarse_parts,
    path,
    both,
    docs,
    coarse_w,
    middle_w,
    fine_w,
    middle_send,
    fine_out,
    fine_in,
    fine_send,
    middle_block,
    fine_block,
    middle_term,
    fine_term,
    sums,
    from_core,
    from_line,
    coarse_total,
    flipped,
    quad_t,
    total,
    pre_give,
    pre_take,
    act_keep,
    act_give,
    act_take,
    back_give,
    back_take,
    path_send,
    path_recv,
    mem_send,
    mem_recv,
    weight_recv,
    grp_send,
    grp_recv,
    quad_send,
    quad_recv,
    gather_send,
    gather_recv,
    core_send,
    core_recv,
    fold_send,
    fold_recv,
    local_sem,
    load_sem,
    token_sem,
    out_sem,
    middle_send_on,
    middle_recv_on,
    fine_send_on,
    fine_recv_on,
):
    group = lax.axis_index("grp")
    me = lax.axis_index("mem")
    count = groups * members
    device = group * members + me
    owned = fine_w.shape[0]
    blocks, outer, cores, rows, columns = coarse_w.shape
    _, _, sides, token_count, span = both.shape
    inner = sides * cores
    depth = outer * span
    bits = bits_of(outer)
    line = me // inner
    place = lax.rem(me, inner)
    side = place // cores
    core = lax.rem(place, cores)
    twist = 1 - sides % 2
    slot = lax.rem(group + twist * side, 2)
    mirror = group + 1 - 2 * lax.rem(group, 2)
    width = tokens_grad.shape[1]

    def loop(start, stop, body):
        def wrapped(step, carry):
            body(step)
            return carry

        lax.fori_loop(start, stop, wrapped, 0)

    def flip(r):
        there = line
        for bit in bits:
            if r & bit:
                there = there + bit * (1 - 2 * lax.rem(there // bit, 2))
        return there

    def at_line(r, s, c):
        return flip(r) * inner + s * cores + c

    def to_member(source, target, send, recv, p):
        return pltpu.make_async_remote_copy(
            src_ref=source,
            dst_ref=target,
            send_sem=send,
            recv_sem=recv,
            device_id={"mem": p},
            device_id_type=MESH,
        )

    half = pl.ds(pl.multiple_of(slot * columns, LANES), columns)
    loads = [
        pltpu.make_async_copy(source, target, load_sem.at[index])
        for index, (source, target) in enumerate(
            (
                (coarse_hbm.at[:, :, half], coarse_w.at[:, line, core]),
                (fine_hbm, fine_w),
                (middle_hbm, middle_w),
            )
        )
    ]
    places = [(o, a) for o in range(outer) for a in range(sides)]
    token_loads = [
        pltpu.make_async_copy(
            source.at[:, pl.ds(index * span, span)],
            both.at[which, o, a],
            token_sem.at[which, index],
        )
        for which, source in enumerate((tokens_hbm, cotangent_hbm))
        for index, (o, a) in enumerate(places)
    ]
    loads[0].start()
    for load in token_loads:
        load.start()
    for load in loads[1:]:
        load.start()
    outs = [
        pltpu.make_async_copy(source, target, out_sem.at[index])
        for index, (source, target) in enumerate(
            (
                (all_paths, paths_out),
                (tokens_grad, tokens_out),
                (middle_parts, middle_out),
                (fine_parts, fine_parts_out),
                (coarse_parts, coarse_out),
            )
        )
    ]
    barrier = pltpu.get_barrier_semaphore()

    def anyone(step):
        other = lax.rem(device + step, count)
        return other, (other // members, lax.rem(other, members))

    def greet(step):
        _, where = anyone(step)
        pl.semaphore_signal(barrier, inc=1, device_id=where, device_id_type=MESH)

    loop(1, count, greet)
    loads[0].wait()
    pl.semaphore_wait(barrier, count - 1)

    def path_copy(step):
        _, where = anyone(step)
        return pltpu.make_async_remote_copy(
            src_ref=path_row,
            dst_ref=all_paths.at[device],
            send_sem=path_send,
            recv_sem=path_recv,
            device_id=where,
            device_id_type=MESH,
        )

    loop(1, count, lambda step: path_copy(step).start())
    all_paths[device] = path_row[...]

    quad = [(dy, da) for dy in range(2) for da in range(sides)]
    peers = quad[1:]

    def differs(dy, da):
        return (dy + twist * da) % 2

    def quad_side(da):
        return lax.rem(side + da, sides)

    def quad_copy(stage, source, target, dy, da):
        back_da = (sides - da) % sides
        return pltpu.make_async_remote_copy(
            src_ref=source,
            dst_ref=target.at[dy, back_da],
            send_sem=quad_send.at[stage, dy, da],
            recv_sem=quad_recv.at[stage, dy, back_da],
            device_id=(mirror if dy else group, at_line(0, quad_side(da), core)),
            device_id_type=MESH,
        )

    def quad_wait(stage, source, target, dy, da):
        quad_copy(stage, source, target, dy, (sides - da) % sides).wait_recv()

    def gather_copy(r):
        piece = coarse_w.at[:, line, core]
        return to_member(
            piece, piece, gather_send.at[r, 0], gather_recv.at[r], at_line(r, side, core)
        )

    def gather_wait(r):
        piece = coarse_w.at[:, flip(r), core]
        to_member(
            piece, piece, gather_send.at[r, 0], gather_recv.at[r], at_line(r, side, core)
        ).wait_recv()

    def core_copy(r, step, landing_own):
        there = lax.rem(core + step, cores)
        landing = core if landing_own else lax.rem(core + cores - step, cores)
        piece = coarse_w.at[:, flip(r), landing]
        return to_member(
            piece, piece, core_send.at[0, r, step], core_recv.at[0, r, step], at_line(0, side, there)
        )

    def pass_on(r):
        if r == 0:
            for far in range(outer - 1, 0, -1):
                gather_copy(far).start()
        for step in range(1, cores):
            core_copy(r, step, True).start()

    def doc_copy(dy, da):
        which = 1 - slot if differs(dy, da) else slot
        return quad_copy(0, both.at[which, :, quad_side(da)], docs, dy, da)

    pass_on(0)
    for load in token_loads:
        load.wait()
    for dy, da in peers:
        doc_copy(dy, da).start()
    for which in range(2):
        for index, (o, a) in enumerate(places):
            flipped[which, index * span : (index + 1) * span, :] = both[which, o, a].T
    docs[0, 0] = both[slot, :, side]
    for load in loads[1:]:
        load.wait()
    if outer > 1:
        gather_wait(1)
        pass_on(1)

    def turn(dy, da):
        q = dy * sides + da
        for o in range(outer):
            quad_t[o * span : (o + 1) * span, q * token_count : (q + 1) * token_count] = docs[
                dy, da, o
            ].T

    turn(0, 0)
    others = all_paths.at[pl.ds(0, count - 1)]
    pltpu.make_async_copy(others, others, path_recv).wait()
    scalars = pltpu.make_async_copy(all_paths, path, local_sem.at[0])
    scalars.start()
    scalars.wait()
    outs[0].start()

    def route(document, column):
        return path[document, 0, column]

    def member_copy(index, source, target, p, landing_own):
        landing = me if landing_own else p
        arrived = weight_recv.at[index] if index < 2 else mem_recv.at[index - 2, landing]
        return to_member(source.at[p], target.at[landing], mem_send.at[index], arrived, p)

    def all_of(ref, number, sem):
        some = ref.at[pl.ds(0, number)]
        return pltpu.make_async_copy(some, some, sem)

    near = outer * cores

    def partner(step):
        there = lax.rem(side + step // near, sides)
        rest = lax.rem(step, near)
        return (
            lax.rem(line + rest // cores, outer) * inner
            + there * cores
            + lax.rem(core + lax.rem(rest, cores), cores)
        )

    def spread(index, source, target, start=1, stop=members):
        loop(
            start,
            stop,
            lambda step: member_copy(index, source, target, partner(step), True).start(),
        )

    def arrive(index, target):
        if members > 1:
            all_of(target, members - 1, weight_recv.at[index]).wait()

    def left(index, source):
        if members > 1:
            all_of(source, members - 1, mem_send.at[index]).wait()

    def group_copy(index, source, target, step, landing_own):
        other = lax.rem(group + step, groups)
        landing = group if landing_own else other
        return pltpu.make_async_remote_copy(
            src_ref=source(other),
            dst_ref=target.at[landing],
            send_sem=grp_send.at[index, other],
            recv_sem=grp_recv.at[index, landing],
            device_id={"grp": other},
            device_id_type=MESH,
        )

    def group_spread(*what):
        loop(1, groups, lambda step: group_copy(*what, step, True).start())

    def group_arrive(*what):
        loop(1, groups, lambda step: group_copy(*what, step, False).wait_recv())

    def group_left(*what):
        loop(1, groups, lambda step: group_copy(*what, step, False).wait_send())

    def pick_fine(index):
        held = jnp.clip(route(index, 2) - group * owned, 0, owned - 1)
        fine_out[index // members, lax.rem(index, members)] = fine_w[held]

    def pick_middle(p):
        middle_send[p] = middle_w[route(group * members + p, 1)]

    loop(0, count, pick_fine)
    fine_trade = (0, lambda other: fine_out.at[other], fine_in)
    group_spread(*fine_trade)
    loop(0, members, pick_middle)
    spread(0, middle_send, middle_block)
    fine_in[group] = fine_out[group]
    middle_block[me] = middle_send[me]

    for r in range(2, outer, 2):
        gather_wait(r)
        pass_on(r)
    for dy, da in peers:
        quad_wait(0, both.at[0, :, 0], docs, dy, da)
        turn(dy, da)

    for r in range(3, outer, 2):
        gather_wait(r)
        pass_on(r)
    for r in range(outer):
        for step in range(1, cores):
            core_copy(r, step, False).wait_recv()

    def block_of(dy, da):
        who = (mirror if dy else group) * members + at_line(0, quad_side(da), core)
        return route(who, 0)

    def coarse_of(k):
        return coarse_w[k].reshape(depth, columns)

    def wide_of(dy, da):
        return jnp.concatenate([docs[dy, da, o] for o in range(outer)], axis=1)

    first = slot == 0
    for dy, da in peers:
        pre_give[dy, da] = dot(wide_of(dy, da), coarse_of(block_of(dy, da))).astype(BF16)
        quad_copy(1, pre_give.at[dy, da], pre_take, dy, da).start()
    def merge_fine(p):
        owner = route(group * members + p, 2) // owned
        fine_send[p] = fine_in[owner, p]

    group_arrive(*fine_trade)
    loop(0, members, merge_fine)
    spread(1, fine_send, fine_block)
    fine_block[me] = fine_send[me]

    pre_own = dot(wide_of(0, 0), coarse_of(block_of(0, 0)))
    pre_other = jnp.zeros_like(pre_own)

    def whole(which):
        return jnp.concatenate([both[which, o, a] for o, a in places], axis=1)

    def compute(block, term):
        weights = block[...].reshape(width, block.shape[-1])
        value, part = level(weights, whole(0), whole(1), flipped[0], flipped[1])
        term[...] = value.reshape(term.shape)
        return part

    middle_own = middle_parts.at[group]
    fine_own = fine_parts.at[group]

    for dy, da in peers:
        quad_wait(1, pre_give.at[0, 0], pre_take, dy, da)
    for dy, da in peers:
        if differs(dy, da):
            pre_other = pre_other + pre_take[dy, da].astype(F32)
        else:
            pre_own = pre_own + pre_take[dy, da].astype(F32)
    hidden, before_grad = gelu_parts(
        jnp.where(first, pre_own, pre_other), jnp.where(first, pre_other, pre_own)
    )
    hidden, before_grad = hidden.astype(F32), before_grad.astype(F32)
    act_give[...] = jnp.where(first, hidden, before_grad).astype(BF16)
    act_keep[...] = jnp.where(first, before_grad, hidden).astype(BF16)
    act_take[0, 0] = act_keep[...]
    for dy, da in peers:
        quad_copy(2, act_give if differs(dy, da) else act_keep, act_take, dy, da).start()

    arrive(0, middle_block)
    total[...] = compute(middle_block, middle_term)
    spread(2, middle_term, middle_own)
    middle_parts[group, me] = middle_term[me]

    arrive(1, fine_block)
    total[...] += compute(fine_block, fine_term)
    spread(3, fine_term, fine_own)
    fine_parts[group, me] = fine_term[me]

    for dy, da in peers:
        quad_wait(2, act_keep, act_take, dy, da)

    for k in range(blocks):
        acts = [
            jnp.where(block_of(dy, da) == k, act_take[dy, da].astype(F32), 0.0).astype(BF16)
            for dy, da in quad
        ]
        value = dot(quad_t[...], jnp.concatenate(acts, axis=0))
        sums[:, :, k] = value.astype(BF16).reshape(outer, cores, rows, columns)

    order = list(range(outer - 1, 0, -2)) + list(range(outer - 2, 0, -2)) + [0]

    def fold_core(r, step):
        there = lax.rem(core + step, cores)
        return to_member(
            sums.at[flip(r), there],
            from_core.at[r, step],
            core_send.at[1, r, step],
            core_recv.at[1, r, step],
            at_line(0, side, there),
        )

    def fold_line(r, bit):
        return to_member(
            sums.at[flip(r), core],
            from_line.at[r ^ bit, bits.index(bit)],
            fold_send.at[r],
            fold_recv.at[r ^ bit, bits.index(bit)],
            at_line(bit, side, core),
        )

    def fold_line_wait(r, bit):
        to_member(
            sums.at[flip(r), core],
            from_line.at[r, bits.index(bit)],
            fold_send.at[r],
            fold_recv.at[r, bits.index(bit)],
            at_line(bit, side, core),
        ).wait_recv()

    def lower(r):
        return [bit for bit in reversed(bits) if r == 0 or bit < (r & -r)]

    for r in order:
        for step in range(1, cores):
            fold_core(r, step).start()

    def back_copy(dy, da):
        return quad_copy(3, back_give.at[dy, da], back_take, dy, da)

    @pl.when(first)
    def _():
        for dy, da in peers:
            back_give[dy, da] = dot_transposed(
                act_take[dy, da], coarse_of(block_of(dy, da))
            ).astype(BF16)
            back_copy(dy, da).start()

    def hand_on(target, send_on, recv_on, p, step, landing_own):
        other = lax.rem(group + step, groups)
        landing = group if landing_own else other
        return pltpu.make_async_remote_copy(
            src_ref=target.at[group, p],
            dst_ref=target.at[landing, p],
            send_sem=send_on,
            recv_sem=recv_on,
            device_id={"grp": other},
            device_id_type=MESH,
        )

    def relay(index, source, target, send_on, recv_on, first_step=0, last_step=members):
        own = target.at[group]

        def start(p):
            loop(1, groups, lambda step: hand_on(target, send_on, recv_on, p, step, True).start())

        def body(step):
            p = partner(step)
            member_copy(index, source, own, p, False).wait_recv()
            start(p)

        if first_step == 0:
            start(me)
        loop(max(first_step, 1), last_step, body)

    def relay_done(target, send_on, recv_on):
        if groups > 1:
            all_of(target, groups - 1, recv_on).wait()
            all_of(target, groups - 1, send_on).wait()

    def folded(r):
        value = sums[flip(r), core].astype(F32)
        for step in range(1, cores):
            value = value + from_core[r, step].astype(F32)
        for bit in lower(r):
            value = value + from_line[r, bits.index(bit)].astype(F32)
        return value

    relay(2, middle_term, middle_parts, middle_send_on, middle_recv_on, 0, near)
    for r in order:
        for step in range(1, cores):
            fold_core(r, step).wait_recv()
        for bit in lower(r):
            fold_line_wait(r, bit)
        if r:
            sums[flip(r), core] = folded(r).astype(BF16)
            fold_line(r, r & -r).start()
            if r == 1:
                relay(2, middle_term, middle_parts, middle_send_on, middle_recv_on, near, members)
            if r == order[-2]:
                relay(3, fine_term, fine_parts, fine_send_on, fine_recv_on)
        else:
            coarse_total[...] = folded(0).astype(BF16)

    coarse_trade = (1, lambda other: coarse_total, coarse_parts)
    group_spread(*coarse_trade)
    coarse_parts[group] = coarse_total[...]

    def add_back(dy, da, piece):
        for o in range(outer):
            columns_of = pl.ds(pl.multiple_of((o * sides + quad_side(da)) * span, span), span)
            total[:, columns_of] += piece[:, o * span : (o + 1) * span]

    @pl.when(first)
    def _():
        add_back(0, 0, dot_transposed(act_take[0, 0], coarse_of(block_of(0, 0))))
        for dy, da in peers:
            if not differs(dy, da):
                quad_wait(3, back_give.at[0, 0], back_take, dy, da)
                add_back(dy, da, back_take[dy, da].astype(F32))
        for dy, da in peers:
            back_copy(dy, da).wait_send()

    @pl.when(slot == 1)
    def _():
        for dy, da in peers:
            if differs(dy, da):
                quad_wait(3, back_give.at[0, 0], back_take, dy, da)
                add_back(dy, da, back_take[dy, da].astype(F32))

    tokens_grad[...] = total[...].astype(BF16)
    outs[1].start()
    pltpu.make_async_copy(others, others, path_send).wait()
    for dy, da in peers:
        doc_copy(dy, da).wait_send()
        quad_copy(1, pre_give.at[dy, da], pre_take, dy, da).wait_send()
        quad_copy(2, act_give if differs(dy, da) else act_keep, act_take, dy, da).wait_send()
    for r in range(outer):
        if r:
            gather_copy(r).wait_send()
        for step in range(1, cores):
            core_copy(r, step, True).wait_send()
            fold_core(r, step).wait_send()
        if r:
            fold_line(r, r & -r).wait_send()
    left(0, middle_send)
    left(1, fine_send)
    group_left(*fine_trade)
    left(2, middle_term)
    left(3, fine_term)
    relay_done(middle_parts, middle_send_on, middle_recv_on)
    outs[2].start()
    relay_done(fine_parts, fine_send_on, fine_recv_on)
    outs[3].start()
    group_arrive(*coarse_trade)
    outs[4].start()
    group_left(*coarse_trade)
    for out in outs:
        out.wait()


def exchange(path, tokens, cotangent, coarse_w, middle_w, fine_w, groups, members):
    blocks, rows, wide = coarse_w.shape
    medium, narrow = middle_w.shape[2], fine_w.shape[2]
    token_count, width = tokens.shape
    count = groups * members
    outer, sides, cores = plan(members, rows)
    span = cores * rows
    depth = outer * span
    steps = max(len(bits_of(outer)), 1)
    columns = wide // 2

    def stack(*shape):
        return pltpu.VMEM(shape, BF16)

    def sems(*shape):
        return pltpu.SemaphoreType.DMA(shape)

    vmem = pl.BlockSpec(memory_space=pltpu.VMEM)
    return pl.pallas_call(
        functools.partial(main_kernel, groups, members),
        out_shape=(
            jax.ShapeDtypeStruct((count,) + path.shape, jnp.int32),
            jax.ShapeDtypeStruct(tokens.shape, BF16),
            jax.ShapeDtypeStruct((groups, members, rows, medium), BF16),
            jax.ShapeDtypeStruct((groups, members, rows, narrow), BF16),
            jax.ShapeDtypeStruct((groups, blocks, rows, columns), BF16),
        ),
        in_specs=[vmem] + [pl.BlockSpec(memory_space=pl.ANY)] * 5,
        out_specs=(pl.BlockSpec(memory_space=pl.ANY),) * 5,
        scratch_shapes=[
            pltpu.VMEM((count,) + path.shape, jnp.int32),
            stack(*tokens.shape),
            stack(groups, members, rows, medium),
            stack(groups, members, rows, narrow),
            stack(groups, blocks, rows, columns),
            pltpu.SMEM((count,) + path.shape, jnp.int32),
            stack(2, outer, sides, token_count, span),
            stack(2, sides, outer, token_count, span),
            stack(blocks, outer, cores, rows, columns),
            stack(*middle_w.shape),
            stack(*fine_w.shape),
            stack(members, rows, medium),
            stack(groups, members, rows, narrow),
            stack(groups, members, rows, narrow),
            stack(members, rows, narrow),
            stack(members, rows, medium),
            stack(members, rows, narrow),
            stack(members, rows, medium),
            stack(members, rows, narrow),
            stack(outer, cores, blocks, rows, columns),
            stack(outer, cores, blocks, rows, columns),
            stack(outer, steps, blocks, rows, columns),
            stack(blocks, rows, columns),
            stack(2, width, token_count),
            stack(depth, 2 * sides * token_count),
            pltpu.VMEM((token_count, width), F32),
            stack(2, sides, token_count, columns),
            stack(2, sides, token_count, columns),
            stack(token_count, columns),
            stack(token_count, columns),
            stack(2, sides, token_count, columns),
            stack(2, sides, token_count, depth),
            stack(2, sides, token_count, depth),
            pltpu.SemaphoreType.DMA,
            pltpu.SemaphoreType.DMA,
            sems(4),
            sems(2, members),
            sems(2),
            sems(2, groups),
            sems(2, groups),
            sems(4, 2, sides),
            sems(4, 2, sides),
            sems(outer, steps),
            sems(outer),
            sems(2, outer, cores),
            sems(2, outer, cores),
            sems(outer),
            sems(outer, steps),
            sems(1),
            sems(3),
            sems(2, outer * sides),
            sems(5),
            pltpu.SemaphoreType.DMA,
            pltpu.SemaphoreType.DMA,
            pltpu.SemaphoreType.DMA,
            pltpu.SemaphoreType.DMA,
        ],
        compiler_params=pltpu.CompilerParams(
            collective_id=0, has_side_effects=True, vmem_limit_bytes=60 * 2**20
        ),
        name="exchange",
    )(path, tokens, cotangent, coarse_w, middle_w, fine_w)


def collect_kernel(
    path_hbm,
    tokens_hbm,
    middle_hbm,
    fine_hbm,
    coarse_hbm,
    tokens_out,
    coarse_out,
    middle_out,
    fine_out,
    path,
    tokens_grad,
    coarse_grad,
    middle_grad,
    fine_grad,
    coarse_parts,
    middle_parts,
    fine_parts,
    middle_sum,
    fine_sum,
    middle_last,
    fine_last,
    load_sem,
    out_sem,
):
    count = middle_parts.shape[0]
    owned = fine_grad.shape[0]
    first_owned = lax.axis_index("grp") * owned
    loads = [
        pltpu.make_async_copy(source, target, load_sem.at[index])
        for index, (source, target) in enumerate(
            (
                (path_hbm, path),
                (middle_hbm, middle_parts),
                (fine_hbm, fine_parts),
                (coarse_hbm, coarse_parts),
                (tokens_hbm, tokens_grad),
            )
        )
    ]
    outs = [
        pltpu.make_async_copy(source, target, out_sem.at[index])
        for index, (source, target) in enumerate(
            (
                (tokens_grad, tokens_out),
                (coarse_grad, coarse_out),
                (middle_grad, middle_out),
                (fine_grad, fine_out),
            )
        )
    ]
    for load in loads:
        load.start()
    for last in (middle_last, fine_last):
        for k in range(last.shape[0]):
            last[k] = count
    middle_grad[...] = jnp.zeros_like(middle_grad)
    middle_sum[count] = jnp.zeros(middle_sum.shape[1:], F32)
    fine_sum[count] = jnp.zeros(fine_sum.shape[1:], F32)
    loads[0].wait()
    loads[1].wait()

    def add_middle(document, carry):
        k = path[document, 0, 1]
        value = middle_parts[document].astype(F32) + middle_sum[middle_last[k]]
        middle_sum[document] = value
        middle_grad[k] = value.astype(BF16)
        middle_last[k] = document
        return carry

    lax.fori_loop(0, count, add_middle, 0)
    outs[2].start()
    fine_grad[...] = jnp.zeros_like(fine_grad)
    loads[2].wait()

    def add_fine(document, carry):
        place = path[document, 0, 2] - first_owned

        @pl.when((place >= 0) & (place < owned))
        def _():
            piece = fine_parts[document].astype(F32) + fine_sum[fine_last[place]]
            fine_sum[document] = piece
            fine_grad[place] = piece.astype(BF16)
            fine_last[place] = document

        return carry

    lax.fori_loop(0, count, add_fine, 0)
    outs[3].start()
    loads[3].wait()
    groups, _, _, columns = coarse_parts.shape
    outer, sides, cores = plan(lax.axis_size("mem"), coarse_grad.shape[1])
    side = lax.rem(lax.axis_index("mem"), sides * cores) // cores
    for s in range(2):
        held = lax.rem(s + (1 - sides % 2) * side, 2)
        value = coarse_parts[held].astype(F32)
        for other in range(2, groups, 2):
            value = value + coarse_parts[held + other].astype(F32)
        coarse_grad[:, :, s * columns : (s + 1) * columns] = value.astype(BF16)
    outs[1].start()
    loads[4].wait()
    outs[0].start()
    for out in outs:
        out.wait()


def collect(paths, tokens_grad, middle_parts, fine_parts, coarse_parts, shapes):
    hbm = pl.BlockSpec(memory_space=pl.ANY)
    count, rows, medium = middle_parts.shape
    narrow = fine_parts.shape[2]
    outs = (tokens_grad.shape,) + shapes
    return pl.pallas_call(
        collect_kernel,
        out_shape=tuple(jax.ShapeDtypeStruct(shape, BF16) for shape in outs),
        in_specs=[hbm] * 5,
        out_specs=(hbm,) * 4,
        scratch_shapes=[pltpu.SMEM(paths.shape, jnp.int32)]
        + [pltpu.VMEM(shape, BF16) for shape in outs]
        + [
            pltpu.VMEM(coarse_parts.shape, BF16),
            pltpu.VMEM(middle_parts.shape, BF16),
            pltpu.VMEM(fine_parts.shape, BF16),
            pltpu.VMEM((count + 1, rows, medium), F32),
            pltpu.VMEM((count + 1, rows, narrow), F32),
            pltpu.SMEM((shapes[1][0],), jnp.int32),
            pltpu.SMEM((shapes[2][0],), jnp.int32),
            pltpu.SemaphoreType.DMA((5,)),
            pltpu.SemaphoreType.DMA((4,)),
        ],
        compiler_params=pltpu.CompilerParams(vmem_limit_bytes=60 * 2**20),
        name="collect",
    )(paths, tokens_grad, middle_parts, fine_parts, coarse_parts)


def on_device(tokens, cotangent, path, coarse_weights, middle_weights, fine_weights):
    members = lax.axis_size("mem")
    groups = lax.axis_size("grp")
    paths, tokens_grad, middle_parts, fine_parts, coarse_parts = exchange(
        path, tokens, cotangent, coarse_weights, middle_weights, fine_weights, groups, members
    )
    flat = lambda parts: parts.reshape((groups * members,) + parts.shape[2:])
    return collect(
        paths,
        tokens_grad,
        flat(middle_parts),
        flat(fine_parts),
        coarse_parts,
        (coarse_weights.shape, middle_weights.shape, fine_weights.shape),
    )


def solution(mesh):
    return jax.shard_map(
        on_device,
        mesh=mesh,
        in_specs=(
            P(("grp", "mem"), None),
            P(("grp", "mem"), None),
            P(("grp", "mem"), None),
            P(None, "mem", None),
            P(None, "mem", None),
            P("grp", "mem", None),
        ),
        out_specs=(
            P(("grp", "mem"), None),
            P(None, "mem", None),
            P(None, "mem", None),
            P("grp", "mem", None),
        ),
        check_vma=False,
    )
```

```python
import functools
import math

import jax
import jax.numpy as jnp
from jax import lax
from jax.experimental import pallas as pl
from jax.experimental.pallas import tpu as pltpu
from jax.sharding import PartitionSpec as P

MESH = pl.DeviceIdType.MESH
LANES = 128
F32 = jnp.float32
BF16 = jnp.bfloat16


def gelu_parts(before, hidden_grad):
    scale = math.sqrt(2.0 / math.pi)
    square = before * before
    tanh = jnp.tanh(scale * (before + 0.044715 * (square * before)))
    half = 0.5 * (1.0 + tanh)
    hidden = before * half
    slope = half + 0.5 * before * (1.0 - tanh * tanh) * (scale * (1.0 + 3 * 0.044715 * square))
    return hidden.astype(BF16), (hidden_grad * slope).astype(BF16)


def dot(left, right):
    return jnp.dot(left, right, preferred_element_type=F32)


def dot_transposed(left, right):
    return lax.dot_general(left, right, (((1,), (1,)), ((), ())), preferred_element_type=F32)


def level(weights, x, g, xt, gt):
    width = weights.shape[1]
    half = width // 2
    if half % LANES == 0:
        up = weights[:, :half]
        down = weights[:, half:]
        hidden, grad = gelu_parts(dot(x, up), dot(g, down))
        term = jnp.concatenate(
            [dot(xt, grad).astype(BF16), dot(gt, hidden).astype(BF16)], axis=1
        )
        return term, dot_transposed(grad, up)
    before = dot(x, weights)
    hidden_grad = pltpu.roll(dot(g, weights), half, 1)
    hidden, grad = gelu_parts(before, hidden_grad)
    first = lax.broadcasted_iota(jnp.int32, grad.shape, 1) < half
    grad = jnp.where(first, grad.astype(F32), 0.0).astype(BF16)
    hidden = jnp.where(first, hidden.astype(F32), 0.0)
    hidden = pltpu.roll(hidden, half, 1).astype(BF16)
    term = (dot(xt, grad) + dot(gt, hidden)).astype(BF16)
    return term, dot_transposed(grad, weights)


def plan(members, rows):
    inner = max(k for k in range(1, math.isqrt(members) + 1) if members % k == 0)
    cores = next(
        k for k in range(1, inner + 1) if inner % k == 0 and (k * rows % LANES == 0 or k == inner)
    )
    return members // inner, inner // cores, cores


def bits_of(outer):
    bits = []
    while outer > 1:
        outer //= 2
        bits.append(outer)
    return bits


def main_kernel(
    groups,
    members,
    path_row,
    tokens_hbm,
    cotangent_hbm,
    coarse_hbm,
    middle_hbm,
    fine_hbm,
    paths_out,
    tokens_out,
    middle_out,
    fine_parts_out,
    coarse_out,
    all_paths,
    tokens_grad,
    middle_parts,
    fine_parts,
    coarse_parts,
    path,
    both,
    docs,
    coarse_w,
    middle_w,
    fine_w,
    middle_send,
    fine_out,
    fine_in,
    fine_send,
    middle_block,
    fine_block,
    middle_term,
    fine_term,
    sums,
    from_core,
    from_line,
    coarse_total,
    flipped,
    quad_t,
    total,
    pre_give,
    pre_take,
    act_keep,
    act_give,
    act_take,
    back_give,
    back_take,
    path_send,
    path_recv,
    mem_send,
    mem_recv,
    weight_recv,
    grp_send,
    grp_recv,
    quad_send,
    quad_recv,
    gather_send,
    gather_recv,
    core_send,
    core_recv,
    fold_send,
    fold_recv,
    local_sem,
    load_sem,
    token_sem,
    out_sem,
    middle_send_on,
    middle_recv_on,
    fine_send_on,
    fine_recv_on,
):
    group = lax.axis_index("grp")
    me = lax.axis_index("mem")
    count = groups * members
    device = group * members + me
    owned = fine_w.shape[0]
    blocks, outer, cores, rows, columns = coarse_w.shape
    _, _, sides, token_count, span = both.shape
    inner = sides * cores
    depth = outer * span
    bits = bits_of(outer)
    line = me // inner
    place = lax.rem(me, inner)
    side = place // cores
    core = lax.rem(place, cores)
    twist = 1 - sides % 2
    slot = lax.rem(group + twist * side, 2)
    mirror = group + 1 - 2 * lax.rem(group, 2)
    width = tokens_grad.shape[1]

    def loop(start, stop, body):
        def wrapped(step, carry):
            body(step)
            return carry

        lax.fori_loop(start, stop, wrapped, 0)

    def flip(r):
        there = line
        for bit in bits:
            if r & bit:
                there = there + bit * (1 - 2 * lax.rem(there // bit, 2))
        return there

    def at_line(r, s, c):
        return flip(r) * inner + s * cores + c

    def to_member(source, target, send, recv, p):
        return pltpu.make_async_remote_copy(
            src_ref=source,
            dst_ref=target,
            send_sem=send,
            recv_sem=recv,
            device_id={"mem": p},
            device_id_type=MESH,
        )

    half = pl.ds(pl.multiple_of(slot * columns, LANES), columns)
    loads = [
        pltpu.make_async_copy(source, target, load_sem.at[index])
        for index, (source, target) in enumerate(
            (
                (coarse_hbm.at[:, :, half], coarse_w.at[:, line, core]),
                (fine_hbm, fine_w),
                (middle_hbm, middle_w),
            )
        )
    ]
    places = [(o, a) for o in range(outer) for a in range(sides)]
    token_loads = [
        pltpu.make_async_copy(
            source.at[:, pl.ds(index * span, span)],
            both.at[which, o, a],
            token_sem,
        )
        for which, source in enumerate((tokens_hbm, cotangent_hbm))
        for index, (o, a) in enumerate(places)
    ]
    loads[0].start()
    for load in token_loads:
        load.start()
    for load in loads[1:]:
        load.start()
    outs = [
        pltpu.make_async_copy(source, target, out_sem.at[index])
        for index, (source, target) in enumerate(
            (
                (all_paths, paths_out),
                (tokens_grad, tokens_out),
                (middle_parts, middle_out),
                (fine_parts, fine_parts_out),
                (coarse_parts, coarse_out),
            )
        )
    ]
    barrier = pltpu.get_barrier_semaphore()

    def anyone(step):
        other = lax.rem(device + step, count)
        return other, (other // members, lax.rem(other, members))

    def greet(step):
        _, where = anyone(step)
        pl.semaphore_signal(barrier, inc=1, device_id=where, device_id_type=MESH)

    loop(1, count, greet)
    loads[0].wait()
    pl.semaphore_wait(barrier, count - 1)

    def path_copy(step):
        _, where = anyone(step)
        return pltpu.make_async_remote_copy(
            src_ref=path_row,
            dst_ref=all_paths.at[device],
            send_sem=path_send,
            recv_sem=path_recv,
            device_id=where,
            device_id_type=MESH,
        )

    loop(1, count, lambda step: path_copy(step).start())
    all_paths[device] = path_row[...]

    quad = [(dy, da) for dy in range(2) for da in range(sides)]
    peers = quad[1:]

    def differs(dy, da):
        return (dy + twist * da) % 2

    def quad_side(da):
        return lax.rem(side + da, sides)

    def quad_copy(stage, source, target, dy, da):
        back_da = (sides - da) % sides
        return pltpu.make_async_remote_copy(
            src_ref=source,
            dst_ref=target.at[dy, back_da],
            send_sem=quad_send.at[stage, dy, da],
            recv_sem=quad_recv.at[stage, dy, back_da],
            device_id=(mirror if dy else group, at_line(0, quad_side(da), core)),
            device_id_type=MESH,
        )

    def quad_wait(stage, source, target, dy, da):
        quad_copy(stage, source, target, dy, (sides - da) % sides).wait_recv()

    def gather_copy(r):
        piece = coarse_w.at[:, line, core]
        return to_member(
            piece, piece, gather_send, gather_recv.at[r], at_line(r, side, core)
        )

    def gather_wait(r):
        piece = coarse_w.at[:, flip(r), core]
        to_member(
            piece, piece, gather_send, gather_recv.at[r], at_line(r, side, core)
        ).wait_recv()

    def core_copy(r, step, landing_own):
        there = lax.rem(core + step, cores)
        landing = core if landing_own else lax.rem(core + cores - step, cores)
        piece = coarse_w.at[:, flip(r), landing]
        return to_member(
            piece, piece, core_send.at[0, step], core_recv.at[0, r, step], at_line(0, side, there)
        )

    def pass_on(r):
        if r == 0:
            for far in range(1, outer):
                gather_copy(far).start()
        for step in range(1, cores):
            core_copy(r, step, True).start()

    def doc_copy(dy, da):
        which = 1 - slot if differs(dy, da) else slot
        return quad_copy(0, both.at[which, :, quad_side(da)], docs, dy, da)

    pass_on(0)
    pltpu.make_async_copy(both, both, token_sem).wait()
    for dy, da in peers:
        doc_copy(dy, da).start()
    for which in range(2):
        for index, (o, a) in enumerate(places):
            flipped[which, index * span : (index + 1) * span, :] = both[which, o, a].T
    docs[0, 0] = both[slot, :, side]
    for load in loads[1:]:
        load.wait()
    if outer > 1:
        gather_wait(1)
        pass_on(1)

    def turn(dy, da):
        q = dy * sides + da
        for o in range(outer):
            quad_t[o * span : (o + 1) * span, q * token_count : (q + 1) * token_count] = docs[
                dy, da, o
            ].T

    turn(0, 0)
    others = all_paths.at[pl.ds(0, count - 1)]
    pltpu.make_async_copy(others, others, path_recv).wait()
    scalars = pltpu.make_async_copy(all_paths, path, local_sem.at[0])
    scalars.start()
    scalars.wait()
    outs[0].start()

    def route(document, column):
        return path[document, 0, column]

    def member_copy(index, source, target, p, landing_own):
        landing = me if landing_own else p
        arrived = weight_recv.at[index] if index < 2 else mem_recv.at[index - 2, landing]
        return to_member(source.at[p], target.at[landing], mem_send.at[index], arrived, p)

    def all_of(ref, number, sem):
        some = ref.at[pl.ds(0, number)]
        return pltpu.make_async_copy(some, some, sem)

    near = outer * cores

    def partner(step):
        there = lax.rem(side + step // near, sides)
        rest = lax.rem(step, near)
        return (
            lax.rem(line + rest // cores, outer) * inner
            + there * cores
            + lax.rem(core + lax.rem(rest, cores), cores)
        )

    def spread(index, source, target, start=1, stop=members):
        loop(
            start,
            stop,
            lambda step: member_copy(index, source, target, partner(step), True).start(),
        )

    def arrive(index, target):
        if members > 1:
            all_of(target, members - 1, weight_recv.at[index]).wait()

    def left(index, source):
        if members > 1:
            all_of(source, members - 1, mem_send.at[index]).wait()

    def group_copy(index, source, target, step, landing_own):
        other = lax.rem(group + step, groups)
        landing = group if landing_own else other
        return pltpu.make_async_remote_copy(
            src_ref=source(other),
            dst_ref=target.at[landing],
            send_sem=grp_send.at[index, other],
            recv_sem=grp_recv.at[index, landing],
            device_id={"grp": other},
            device_id_type=MESH,
        )

    def group_spread(*what):
        loop(1, groups, lambda step: group_copy(*what, step, True).start())

    def group_arrive(*what):
        loop(1, groups, lambda step: group_copy(*what, step, False).wait_recv())

    def group_left(*what):
        loop(1, groups, lambda step: group_copy(*what, step, False).wait_send())

    def pick_fine(index):
        held = jnp.clip(route(index, 2) - group * owned, 0, owned - 1)
        fine_out[index // members, lax.rem(index, members)] = fine_w[held]

    def pick_middle(p):
        middle_send[p] = middle_w[route(group * members + p, 1)]

    loop(0, count, pick_fine)
    fine_trade = (0, lambda other: fine_out.at[other], fine_in)
    group_spread(*fine_trade)
    loop(0, members, pick_middle)
    spread(0, middle_send, middle_block)
    fine_in[group] = fine_out[group]
    middle_block[me] = middle_send[me]

    for r in range(2, outer, 2):
        gather_wait(r)
        pass_on(r)
    for dy, da in peers:
        quad_wait(0, both.at[0, :, 0], docs, dy, da)
        turn(dy, da)

    for r in range(3, outer, 2):
        gather_wait(r)
        pass_on(r)
    for r in range(outer):
        for step in range(1, cores):
            core_copy(r, step, False).wait_recv()

    def block_of(dy, da):
        who = (mirror if dy else group) * members + at_line(0, quad_side(da), core)
        return route(who, 0)

    def coarse_of(k):
        return coarse_w[k].reshape(depth, columns)

    def wide_of(dy, da):
        return jnp.concatenate([docs[dy, da, o] for o in range(outer)], axis=1)

    first = slot == 0
    for dy, da in peers:
        pre_give[dy, da] = dot(wide_of(dy, da), coarse_of(block_of(dy, da))).astype(BF16)
        quad_copy(1, pre_give.at[dy, da], pre_take, dy, da).start()
    def merge_fine(p):
        owner = route(group * members + p, 2) // owned
        fine_send[p] = fine_in[owner, p]

    group_arrive(*fine_trade)
    loop(0, members, merge_fine)
    spread(1, fine_send, fine_block)
    fine_block[me] = fine_send[me]

    pre_own = dot(wide_of(0, 0), coarse_of(block_of(0, 0)))
    pre_other = jnp.zeros_like(pre_own)

    def whole(which):
        return jnp.concatenate([both[which, o, a] for o, a in places], axis=1)

    def compute(block, term):
        weights = block[...].reshape(width, block.shape[-1])
        value, part = level(weights, whole(0), whole(1), flipped[0], flipped[1])
        term[...] = value.reshape(term.shape)
        return part

    middle_own = middle_parts.at[group]
    fine_own = fine_parts.at[group]

    for dy, da in peers:
        quad_wait(1, pre_give.at[0, 0], pre_take, dy, da)
    for dy, da in peers:
        if differs(dy, da):
            pre_other = pre_other + pre_take[dy, da].astype(F32)
        else:
            pre_own = pre_own + pre_take[dy, da].astype(F32)
    hidden, before_grad = gelu_parts(
        jnp.where(first, pre_own, pre_other), jnp.where(first, pre_other, pre_own)
    )
    hidden, before_grad = hidden.astype(F32), before_grad.astype(F32)
    act_give[...] = jnp.where(first, hidden, before_grad).astype(BF16)
    act_keep[...] = jnp.where(first, before_grad, hidden).astype(BF16)
    act_take[0, 0] = act_keep[...]
    for dy, da in peers:
        quad_copy(2, act_give if differs(dy, da) else act_keep, act_take, dy, da).start()

    arrive(0, middle_block)
    total[...] = compute(middle_block, middle_term)
    spread(2, middle_term, middle_own)
    middle_parts[group, me] = middle_term[me]

    arrive(1, fine_block)
    total[...] += compute(fine_block, fine_term)
    spread(3, fine_term, fine_own)
    fine_parts[group, me] = fine_term[me]

    for dy, da in peers:
        quad_wait(2, act_keep, act_take, dy, da)

    for k in range(blocks):
        acts = [
            jnp.where(block_of(dy, da) == k, act_take[dy, da].astype(F32), 0.0).astype(BF16)
            for dy, da in quad
        ]
        value = dot(quad_t[...], jnp.concatenate(acts, axis=0))
        sums[:, :, k] = value.astype(BF16).reshape(outer, cores, rows, columns)

    order = list(range(outer - 1, 0, -2)) + list(range(outer - 2, 0, -2)) + [0]

    def fold_core(r, step):
        there = lax.rem(core + step, cores)
        return to_member(
            sums.at[flip(r), there],
            from_core.at[r, step],
            core_send.at[1, step],
            core_recv.at[1, r, step],
            at_line(0, side, there),
        )

    def fold_line(r, bit):
        return to_member(
            sums.at[flip(r), core],
            from_line.at[r ^ bit, bits.index(bit)],
            fold_send,
            fold_recv.at[r ^ bit, bits.index(bit)],
            at_line(bit, side, core),
        )

    def fold_line_wait(r, bit):
        to_member(
            sums.at[flip(r), core],
            from_line.at[r, bits.index(bit)],
            fold_send,
            fold_recv.at[r, bits.index(bit)],
            at_line(bit, side, core),
        ).wait_recv()

    def lower(r):
        return [bit for bit in reversed(bits) if r == 0 or bit < (r & -r)]

    for r in order:
        for step in range(1, cores):
            fold_core(r, step).start()

    def back_copy(dy, da):
        return quad_copy(3, back_give.at[dy, da], back_take, dy, da)

    @pl.when(first)
    def _():
        for dy, da in peers:
            back_give[dy, da] = dot_transposed(
                act_take[dy, da], coarse_of(block_of(dy, da))
            ).astype(BF16)
            back_copy(dy, da).start()

    def hand_on(target, send_on, recv_on, p, step, landing_own):
        other = lax.rem(group + step, groups)
        landing = group if landing_own else other
        return pltpu.make_async_remote_copy(
            src_ref=target.at[group, p],
            dst_ref=target.at[landing, p],
            send_sem=send_on,
            recv_sem=recv_on,
            device_id={"grp": other},
            device_id_type=MESH,
        )

    def relay(index, source, target, send_on, recv_on, first_step=0, last_step=members):
        own = target.at[group]

        def start(p):
            loop(1, groups, lambda step: hand_on(target, send_on, recv_on, p, step, True).start())

        def body(step):
            p = partner(step)
            member_copy(index, source, own, p, False).wait_recv()
            start(p)

        if first_step == 0:
            start(me)
        loop(max(first_step, 1), last_step, body)

    def relay_done(target, send_on, recv_on):
        if groups > 1:
            all_of(target, groups - 1, recv_on).wait()
            all_of(target, groups - 1, send_on).wait()

    def folded(r):
        value = sums[flip(r), core].astype(F32)
        for step in range(1, cores):
            value = value + from_core[r, step].astype(F32)
        for bit in lower(r):
            value = value + from_line[r, bits.index(bit)].astype(F32)
        return value

    relay(2, middle_term, middle_parts, middle_send_on, middle_recv_on, 0, near)
    for r in order:
        for step in range(1, cores):
            fold_core(r, step).wait_recv()
        for bit in lower(r):
            fold_line_wait(r, bit)
        if r:
            sums[flip(r), core] = folded(r).astype(BF16)
            fold_line(r, r & -r).start()
            if r == 1:
                relay(2, middle_term, middle_parts, middle_send_on, middle_recv_on, near, members)
            if r == order[-2]:
                relay(3, fine_term, fine_parts, fine_send_on, fine_recv_on)
        else:
            coarse_total[...] = folded(0).astype(BF16)

    coarse_trade = (1, lambda other: coarse_total, coarse_parts)
    group_spread(*coarse_trade)
    coarse_parts[group] = coarse_total[...]

    def add_back(dy, da, piece):
        for o in range(outer):
            columns_of = pl.ds(pl.multiple_of((o * sides + quad_side(da)) * span, span), span)
            total[:, columns_of] += piece[:, o * span : (o + 1) * span]

    @pl.when(first)
    def _():
        add_back(0, 0, dot_transposed(act_take[0, 0], coarse_of(block_of(0, 0))))
        for dy, da in peers:
            if not differs(dy, da):
                quad_wait(3, back_give.at[0, 0], back_take, dy, da)
                add_back(dy, da, back_take[dy, da].astype(F32))
        for dy, da in peers:
            back_copy(dy, da).wait_send()

    @pl.when(slot == 1)
    def _():
        for dy, da in peers:
            if differs(dy, da):
                quad_wait(3, back_give.at[0, 0], back_take, dy, da)
                add_back(dy, da, back_take[dy, da].astype(F32))

    tokens_grad[...] = total[...].astype(BF16)
    outs[1].start()
    pltpu.make_async_copy(others, others, path_send).wait()
    for dy, da in peers:
        doc_copy(dy, da).wait_send()
        quad_copy(1, pre_give.at[dy, da], pre_take, dy, da).wait_send()
        quad_copy(2, act_give if differs(dy, da) else act_keep, act_take, dy, da).wait_send()
    for step in range(1, cores):
        some = coarse_w.at[:, :, core]
        pltpu.make_async_copy(some, some, core_send.at[0, step]).wait()
        some = sums.at[:, core]
        pltpu.make_async_copy(some, some, core_send.at[1, step]).wait()
    if outer > 1:
        some = coarse_w.at[:, pl.ds(0, outer - 1), core]
        pltpu.make_async_copy(some, some, gather_send).wait()
        some = sums.at[pl.ds(0, outer - 1), core]
        pltpu.make_async_copy(some, some, fold_send).wait()
    left(0, middle_send)
    left(1, fine_send)
    group_left(*fine_trade)
    left(2, middle_term)
    left(3, fine_term)
    relay_done(middle_parts, middle_send_on, middle_recv_on)
    outs[2].start()
    relay_done(fine_parts, fine_send_on, fine_recv_on)
    outs[3].start()
    group_arrive(*coarse_trade)
    outs[4].start()
    group_left(*coarse_trade)
    for out in outs:
        out.wait()


def exchange(path, tokens, cotangent, coarse_w, middle_w, fine_w, groups, members):
    blocks, rows, wide = coarse_w.shape
    medium, narrow = middle_w.shape[2], fine_w.shape[2]
    token_count, width = tokens.shape
    count = groups * members
    outer, sides, cores = plan(members, rows)
    span = cores * rows
    depth = outer * span
    steps = max(len(bits_of(outer)), 1)
    columns = wide // 2

    def stack(*shape):
        return pltpu.VMEM(shape, BF16)

    def sems(*shape):
        return pltpu.SemaphoreType.DMA(shape)

    vmem = pl.BlockSpec(memory_space=pltpu.VMEM)
    return pl.pallas_call(
        functools.partial(main_kernel, groups, members),
        out_shape=(
            jax.ShapeDtypeStruct((count,) + path.shape, jnp.int32),
            jax.ShapeDtypeStruct(tokens.shape, BF16),
            jax.ShapeDtypeStruct((groups, members, rows, medium), BF16),
            jax.ShapeDtypeStruct((groups, members, rows, narrow), BF16),
            jax.ShapeDtypeStruct((groups, blocks, rows, columns), BF16),
        ),
        in_specs=[vmem] + [pl.BlockSpec(memory_space=pl.ANY)] * 5,
        out_specs=(pl.BlockSpec(memory_space=pl.ANY),) * 5,
        scratch_shapes=[
            pltpu.VMEM((count,) + path.shape, jnp.int32),
            stack(*tokens.shape),
            stack(groups, members, rows, medium),
            stack(groups, members, rows, narrow),
            stack(groups, blocks, rows, columns),
            pltpu.SMEM((count,) + path.shape, jnp.int32),
            stack(2, outer, sides, token_count, span),
            stack(2, sides, outer, token_count, span),
            stack(blocks, outer, cores, rows, columns),
            stack(*middle_w.shape),
            stack(*fine_w.shape),
            stack(members, rows, medium),
            stack(groups, members, rows, narrow),
            stack(groups, members, rows, narrow),
            stack(members, rows, narrow),
            stack(members, rows, medium),
            stack(members, rows, narrow),
            stack(members, rows, medium),
            stack(members, rows, narrow),
            stack(outer, cores, blocks, rows, columns),
            stack(outer, cores, blocks, rows, columns),
            stack(outer, steps, blocks, rows, columns),
            stack(blocks, rows, columns),
            stack(2, width, token_count),
            stack(depth, 2 * sides * token_count),
            pltpu.VMEM((token_count, width), F32),
            stack(2, sides, token_count, columns),
            stack(2, sides, token_count, columns),
            stack(token_count, columns),
            stack(token_count, columns),
            stack(2, sides, token_count, columns),
            stack(2, sides, token_count, depth),
            stack(2, sides, token_count, depth),
            pltpu.SemaphoreType.DMA,
            pltpu.SemaphoreType.DMA,
            sems(4),
            sems(2, members),
            sems(2),
            sems(2, groups),
            sems(2, groups),
            sems(4, 2, sides),
            sems(4, 2, sides),
            pltpu.SemaphoreType.DMA,
            sems(outer),
            sems(2, cores),
            sems(2, outer, cores),
            pltpu.SemaphoreType.DMA,
            sems(outer, steps),
            sems(1),
            sems(3),
            pltpu.SemaphoreType.DMA,
            sems(5),
            pltpu.SemaphoreType.DMA,
            pltpu.SemaphoreType.DMA,
            pltpu.SemaphoreType.DMA,
            pltpu.SemaphoreType.DMA,
        ],
        compiler_params=pltpu.CompilerParams(
            collective_id=0, has_side_effects=True, vmem_limit_bytes=60 * 2**20
        ),
        name="exchange",
    )(path, tokens, cotangent, coarse_w, middle_w, fine_w)


def collect_kernel(
    path_hbm,
    tokens_hbm,
    middle_hbm,
    fine_hbm,
    coarse_hbm,
    tokens_out,
    coarse_out,
    middle_out,
    fine_out,
    path,
    tokens_grad,
    coarse_grad,
    middle_grad,
    fine_grad,
    coarse_parts,
    middle_parts,
    fine_parts,
    middle_sum,
    fine_sum,
    middle_last,
    fine_last,
    load_sem,
    out_sem,
):
    count = middle_parts.shape[0]
    owned = fine_grad.shape[0]
    first_owned = lax.axis_index("grp") * owned
    loads = [
        pltpu.make_async_copy(source, target, load_sem.at[index])
        for index, (source, target) in enumerate(
            (
                (path_hbm, path),
                (middle_hbm, middle_parts),
                (fine_hbm, fine_parts),
                (coarse_hbm, coarse_parts),
                (tokens_hbm, tokens_grad),
            )
        )
    ]
    outs = [
        pltpu.make_async_copy(source, target, out_sem.at[index])
        for index, (source, target) in enumerate(
            (
                (tokens_grad, tokens_out),
                (coarse_grad, coarse_out),
                (middle_grad, middle_out),
                (fine_grad, fine_out),
            )
        )
    ]
    for load in loads:
        load.start()
    for last in (middle_last, fine_last):
        for k in range(last.shape[0]):
            last[k] = count
    middle_grad[...] = jnp.zeros_like(middle_grad)
    middle_sum[count] = jnp.zeros(middle_sum.shape[1:], F32)
    fine_sum[count] = jnp.zeros(fine_sum.shape[1:], F32)
    loads[0].wait()
    loads[1].wait()

    def add_middle(document, carry):
        k = path[document, 0, 1]
        value = middle_parts[document].astype(F32) + middle_sum[middle_last[k]]
        middle_sum[document] = value
        middle_grad[k] = value.astype(BF16)
        middle_last[k] = document
        return carry

    lax.fori_loop(0, count, add_middle, 0)
    outs[2].start()
    fine_grad[...] = jnp.zeros_like(fine_grad)
    loads[2].wait()

    def add_fine(document, carry):
        place = path[document, 0, 2] - first_owned

        @pl.when((place >= 0) & (place < owned))
        def _():
            piece = fine_parts[document].astype(F32) + fine_sum[fine_last[place]]
            fine_sum[document] = piece
            fine_grad[place] = piece.astype(BF16)
            fine_last[place] = document

        return carry

    lax.fori_loop(0, count, add_fine, 0)
    outs[3].start()
    loads[3].wait()
    groups, _, _, columns = coarse_parts.shape
    outer, sides, cores = plan(lax.axis_size("mem"), coarse_grad.shape[1])
    side = lax.rem(lax.axis_index("mem"), sides * cores) // cores
    for s in range(2):
        held = lax.rem(s + (1 - sides % 2) * side, 2)
        value = coarse_parts[held].astype(F32)
        for other in range(2, groups, 2):
            value = value + coarse_parts[held + other].astype(F32)
        coarse_grad[:, :, s * columns : (s + 1) * columns] = value.astype(BF16)
    outs[1].start()
    loads[4].wait()
    outs[0].start()
    for out in outs:
        out.wait()


def collect(paths, tokens_grad, middle_parts, fine_parts, coarse_parts, shapes):
    hbm = pl.BlockSpec(memory_space=pl.ANY)
    count, rows, medium = middle_parts.shape
    narrow = fine_parts.shape[2]
    outs = (tokens_grad.shape,) + shapes
    return pl.pallas_call(
        collect_kernel,
        out_shape=tuple(jax.ShapeDtypeStruct(shape, BF16) for shape in outs),
        in_specs=[hbm] * 5,
        out_specs=(hbm,) * 4,
        scratch_shapes=[pltpu.SMEM(paths.shape, jnp.int32)]
        + [pltpu.VMEM(shape, BF16) for shape in outs]
        + [
            pltpu.VMEM(coarse_parts.shape, BF16),
            pltpu.VMEM(middle_parts.shape, BF16),
            pltpu.VMEM(fine_parts.shape, BF16),
            pltpu.VMEM((count + 1, rows, medium), F32),
            pltpu.VMEM((count + 1, rows, narrow), F32),
            pltpu.SMEM((shapes[1][0],), jnp.int32),
            pltpu.SMEM((shapes[2][0],), jnp.int32),
            pltpu.SemaphoreType.DMA((5,)),
            pltpu.SemaphoreType.DMA((4,)),
        ],
        compiler_params=pltpu.CompilerParams(vmem_limit_bytes=60 * 2**20),
        name="collect",
    )(paths, tokens_grad, middle_parts, fine_parts, coarse_parts)


def on_device(tokens, cotangent, path, coarse_weights, middle_weights, fine_weights):
    members = lax.axis_size("mem")
    groups = lax.axis_size("grp")
    paths, tokens_grad, middle_parts, fine_parts, coarse_parts = exchange(
        path, tokens, cotangent, coarse_weights, middle_weights, fine_weights, groups, members
    )
    flat = lambda parts: parts.reshape((groups * members,) + parts.shape[2:])
    return collect(
        paths,
        tokens_grad,
        flat(middle_parts),
        flat(fine_parts),
        coarse_parts,
        (coarse_weights.shape, middle_weights.shape, fine_weights.shape),
    )


def solution(mesh):
    return jax.shard_map(
        on_device,
        mesh=mesh,
        in_specs=(
            P(("grp", "mem"), None),
            P(("grp", "mem"), None),
            P(("grp", "mem"), None),
            P(None, "mem", None),
            P(None, "mem", None),
            P("grp", "mem", None),
        ),
        out_specs=(
            P(("grp", "mem"), None),
            P(None, "mem", None),
            P(None, "mem", None),
            P("grp", "mem", None),
        ),
        check_vma=False,
    )
```

```python
import functools
import math

import jax
import jax.numpy as jnp
from jax import lax
from jax.experimental import pallas as pl
from jax.experimental.pallas import tpu as pltpu
from jax.sharding import PartitionSpec as P

MESH = pl.DeviceIdType.MESH
LANES = 128
F32 = jnp.float32
BF16 = jnp.bfloat16


def gelu_parts(before, hidden_grad):
    scale = math.sqrt(2.0 / math.pi)
    square = before * before
    tanh = jnp.tanh(scale * (before + 0.044715 * (square * before)))
    half = 0.5 * (1.0 + tanh)
    hidden = before * half
    slope = half + 0.5 * before * (1.0 - tanh * tanh) * (scale * (1.0 + 3 * 0.044715 * square))
    return hidden.astype(BF16), (hidden_grad * slope).astype(BF16)


def dot(left, right):
    return jnp.dot(left, right, preferred_element_type=F32)


def dot_transposed(left, right):
    return lax.dot_general(left, right, (((1,), (1,)), ((), ())), preferred_element_type=F32)


def level(weights, x, g, xt, gt):
    width = weights.shape[1]
    half = width // 2
    if half % LANES == 0:
        up = weights[:, :half]
        down = weights[:, half:]
        hidden, grad = gelu_parts(dot(x, up), dot(g, down))
        term = jnp.concatenate(
            [dot(xt, grad).astype(BF16), dot(gt, hidden).astype(BF16)], axis=1
        )
        return term, dot_transposed(grad, up)
    before = dot(x, weights)
    hidden_grad = pltpu.roll(dot(g, weights), half, 1)
    hidden, grad = gelu_parts(before, hidden_grad)
    first = lax.broadcasted_iota(jnp.int32, grad.shape, 1) < half
    grad = jnp.where(first, grad.astype(F32), 0.0).astype(BF16)
    hidden = jnp.where(first, hidden.astype(F32), 0.0)
    hidden = pltpu.roll(hidden, half, 1).astype(BF16)
    term = (dot(xt, grad) + dot(gt, hidden)).astype(BF16)
    return term, dot_transposed(grad, weights)


def plan(members, rows):
    inner = max(k for k in range(1, math.isqrt(members) + 1) if members % k == 0)
    cores = next(
        k for k in range(1, inner + 1) if inner % k == 0 and (k * rows % LANES == 0 or k == inner)
    )
    return members // inner, inner // cores, cores


def bits_of(outer):
    bits = []
    while outer > 1:
        outer //= 2
        bits.append(outer)
    return bits


def main_kernel(
    groups,
    members,
    path_row,
    tokens_hbm,
    cotangent_hbm,
    coarse_hbm,
    middle_hbm,
    fine_hbm,
    paths_out,
    tokens_out,
    middle_out,
    fine_parts_out,
    coarse_out,
    all_paths,
    tokens_grad,
    middle_parts,
    fine_parts,
    coarse_parts,
    path,
    both,
    docs,
    coarse_w,
    middle_w,
    fine_w,
    middle_send,
    fine_out,
    fine_in,
    fine_send,
    middle_block,
    fine_block,
    middle_term,
    fine_term,
    sums,
    from_core,
    from_line,
    coarse_total,
    flipped,
    quad_t,
    total,
    pre_give,
    pre_take,
    act_keep,
    act_give,
    act_take,
    back_give,
    back_take,
    path_send,
    path_recv,
    mem_send,
    mem_recv,
    weight_recv,
    grp_send,
    grp_recv,
    quad_send,
    quad_recv,
    gather_send,
    gather_recv,
    core_send,
    core_recv,
    fold_send,
    fold_recv,
    local_sem,
    load_sem,
    token_sem,
    out_sem,
    middle_send_on,
    middle_recv_on,
    fine_send_on,
    fine_recv_on,
):
    group = lax.axis_index("grp")
    me = lax.axis_index("mem")
    count = groups * members
    device = group * members + me
    owned = fine_w.shape[0]
    blocks, outer, cores, rows, columns = coarse_w.shape
    _, _, sides, token_count, span = both.shape
    inner = sides * cores
    depth = outer * span
    bits = bits_of(outer)
    line = me // inner
    place = lax.rem(me, inner)
    side = place // cores
    core = lax.rem(place, cores)
    twist = 1 - sides % 2
    slot = lax.rem(group + twist * side, 2)
    mirror = group + 1 - 2 * lax.rem(group, 2)
    width = tokens_grad.shape[1]

    def loop(start, stop, body):
        def wrapped(step, carry):
            body(step)
            return carry

        lax.fori_loop(start, stop, wrapped, 0)

    def flip(r):
        there = line
        for bit in bits:
            if r & bit:
                there = there + bit * (1 - 2 * lax.rem(there // bit, 2))
        return there

    def at_line(r, s, c):
        return flip(r) * inner + s * cores + c

    def to_member(source, target, send, recv, p):
        return pltpu.make_async_remote_copy(
            src_ref=source,
            dst_ref=target,
            send_sem=send,
            recv_sem=recv,
            device_id={"mem": p},
            device_id_type=MESH,
        )

    half = pl.ds(pl.multiple_of(slot * columns, LANES), columns)
    loads = [
        pltpu.make_async_copy(source, target, load_sem.at[index])
        for index, (source, target) in enumerate(
            (
                (coarse_hbm.at[:, :, half], coarse_w.at[:, line, core]),
                (fine_hbm, fine_w),
                (middle_hbm, middle_w),
            )
        )
    ]
    places = [(o, a) for o in range(outer) for a in range(sides)]
    token_loads = [
        pltpu.make_async_copy(
            source.at[:, pl.ds(index * span, span)],
            both.at[which, o, a],
            token_sem,
        )
        for which, source in enumerate((tokens_hbm, cotangent_hbm))
        for index, (o, a) in enumerate(places)
    ]
    loads[0].start()
    for load in token_loads:
        load.start()
    for load in loads[1:]:
        load.start()
    outs = [
        pltpu.make_async_copy(source, target, out_sem.at[index])
        for index, (source, target) in enumerate(
            (
                (all_paths, paths_out),
                (tokens_grad, tokens_out),
                (middle_parts, middle_out),
                (fine_parts, fine_parts_out),
                (coarse_parts, coarse_out),
            )
        )
    ]
    barrier = pltpu.get_barrier_semaphore()

    def anyone(step):
        other = lax.rem(device + step, count)
        return other, (other // members, lax.rem(other, members))

    def greet(step):
        _, where = anyone(step)
        pl.semaphore_signal(barrier, inc=1, device_id=where, device_id_type=MESH)

    loop(1, count, greet)
    loads[0].wait()
    pl.semaphore_wait(barrier, count - 1)

    def path_copy(step):
        _, where = anyone(step)
        return pltpu.make_async_remote_copy(
            src_ref=path_row,
            dst_ref=all_paths.at[device],
            send_sem=path_send,
            recv_sem=path_recv,
            device_id=where,
            device_id_type=MESH,
        )

    loop(1, count, lambda step: path_copy(step).start())
    all_paths[device] = path_row[...]

    quad = [(dy, da) for dy in range(2) for da in range(sides)]
    peers = quad[1:]

    def differs(dy, da):
        return (dy + twist * da) % 2

    def quad_side(da):
        return lax.rem(side + da, sides)

    def quad_copy(stage, source, target, dy, da):
        back_da = (sides - da) % sides
        return pltpu.make_async_remote_copy(
            src_ref=source,
            dst_ref=target.at[dy, back_da],
            send_sem=quad_send.at[stage, dy, da],
            recv_sem=quad_recv.at[stage, dy, back_da],
            device_id=(mirror if dy else group, at_line(0, quad_side(da), core)),
            device_id_type=MESH,
        )

    def quad_wait(stage, source, target, dy, da):
        quad_copy(stage, source, target, dy, (sides - da) % sides).wait_recv()

    def gather_copy(r):
        piece = coarse_w.at[:, line, core]
        return to_member(
            piece, piece, gather_send, gather_recv.at[r], at_line(r, side, core)
        )

    def gather_wait(r):
        piece = coarse_w.at[:, flip(r), core]
        to_member(
            piece, piece, gather_send, gather_recv.at[r], at_line(r, side, core)
        ).wait_recv()

    def core_copy(r, step, landing_own):
        there = lax.rem(core + step, cores)
        landing = core if landing_own else lax.rem(core + cores - step, cores)
        piece = coarse_w.at[:, flip(r), landing]
        return to_member(
            piece, piece, core_send.at[0, step], core_recv.at[0, r, step], at_line(0, side, there)
        )

    def pass_on(r):
        if r == 0:
            for far in range(1, outer):
                gather_copy(far).start()
        for step in range(1, cores):
            core_copy(r, step, True).start()

    def doc_copy(dy, da):
        which = 1 - slot if differs(dy, da) else slot
        return quad_copy(0, both.at[which, :, quad_side(da)], docs, dy, da)

    pass_on(0)
    pltpu.make_async_copy(both, both, token_sem).wait()
    for dy, da in peers:
        doc_copy(dy, da).start()
    for which in range(2):
        for index, (o, a) in enumerate(places):
            flipped[which, index * span : (index + 1) * span, :] = both[which, o, a].T
    docs[0, 0] = both[slot, :, side]
    for load in loads[1:]:
        load.wait()
    if outer > 1:
        gather_wait(1)
        pass_on(1)

    def turn(dy, da):
        q = dy * sides + da
        for o in range(outer):
            quad_t[o * span : (o + 1) * span, q * token_count : (q + 1) * token_count] = docs[
                dy, da, o
            ].T

    turn(0, 0)
    others = all_paths.at[pl.ds(0, count - 1)]
    pltpu.make_async_copy(others, others, path_recv).wait()
    scalars = pltpu.make_async_copy(all_paths, path, local_sem.at[0])
    scalars.start()
    scalars.wait()
    outs[0].start()

    def route(document, column):
        return path[document, 0, column]

    def member_copy(index, source, target, p, landing_own):
        landing = me if landing_own else p
        arrived = weight_recv.at[index] if index < 2 else mem_recv.at[index - 2, landing]
        return to_member(source.at[p], target.at[landing], mem_send.at[index], arrived, p)

    def all_of(ref, number, sem):
        some = ref.at[pl.ds(0, number)]
        return pltpu.make_async_copy(some, some, sem)

    near = outer * cores

    def partner(step):
        there = lax.rem(side + step // near, sides)
        rest = lax.rem(step, near)
        return (
            lax.rem(line + rest // cores, outer) * inner
            + there * cores
            + lax.rem(core + lax.rem(rest, cores), cores)
        )

    def spread(index, source, target, start=1, stop=members):
        loop(
            start,
            stop,
            lambda step: member_copy(index, source, target, partner(step), True).start(),
        )

    def arrive(index, target):
        if members > 1:
            all_of(target, members - 1, weight_recv.at[index]).wait()

    def left(index, source):
        if members > 1:
            all_of(source, members - 1, mem_send.at[index]).wait()

    def group_copy(index, source, target, step, landing_own):
        other = lax.rem(group + step, groups)
        landing = group if landing_own else other
        return pltpu.make_async_remote_copy(
            src_ref=source(other),
            dst_ref=target.at[landing],
            send_sem=grp_send.at[index, other],
            recv_sem=grp_recv.at[index, landing],
            device_id={"grp": other},
            device_id_type=MESH,
        )

    def group_spread(*what):
        loop(1, groups, lambda step: group_copy(*what, step, True).start())

    def group_arrive(*what):
        loop(1, groups, lambda step: group_copy(*what, step, False).wait_recv())

    def group_left(*what):
        loop(1, groups, lambda step: group_copy(*what, step, False).wait_send())

    def pick_fine(index):
        held = jnp.clip(route(index, 2) - group * owned, 0, owned - 1)
        fine_out[index // members, lax.rem(index, members)] = fine_w[held]

    def pick_middle(p):
        middle_send[p] = middle_w[route(group * members + p, 1)]

    loop(0, count, pick_fine)
    fine_trade = (0, lambda other: fine_out.at[other], fine_in)
    group_spread(*fine_trade)
    loop(0, members, pick_middle)
    spread(0, middle_send, middle_block)
    fine_in[group] = fine_out[group]
    middle_block[me] = middle_send[me]

    for r in range(2, outer, 2):
        gather_wait(r)
        pass_on(r)
    for dy, da in peers:
        quad_wait(0, both.at[0, :, 0], docs, dy, da)
        turn(dy, da)

    for r in range(3, outer, 2):
        gather_wait(r)
        pass_on(r)
    for r in range(outer):
        for step in range(1, cores):
            core_copy(r, step, False).wait_recv()

    def block_of(dy, da):
        who = (mirror if dy else group) * members + at_line(0, quad_side(da), core)
        return route(who, 0)

    def coarse_of(k):
        return coarse_w[k].reshape(depth, columns)

    def wide_of(dy, da):
        return jnp.concatenate([docs[dy, da, o] for o in range(outer)], axis=1)

    first = slot == 0
    for dy, da in peers:
        pre_give[dy, da] = dot(wide_of(dy, da), coarse_of(block_of(dy, da))).astype(BF16)
        quad_copy(1, pre_give.at[dy, da], pre_take, dy, da).start()
    def merge_fine(p):
        owner = route(group * members + p, 2) // owned
        fine_send[p] = fine_in[owner, p]

    group_arrive(*fine_trade)
    loop(0, members, merge_fine)
    spread(1, fine_send, fine_block)
    fine_block[me] = fine_send[me]

    pre_own = dot(wide_of(0, 0), coarse_of(block_of(0, 0)))
    pre_other = jnp.zeros_like(pre_own)

    def whole(which):
        return jnp.concatenate([both[which, o, a] for o, a in places], axis=1)

    def compute(block, term):
        weights = block[...].reshape(width, block.shape[-1])
        value, part = level(weights, whole(0), whole(1), flipped[0], flipped[1])
        term[...] = value.reshape(term.shape)
        return part

    middle_own = middle_parts.at[group]
    fine_own = fine_parts.at[group]

    for dy, da in peers:
        quad_wait(1, pre_give.at[0, 0], pre_take, dy, da)
    for dy, da in peers:
        if differs(dy, da):
            pre_other = pre_other + pre_take[dy, da].astype(F32)
        else:
            pre_own = pre_own + pre_take[dy, da].astype(F32)
    hidden, before_grad = gelu_parts(
        jnp.where(first, pre_own, pre_other), jnp.where(first, pre_other, pre_own)
    )
    hidden, before_grad = hidden.astype(F32), before_grad.astype(F32)
    act_give[...] = jnp.where(first, hidden, before_grad).astype(BF16)
    act_keep[...] = jnp.where(first, before_grad, hidden).astype(BF16)
    act_take[0, 0] = act_keep[...]
    for dy, da in peers:
        quad_copy(2, act_give if differs(dy, da) else act_keep, act_take, dy, da).start()

    arrive(0, middle_block)
    total[...] = compute(middle_block, middle_term)
    spread(2, middle_term, middle_own)
    middle_parts[group, me] = middle_term[me]

    for dy, da in peers:
        quad_wait(2, act_keep, act_take, dy, da)

    for k in range(blocks):
        acts = [
            jnp.where(block_of(dy, da) == k, act_take[dy, da].astype(F32), 0.0).astype(BF16)
            for dy, da in quad
        ]
        value = dot(quad_t[...], jnp.concatenate(acts, axis=0))
        sums[:, :, k] = value.astype(BF16).reshape(outer, cores, rows, columns)

    order = list(range(outer - 1, 0, -2)) + list(range(outer - 2, 0, -2)) + [0]

    def fold_core(r, step):
        there = lax.rem(core + step, cores)
        return to_member(
            sums.at[flip(r), there],
            from_core.at[r, step],
            core_send.at[1, step],
            core_recv.at[1, r, step],
            at_line(0, side, there),
        )

    def fold_line(r, bit):
        return to_member(
            sums.at[flip(r), core],
            from_line.at[r ^ bit, bits.index(bit)],
            fold_send,
            fold_recv.at[r ^ bit, bits.index(bit)],
            at_line(bit, side, core),
        )

    def fold_line_wait(r, bit):
        to_member(
            sums.at[flip(r), core],
            from_line.at[r, bits.index(bit)],
            fold_send,
            fold_recv.at[r, bits.index(bit)],
            at_line(bit, side, core),
        ).wait_recv()

    def lower(r):
        return [bit for bit in reversed(bits) if r == 0 or bit < (r & -r)]

    for r in order:
        for step in range(1, cores):
            fold_core(r, step).start()

    def back_copy(dy, da):
        return quad_copy(3, back_give.at[dy, da], back_take, dy, da)

    @pl.when(first)
    def _():
        for dy, da in peers:
            back_give[dy, da] = dot_transposed(
                act_take[dy, da], coarse_of(block_of(dy, da))
            ).astype(BF16)
            back_copy(dy, da).start()

    def hand_on(target, send_on, recv_on, p, step, landing_own):
        other = lax.rem(group + step, groups)
        landing = group if landing_own else other
        return pltpu.make_async_remote_copy(
            src_ref=target.at[group, p],
            dst_ref=target.at[landing, p],
            send_sem=send_on,
            recv_sem=recv_on,
            device_id={"grp": other},
            device_id_type=MESH,
        )

    def relay(index, source, target, send_on, recv_on, first_step=0, last_step=members):
        own = target.at[group]

        def start(p):
            loop(1, groups, lambda step: hand_on(target, send_on, recv_on, p, step, True).start())

        def body(step):
            p = partner(step)
            member_copy(index, source, own, p, False).wait_recv()
            start(p)

        if first_step == 0:
            start(me)
        loop(max(first_step, 1), last_step, body)

    def relay_done(target, send_on, recv_on):
        if groups > 1:
            all_of(target, groups - 1, recv_on).wait()
            all_of(target, groups - 1, send_on).wait()

    def folded(r):
        value = sums[flip(r), core].astype(F32)
        for step in range(1, cores):
            value = value + from_core[r, step].astype(F32)
        for bit in lower(r):
            value = value + from_line[r, bits.index(bit)].astype(F32)
        return value

    arrive(1, fine_block)
    total[...] += compute(fine_block, fine_term)
    spread(3, fine_term, fine_own)
    fine_parts[group, me] = fine_term[me]

    relay(2, middle_term, middle_parts, middle_send_on, middle_recv_on, 0, near)
    for r in order:
        for step in range(1, cores):
            fold_core(r, step).wait_recv()
        for bit in lower(r):
            fold_line_wait(r, bit)
        if r:
            sums[flip(r), core] = folded(r).astype(BF16)
            fold_line(r, r & -r).start()
            if r == 1:
                relay(2, middle_term, middle_parts, middle_send_on, middle_recv_on, near, members)
            if r == order[-2]:
                relay(3, fine_term, fine_parts, fine_send_on, fine_recv_on)
        else:
            coarse_total[...] = folded(0).astype(BF16)

    coarse_trade = (1, lambda other: coarse_total, coarse_parts)
    group_spread(*coarse_trade)
    coarse_parts[group] = coarse_total[...]

    def add_back(dy, da, piece):
        for o in range(outer):
            columns_of = pl.ds(pl.multiple_of((o * sides + quad_side(da)) * span, span), span)
            total[:, columns_of] += piece[:, o * span : (o + 1) * span]

    @pl.when(first)
    def _():
        add_back(0, 0, dot_transposed(act_take[0, 0], coarse_of(block_of(0, 0))))
        for dy, da in peers:
            if not differs(dy, da):
                quad_wait(3, back_give.at[0, 0], back_take, dy, da)
                add_back(dy, da, back_take[dy, da].astype(F32))
        for dy, da in peers:
            back_copy(dy, da).wait_send()

    @pl.when(slot == 1)
    def _():
        for dy, da in peers:
            if differs(dy, da):
                quad_wait(3, back_give.at[0, 0], back_take, dy, da)
                add_back(dy, da, back_take[dy, da].astype(F32))

    tokens_grad[...] = total[...].astype(BF16)
    outs[1].start()
    pltpu.make_async_copy(others, others, path_send).wait()
    for dy, da in peers:
        doc_copy(dy, da).wait_send()
        quad_copy(1, pre_give.at[dy, da], pre_take, dy, da).wait_send()
        quad_copy(2, act_give if differs(dy, da) else act_keep, act_take, dy, da).wait_send()
    for step in range(1, cores):
        some = coarse_w.at[:, :, core]
        pltpu.make_async_copy(some, some, core_send.at[0, step]).wait()
        some = sums.at[:, core]
        pltpu.make_async_copy(some, some, core_send.at[1, step]).wait()
    if outer > 1:
        some = coarse_w.at[:, pl.ds(0, outer - 1), core]
        pltpu.make_async_copy(some, some, gather_send).wait()
        some = sums.at[pl.ds(0, outer - 1), core]
        pltpu.make_async_copy(some, some, fold_send).wait()
    left(0, middle_send)
    left(1, fine_send)
    group_left(*fine_trade)
    left(2, middle_term)
    left(3, fine_term)
    relay_done(middle_parts, middle_send_on, middle_recv_on)
    outs[2].start()
    relay_done(fine_parts, fine_send_on, fine_recv_on)
    outs[3].start()
    group_arrive(*coarse_trade)
    outs[4].start()
    group_left(*coarse_trade)
    for out in outs:
        out.wait()


def exchange(path, tokens, cotangent, coarse_w, middle_w, fine_w, groups, members):
    blocks, rows, wide = coarse_w.shape
    medium, narrow = middle_w.shape[2], fine_w.shape[2]
    token_count, width = tokens.shape
    count = groups * members
    outer, sides, cores = plan(members, rows)
    span = cores * rows
    depth = outer * span
    steps = max(len(bits_of(outer)), 1)
    columns = wide // 2

    def stack(*shape):
        return pltpu.VMEM(shape, BF16)

    def sems(*shape):
        return pltpu.SemaphoreType.DMA(shape)

    vmem = pl.BlockSpec(memory_space=pltpu.VMEM)
    return pl.pallas_call(
        functools.partial(main_kernel, groups, members),
        out_shape=(
            jax.ShapeDtypeStruct((count,) + path.shape, jnp.int32),
            jax.ShapeDtypeStruct(tokens.shape, BF16),
            jax.ShapeDtypeStruct((groups, members, rows, medium), BF16),
            jax.ShapeDtypeStruct((groups, members, rows, narrow), BF16),
            jax.ShapeDtypeStruct((groups, blocks, rows, columns), BF16),
        ),
        in_specs=[vmem] + [pl.BlockSpec(memory_space=pl.ANY)] * 5,
        out_specs=(pl.BlockSpec(memory_space=pl.ANY),) * 5,
        scratch_shapes=[
            pltpu.VMEM((count,) + path.shape, jnp.int32),
            stack(*tokens.shape),
            stack(groups, members, rows, medium),
            stack(groups, members, rows, narrow),
            stack(groups, blocks, rows, columns),
            pltpu.SMEM((count,) + path.shape, jnp.int32),
            stack(2, outer, sides, token_count, span),
            stack(2, sides, outer, token_count, span),
            stack(blocks, outer, cores, rows, columns),
            stack(*middle_w.shape),
            stack(*fine_w.shape),
            stack(members, rows, medium),
            stack(groups, members, rows, narrow),
            stack(groups, members, rows, narrow),
            stack(members, rows, narrow),
            stack(members, rows, medium),
            stack(members, rows, narrow),
            stack(members, rows, medium),
            stack(members, rows, narrow),
            stack(outer, cores, blocks, rows, columns),
            stack(outer, cores, blocks, rows, columns),
            stack(outer, steps, blocks, rows, columns),
            stack(blocks, rows, columns),
            stack(2, width, token_count),
            stack(depth, 2 * sides * token_count),
            pltpu.VMEM((token_count, width), F32),
            stack(2, sides, token_count, columns),
            stack(2, sides, token_count, columns),
            stack(token_count, columns),
            stack(token_count, columns),
            stack(2, sides, token_count, columns),
            stack(2, sides, token_count, depth),
            stack(2, sides, token_count, depth),
            pltpu.SemaphoreType.DMA,
            pltpu.SemaphoreType.DMA,
            sems(4),
            sems(2, members),
            sems(2),
            sems(2, groups),
            sems(2, groups),
            sems(4, 2, sides),
            sems(4, 2, sides),
            pltpu.SemaphoreType.DMA,
            sems(outer),
            sems(2, cores),
            sems(2, outer, cores),
            pltpu.SemaphoreType.DMA,
            sems(outer, steps),
            sems(1),
            sems(3),
            pltpu.SemaphoreType.DMA,
            sems(5),
            pltpu.SemaphoreType.DMA,
            pltpu.SemaphoreType.DMA,
            pltpu.SemaphoreType.DMA,
            pltpu.SemaphoreType.DMA,
        ],
        compiler_params=pltpu.CompilerParams(
            collective_id=0, has_side_effects=True, vmem_limit_bytes=60 * 2**20
        ),
        name="exchange",
    )(path, tokens, cotangent, coarse_w, middle_w, fine_w)


def collect_kernel(
    path_hbm,
    tokens_hbm,
    middle_hbm,
    fine_hbm,
    coarse_hbm,
    tokens_out,
    coarse_out,
    middle_out,
    fine_out,
    path,
    tokens_grad,
    coarse_grad,
    middle_grad,
    fine_grad,
    coarse_parts,
    middle_parts,
    fine_parts,
    middle_sum,
    fine_sum,
    middle_last,
    fine_last,
    load_sem,
    out_sem,
):
    count = middle_parts.shape[0]
    owned = fine_grad.shape[0]
    first_owned = lax.axis_index("grp") * owned
    loads = [
        pltpu.make_async_copy(source, target, load_sem.at[index])
        for index, (source, target) in enumerate(
            (
                (path_hbm, path),
                (middle_hbm, middle_parts),
                (fine_hbm, fine_parts),
                (coarse_hbm, coarse_parts),
                (tokens_hbm, tokens_grad),
            )
        )
    ]
    outs = [
        pltpu.make_async_copy(source, target, out_sem.at[index])
        for index, (source, target) in enumerate(
            (
                (tokens_grad, tokens_out),
                (coarse_grad, coarse_out),
                (middle_grad, middle_out),
                (fine_grad, fine_out),
            )
        )
    ]
    for load in loads:
        load.start()
    for last in (middle_last, fine_last):
        for k in range(last.shape[0]):
            last[k] = count
    middle_grad[...] = jnp.zeros_like(middle_grad)
    middle_sum[count] = jnp.zeros(middle_sum.shape[1:], F32)
    fine_sum[count] = jnp.zeros(fine_sum.shape[1:], F32)
    loads[0].wait()
    loads[1].wait()

    def add_middle(document, carry):
        k = path[document, 0, 1]
        value = middle_parts[document].astype(F32) + middle_sum[middle_last[k]]
        middle_sum[document] = value
        middle_grad[k] = value.astype(BF16)
        middle_last[k] = document
        return carry

    lax.fori_loop(0, count, add_middle, 0)
    outs[2].start()
    fine_grad[...] = jnp.zeros_like(fine_grad)
    loads[2].wait()

    def add_fine(document, carry):
        place = path[document, 0, 2] - first_owned

        @pl.when((place >= 0) & (place < owned))
        def _():
            piece = fine_parts[document].astype(F32) + fine_sum[fine_last[place]]
            fine_sum[document] = piece
            fine_grad[place] = piece.astype(BF16)
            fine_last[place] = document

        return carry

    lax.fori_loop(0, count, add_fine, 0)
    outs[3].start()
    loads[3].wait()
    groups, _, _, columns = coarse_parts.shape
    outer, sides, cores = plan(lax.axis_size("mem"), coarse_grad.shape[1])
    side = lax.rem(lax.axis_index("mem"), sides * cores) // cores
    for s in range(2):
        held = lax.rem(s + (1 - sides % 2) * side, 2)
        value = coarse_parts[held].astype(F32)
        for other in range(2, groups, 2):
            value = value + coarse_parts[held + other].astype(F32)
        coarse_grad[:, :, s * columns : (s + 1) * columns] = value.astype(BF16)
    outs[1].start()
    loads[4].wait()
    outs[0].start()
    for out in outs:
        out.wait()


def collect(paths, tokens_grad, middle_parts, fine_parts, coarse_parts, shapes):
    hbm = pl.BlockSpec(memory_space=pl.ANY)
    count, rows, medium = middle_parts.shape
    narrow = fine_parts.shape[2]
    outs = (tokens_grad.shape,) + shapes
    return pl.pallas_call(
        collect_kernel,
        out_shape=tuple(jax.ShapeDtypeStruct(shape, BF16) for shape in outs),
        in_specs=[hbm] * 5,
        out_specs=(hbm,) * 4,
        scratch_shapes=[pltpu.SMEM(paths.shape, jnp.int32)]
        + [pltpu.VMEM(shape, BF16) for shape in outs]
        + [
            pltpu.VMEM(coarse_parts.shape, BF16),
            pltpu.VMEM(middle_parts.shape, BF16),
            pltpu.VMEM(fine_parts.shape, BF16),
            pltpu.VMEM((count + 1, rows, medium), F32),
            pltpu.VMEM((count + 1, rows, narrow), F32),
            pltpu.SMEM((shapes[1][0],), jnp.int32),
            pltpu.SMEM((shapes[2][0],), jnp.int32),
            pltpu.SemaphoreType.DMA((5,)),
            pltpu.SemaphoreType.DMA((4,)),
        ],
        compiler_params=pltpu.CompilerParams(vmem_limit_bytes=60 * 2**20),
        name="collect",
    )(paths, tokens_grad, middle_parts, fine_parts, coarse_parts)


def on_device(tokens, cotangent, path, coarse_weights, middle_weights, fine_weights):
    members = lax.axis_size("mem")
    groups = lax.axis_size("grp")
    paths, tokens_grad, middle_parts, fine_parts, coarse_parts = exchange(
        path, tokens, cotangent, coarse_weights, middle_weights, fine_weights, groups, members
    )
    flat = lambda parts: parts.reshape((groups * members,) + parts.shape[2:])
    return collect(
        paths,
        tokens_grad,
        flat(middle_parts),
        flat(fine_parts),
        coarse_parts,
        (coarse_weights.shape, middle_weights.shape, fine_weights.shape),
    )


def solution(mesh):
    return jax.shard_map(
        on_device,
        mesh=mesh,
        in_specs=(
            P(("grp", "mem"), None),
            P(("grp", "mem"), None),
            P(("grp", "mem"), None),
            P(None, "mem", None),
            P(None, "mem", None),
            P("grp", "mem", None),
        ),
        out_specs=(
            P(("grp", "mem"), None),
            P(None, "mem", None),
            P(None, "mem", None),
            P("grp", "mem", None),
        ),
        check_vma=False,
    )
```

```python
import functools
import math

import jax
import jax.numpy as jnp
from jax import lax
from jax.experimental import pallas as pl
from jax.experimental.pallas import tpu as pltpu
from jax.sharding import PartitionSpec as P

MESH = pl.DeviceIdType.MESH
LANES = 128
F32 = jnp.float32
BF16 = jnp.bfloat16


def gelu_parts(before, hidden_grad):
    scale = math.sqrt(2.0 / math.pi)
    square = before * before
    tanh = jnp.tanh(scale * (before + 0.044715 * (square * before)))
    half = 0.5 * (1.0 + tanh)
    hidden = before * half
    slope = half + 0.5 * before * (1.0 - tanh * tanh) * (scale * (1.0 + 3 * 0.044715 * square))
    return hidden.astype(BF16), (hidden_grad * slope).astype(BF16)


def dot(left, right):
    return jnp.dot(left, right, preferred_element_type=F32)


def dot_transposed(left, right):
    return lax.dot_general(left, right, (((1,), (1,)), ((), ())), preferred_element_type=F32)


def level(weights, x, g, xt, gt):
    width = weights.shape[1]
    half = width // 2
    if half % LANES == 0:
        up = weights[:, :half]
        down = weights[:, half:]
        hidden, grad = gelu_parts(dot(x, up), dot(g, down))
        term = jnp.concatenate(
            [dot(xt, grad).astype(BF16), dot(gt, hidden).astype(BF16)], axis=1
        )
        return term, dot_transposed(grad, up)
    before = dot(x, weights)
    hidden_grad = pltpu.roll(dot(g, weights), half, 1)
    hidden, grad = gelu_parts(before, hidden_grad)
    first = lax.broadcasted_iota(jnp.int32, grad.shape, 1) < half
    grad = jnp.where(first, grad.astype(F32), 0.0).astype(BF16)
    hidden = jnp.where(first, hidden.astype(F32), 0.0)
    hidden = pltpu.roll(hidden, half, 1).astype(BF16)
    term = (dot(xt, grad) + dot(gt, hidden)).astype(BF16)
    return term, dot_transposed(grad, weights)


def plan(members, rows):
    inner = max(k for k in range(1, math.isqrt(members) + 1) if members % k == 0)
    cores = next(
        k for k in range(1, inner + 1) if inner % k == 0 and (k * rows % LANES == 0 or k == inner)
    )
    return members // inner, inner // cores, cores


def bits_of(outer):
    bits = []
    while outer > 1:
        outer //= 2
        bits.append(outer)
    return bits


def main_kernel(
    groups,
    members,
    path_row,
    tokens_hbm,
    cotangent_hbm,
    coarse_hbm,
    middle_hbm,
    fine_hbm,
    paths_out,
    tokens_out,
    middle_out,
    fine_parts_out,
    coarse_out,
    all_paths,
    tokens_grad,
    middle_parts,
    fine_parts,
    coarse_parts,
    path,
    both,
    docs,
    coarse_w,
    middle_w,
    fine_w,
    middle_send,
    fine_out,
    fine_in,
    fine_send,
    middle_block,
    fine_block,
    middle_term,
    fine_term,
    sums,
    from_core,
    from_line,
    coarse_total,
    flipped,
    quad_t,
    total,
    pre_give,
    pre_take,
    act_keep,
    act_give,
    act_take,
    back_give,
    back_take,
    path_send,
    path_recv,
    mem_send,
    mem_recv,
    weight_recv,
    grp_send,
    grp_recv,
    quad_send,
    quad_recv,
    gather_send,
    gather_recv,
    core_send,
    core_recv,
    fold_send,
    fold_recv,
    local_sem,
    load_sem,
    token_sem,
    out_sem,
    middle_send_on,
    middle_recv_on,
    fine_send_on,
    fine_recv_on,
):
    group = lax.axis_index("grp")
    me = lax.axis_index("mem")
    count = groups * members
    device = group * members + me
    owned = fine_w.shape[0]
    blocks, outer, cores, rows, columns = coarse_w.shape
    _, _, sides, token_count, span = both.shape
    inner = sides * cores
    depth = outer * span
    bits = bits_of(outer)
    line = me // inner
    place = lax.rem(me, inner)
    side = place // cores
    core = lax.rem(place, cores)
    twist = 1 - sides % 2
    slot = lax.rem(group + twist * side, 2)
    mirror = group + 1 - 2 * lax.rem(group, 2)
    width = tokens_grad.shape[1]

    def loop(start, stop, body):
        def wrapped(step, carry):
            body(step)
            return carry

        lax.fori_loop(start, stop, wrapped, 0)

    def flip(r):
        there = line
        for bit in bits:
            if r & bit:
                there = there + bit * (1 - 2 * lax.rem(there // bit, 2))
        return there

    def at_line(r, s, c):
        return flip(r) * inner + s * cores + c

    def to_member(source, target, send, recv, p):
        return pltpu.make_async_remote_copy(
            src_ref=source,
            dst_ref=target,
            send_sem=send,
            recv_sem=recv,
            device_id={"mem": p},
            device_id_type=MESH,
        )

    half = pl.ds(pl.multiple_of(slot * columns, LANES), columns)
    loads = [
        pltpu.make_async_copy(source, target, load_sem.at[index])
        for index, (source, target) in enumerate(
            (
                (coarse_hbm.at[:, :, half], coarse_w.at[:, line, core]),
                (fine_hbm, fine_w),
                (middle_hbm, middle_w),
            )
        )
    ]
    places = [(o, a) for o in range(outer) for a in range(sides)]
    token_loads = [
        pltpu.make_async_copy(
            source.at[:, pl.ds(index * span, span)],
            both.at[which, o, a],
            token_sem,
        )
        for which, source in enumerate((tokens_hbm, cotangent_hbm))
        for index, (o, a) in enumerate(places)
    ]
    loads[0].start()
    for load in token_loads:
        load.start()
    for load in loads[1:]:
        load.start()
    outs = [
        pltpu.make_async_copy(source, target, out_sem.at[index])
        for index, (source, target) in enumerate(
            (
                (all_paths, paths_out),
                (tokens_grad, tokens_out),
                (middle_parts, middle_out),
                (fine_parts, fine_parts_out),
                (coarse_parts, coarse_out),
            )
        )
    ]
    barrier = pltpu.get_barrier_semaphore()

    def anyone(step):
        other = lax.rem(device + step, count)
        return other, (other // members, lax.rem(other, members))

    def greet(step):
        _, where = anyone(step)
        pl.semaphore_signal(barrier, inc=1, device_id=where, device_id_type=MESH)

    loop(1, count, greet)
    loads[0].wait()
    pl.semaphore_wait(barrier, count - 1)

    def path_copy(step):
        _, where = anyone(step)
        return pltpu.make_async_remote_copy(
            src_ref=path_row,
            dst_ref=all_paths.at[device],
            send_sem=path_send,
            recv_sem=path_recv,
            device_id=where,
            device_id_type=MESH,
        )

    loop(1, count, lambda step: path_copy(step).start())
    all_paths[device] = path_row[...]

    quad = [(dy, da) for dy in range(2) for da in range(sides)]
    peers = quad[1:]

    def differs(dy, da):
        return (dy + twist * da) % 2

    def quad_side(da):
        return lax.rem(side + da, sides)

    def quad_copy(stage, source, target, dy, da):
        back_da = (sides - da) % sides
        return pltpu.make_async_remote_copy(
            src_ref=source,
            dst_ref=target.at[dy, back_da],
            send_sem=quad_send.at[stage, dy, da],
            recv_sem=quad_recv.at[stage, dy, back_da],
            device_id=(mirror if dy else group, at_line(0, quad_side(da), core)),
            device_id_type=MESH,
        )

    def quad_wait(stage, source, target, dy, da):
        quad_copy(stage, source, target, dy, (sides - da) % sides).wait_recv()

    def gather_copy(r):
        piece = coarse_w.at[:, line, core]
        return to_member(
            piece, piece, gather_send, gather_recv.at[r], at_line(r, side, core)
        )

    def gather_wait(r):
        piece = coarse_w.at[:, flip(r), core]
        to_member(
            piece, piece, gather_send, gather_recv.at[r], at_line(r, side, core)
        ).wait_recv()

    def core_copy(r, step, landing_own):
        there = lax.rem(core + step, cores)
        landing = core if landing_own else lax.rem(core + cores - step, cores)
        piece = coarse_w.at[:, flip(r), landing]
        return to_member(
            piece, piece, core_send.at[0, step], core_recv.at[0, r, step], at_line(0, side, there)
        )

    def pass_on(r):
        if r == 0:
            for far in range(1, outer):
                gather_copy(far).start()
        for step in range(1, cores):
            core_copy(r, step, True).start()

    def doc_copy(dy, da):
        which = 1 - slot if differs(dy, da) else slot
        return quad_copy(0, both.at[which, :, quad_side(da)], docs, dy, da)

    pass_on(0)
    pltpu.make_async_copy(both, both, token_sem).wait()
    for dy, da in peers:
        doc_copy(dy, da).start()
    for which in range(2):
        for index, (o, a) in enumerate(places):
            flipped[which, index * span : (index + 1) * span, :] = both[which, o, a].T
    docs[0, 0] = both[slot, :, side]
    for load in loads[1:]:
        load.wait()
    if outer > 1:
        gather_wait(1)
        pass_on(1)

    def turn(dy, da):
        q = dy * sides + da
        for o in range(outer):
            quad_t[o * span : (o + 1) * span, q * token_count : (q + 1) * token_count] = docs[
                dy, da, o
            ].T

    turn(0, 0)
    others = all_paths.at[pl.ds(0, count - 1)]
    pltpu.make_async_copy(others, others, path_recv).wait()
    scalars = pltpu.make_async_copy(all_paths, path, local_sem.at[0])
    scalars.start()
    scalars.wait()
    outs[0].start()

    def route(document, column):
        return path[document, 0, column]

    def member_copy(index, source, target, p, landing_own):
        landing = me if landing_own else p
        arrived = weight_recv.at[index] if index < 2 else mem_recv.at[index - 2, landing]
        return to_member(source.at[p], target.at[landing], mem_send.at[index], arrived, p)

    def all_of(ref, number, sem):
        some = ref.at[pl.ds(0, number)]
        return pltpu.make_async_copy(some, some, sem)

    near = outer * cores

    def partner(step):
        there = lax.rem(side + step // near, sides)
        rest = lax.rem(step, near)
        return (
            lax.rem(line + rest // cores, outer) * inner
            + there * cores
            + lax.rem(core + lax.rem(rest, cores), cores)
        )

    def spread(index, source, target, start=1, stop=members):
        loop(
            start,
            stop,
            lambda step: member_copy(index, source, target, partner(step), True).start(),
        )

    def arrive(index, target):
        if members > 1:
            all_of(target, members - 1, weight_recv.at[index]).wait()

    def left(index, source):
        if members > 1:
            all_of(source, members - 1, mem_send.at[index]).wait()

    def group_copy(index, source, target, step, landing_own):
        other = lax.rem(group + step, groups)
        landing = group if landing_own else other
        return pltpu.make_async_remote_copy(
            src_ref=source(other),
            dst_ref=target.at[landing],
            send_sem=grp_send.at[index, other],
            recv_sem=grp_recv.at[index, landing],
            device_id={"grp": other},
            device_id_type=MESH,
        )

    def group_spread(*what):
        loop(1, groups, lambda step: group_copy(*what, step, True).start())

    def group_arrive(*what):
        loop(1, groups, lambda step: group_copy(*what, step, False).wait_recv())

    def group_left(*what):
        loop(1, groups, lambda step: group_copy(*what, step, False).wait_send())

    def pick_fine(index):
        held = jnp.clip(route(index, 2) - group * owned, 0, owned - 1)
        fine_out[index // members, lax.rem(index, members)] = fine_w[held]

    def pick_middle(p):
        middle_send[p] = middle_w[route(group * members + p, 1)]

    loop(0, count, pick_fine)
    fine_trade = (0, lambda other: fine_out.at[other], fine_in)
    group_spread(*fine_trade)
    loop(0, members, pick_middle)
    spread(0, middle_send, middle_block)
    fine_in[group] = fine_out[group]
    middle_block[me] = middle_send[me]

    for r in range(2, outer, 2):
        gather_wait(r)
        pass_on(r)
    for dy, da in peers:
        quad_wait(0, both.at[0, :, 0], docs, dy, da)
        turn(dy, da)

    for r in range(3, outer, 2):
        gather_wait(r)
        pass_on(r)
    for r in range(outer):
        for step in range(1, cores):
            core_copy(r, step, False).wait_recv()

    def block_of(dy, da):
        who = (mirror if dy else group) * members + at_line(0, quad_side(da), core)
        return route(who, 0)

    def coarse_of(k):
        return coarse_w[k].reshape(depth, columns)

    def wide_of(dy, da):
        return jnp.concatenate([docs[dy, da, o] for o in range(outer)], axis=1)

    first = slot == 0
    for dy, da in peers:
        pre_give[dy, da] = dot(wide_of(dy, da), coarse_of(block_of(dy, da))).astype(BF16)
        quad_copy(1, pre_give.at[dy, da], pre_take, dy, da).start()
    def merge_fine(p):
        owner = route(group * members + p, 2) // owned
        fine_send[p] = fine_in[owner, p]

    group_arrive(*fine_trade)
    loop(0, members, merge_fine)
    spread(1, fine_send, fine_block)
    fine_block[me] = fine_send[me]

    pre_own = dot(wide_of(0, 0), coarse_of(block_of(0, 0)))
    pre_other = jnp.zeros_like(pre_own)

    def whole(which):
        return jnp.concatenate([both[which, o, a] for o, a in places], axis=1)

    def compute(block, term):
        weights = block[...].reshape(width, block.shape[-1])
        value, part = level(weights, whole(0), whole(1), flipped[0], flipped[1])
        term[...] = value.reshape(term.shape)
        return part

    middle_own = middle_parts.at[group]
    fine_own = fine_parts.at[group]

    for dy, da in peers:
        quad_wait(1, pre_give.at[0, 0], pre_take, dy, da)
    for dy, da in peers:
        if differs(dy, da):
            pre_other = pre_other + pre_take[dy, da].astype(F32)
        else:
            pre_own = pre_own + pre_take[dy, da].astype(F32)
    hidden, before_grad = gelu_parts(
        jnp.where(first, pre_own, pre_other), jnp.where(first, pre_other, pre_own)
    )
    hidden, before_grad = hidden.astype(F32), before_grad.astype(F32)
    act_give[...] = jnp.where(first, hidden, before_grad).astype(BF16)
    act_keep[...] = jnp.where(first, before_grad, hidden).astype(BF16)
    act_take[0, 0] = act_keep[...]
    for dy, da in peers:
        quad_copy(2, act_give if differs(dy, da) else act_keep, act_take, dy, da).start()

    arrive(0, middle_block)
    total[...] = compute(middle_block, middle_term)
    spread(2, middle_term, middle_own)
    middle_parts[group, me] = middle_term[me]

    for dy, da in peers:
        quad_wait(2, act_keep, act_take, dy, da)

    for k in range(blocks):
        acts = [
            jnp.where(block_of(dy, da) == k, act_take[dy, da].astype(F32), 0.0).astype(BF16)
            for dy, da in quad
        ]
        value = dot(quad_t[...], jnp.concatenate(acts, axis=0))
        sums[:, :, k] = value.astype(BF16).reshape(outer, cores, rows, columns)

    order = list(range(outer - 1, 0, -2)) + list(range(outer - 2, 0, -2)) + [0]

    def fold_core(r, step):
        there = lax.rem(core + step, cores)
        return to_member(
            sums.at[flip(r), there],
            from_core.at[r, step],
            core_send.at[1, step],
            core_recv.at[1, r, step],
            at_line(0, side, there),
        )

    def fold_line(r, bit):
        return to_member(
            sums.at[flip(r), core],
            from_line.at[r ^ bit, bits.index(bit)],
            fold_send,
            fold_recv.at[r ^ bit, bits.index(bit)],
            at_line(bit, side, core),
        )

    def fold_line_wait(r, bit):
        to_member(
            sums.at[flip(r), core],
            from_line.at[r, bits.index(bit)],
            fold_send,
            fold_recv.at[r, bits.index(bit)],
            at_line(bit, side, core),
        ).wait_recv()

    def lower(r):
        return [bit for bit in reversed(bits) if r == 0 or bit < (r & -r)]

    for r in order:
        for step in range(1, cores):
            fold_core(r, step).start()

    def back_copy(dy, da):
        return quad_copy(3, back_give.at[dy, da], back_take, dy, da)

    @pl.when(first)
    def _():
        for dy, da in peers:
            back_give[dy, da] = dot_transposed(
                act_take[dy, da], coarse_of(block_of(dy, da))
            ).astype(BF16)
            back_copy(dy, da).start()

    def hand_on(target, send_on, recv_on, p, step, landing_own):
        other = lax.rem(group + step, groups)
        landing = group if landing_own else other
        return pltpu.make_async_remote_copy(
            src_ref=target.at[group, p],
            dst_ref=target.at[landing, p],
            send_sem=send_on,
            recv_sem=recv_on,
            device_id={"grp": other},
            device_id_type=MESH,
        )

    def relay(index, source, target, send_on, recv_on, first_step=0, last_step=members):
        own = target.at[group]

        def start(p):
            loop(1, groups, lambda step: hand_on(target, send_on, recv_on, p, step, True).start())

        def body(step):
            p = partner(step)
            member_copy(index, source, own, p, False).wait_recv()
            start(p)

        if first_step == 0:
            start(me)
        loop(max(first_step, 1), last_step, body)

    def relay_done(target, send_on, recv_on):
        if groups > 1:
            all_of(target, groups - 1, recv_on).wait()
            all_of(target, groups - 1, send_on).wait()

    def folded(r):
        value = sums[flip(r), core].astype(F32)
        for step in range(1, cores):
            value = value + from_core[r, step].astype(F32)
        for bit in lower(r):
            value = value + from_line[r, bits.index(bit)].astype(F32)
        return value

    arrive(1, fine_block)
    total[...] += compute(fine_block, fine_term)
    spread(3, fine_term, fine_own)
    fine_parts[group, me] = fine_term[me]

    relay(2, middle_term, middle_parts, middle_send_on, middle_recv_on, 0, near)
    for r in order:
        for step in range(1, cores):
            fold_core(r, step).wait_recv()
        for bit in lower(r):
            fold_line_wait(r, bit)
        if r:
            sums[flip(r), core] = folded(r).astype(BF16)
            fold_line(r, r & -r).start()
            if r == order[0]:
                relay(2, middle_term, middle_parts, middle_send_on, middle_recv_on, near, members)
            if r == order[-2]:
                relay(3, fine_term, fine_parts, fine_send_on, fine_recv_on)
        else:
            coarse_total[...] = folded(0).astype(BF16)

    coarse_trade = (1, lambda other: coarse_total, coarse_parts)
    group_spread(*coarse_trade)
    coarse_parts[group] = coarse_total[...]

    def add_back(dy, da, piece):
        for o in range(outer):
            columns_of = pl.ds(pl.multiple_of((o * sides + quad_side(da)) * span, span), span)
            total[:, columns_of] += piece[:, o * span : (o + 1) * span]

    @pl.when(first)
    def _():
        add_back(0, 0, dot_transposed(act_take[0, 0], coarse_of(block_of(0, 0))))
        for dy, da in peers:
            if not differs(dy, da):
                quad_wait(3, back_give.at[0, 0], back_take, dy, da)
                add_back(dy, da, back_take[dy, da].astype(F32))
        for dy, da in peers:
            back_copy(dy, da).wait_send()

    @pl.when(slot == 1)
    def _():
        for dy, da in peers:
            if differs(dy, da):
                quad_wait(3, back_give.at[0, 0], back_take, dy, da)
                add_back(dy, da, back_take[dy, da].astype(F32))

    tokens_grad[...] = total[...].astype(BF16)
    outs[1].start()
    pltpu.make_async_copy(others, others, path_send).wait()
    for dy, da in peers:
        doc_copy(dy, da).wait_send()
        quad_copy(1, pre_give.at[dy, da], pre_take, dy, da).wait_send()
        quad_copy(2, act_give if differs(dy, da) else act_keep, act_take, dy, da).wait_send()
    for step in range(1, cores):
        some = coarse_w.at[:, :, core]
        pltpu.make_async_copy(some, some, core_send.at[0, step]).wait()
        some = sums.at[:, core]
        pltpu.make_async_copy(some, some, core_send.at[1, step]).wait()
    if outer > 1:
        some = coarse_w.at[:, pl.ds(0, outer - 1), core]
        pltpu.make_async_copy(some, some, gather_send).wait()
        some = sums.at[pl.ds(0, outer - 1), core]
        pltpu.make_async_copy(some, some, fold_send).wait()
    left(0, middle_send)
    left(1, fine_send)
    group_left(*fine_trade)
    left(2, middle_term)
    left(3, fine_term)
    relay_done(middle_parts, middle_send_on, middle_recv_on)
    outs[2].start()
    relay_done(fine_parts, fine_send_on, fine_recv_on)
    outs[3].start()
    group_arrive(*coarse_trade)
    outs[4].start()
    group_left(*coarse_trade)
    for out in outs:
        out.wait()


def exchange(path, tokens, cotangent, coarse_w, middle_w, fine_w, groups, members):
    blocks, rows, wide = coarse_w.shape
    medium, narrow = middle_w.shape[2], fine_w.shape[2]
    token_count, width = tokens.shape
    count = groups * members
    outer, sides, cores = plan(members, rows)
    span = cores * rows
    depth = outer * span
    steps = max(len(bits_of(outer)), 1)
    columns = wide // 2

    def stack(*shape):
        return pltpu.VMEM(shape, BF16)

    def sems(*shape):
        return pltpu.SemaphoreType.DMA(shape)

    vmem = pl.BlockSpec(memory_space=pltpu.VMEM)
    return pl.pallas_call(
        functools.partial(main_kernel, groups, members),
        out_shape=(
            jax.ShapeDtypeStruct((count,) + path.shape, jnp.int32),
            jax.ShapeDtypeStruct(tokens.shape, BF16),
            jax.ShapeDtypeStruct((groups, members, rows, medium), BF16),
            jax.ShapeDtypeStruct((groups, members, rows, narrow), BF16),
            jax.ShapeDtypeStruct((groups, blocks, rows, columns), BF16),
        ),
        in_specs=[vmem] + [pl.BlockSpec(memory_space=pl.ANY)] * 5,
        out_specs=(pl.BlockSpec(memory_space=pl.ANY),) * 5,
        scratch_shapes=[
            pltpu.VMEM((count,) + path.shape, jnp.int32),
            stack(*tokens.shape),
            stack(groups, members, rows, medium),
            stack(groups, members, rows, narrow),
            stack(groups, blocks, rows, columns),
            pltpu.SMEM((count,) + path.shape, jnp.int32),
            stack(2, outer, sides, token_count, span),
            stack(2, sides, outer, token_count, span),
            stack(blocks, outer, cores, rows, columns),
            stack(*middle_w.shape),
            stack(*fine_w.shape),
            stack(members, rows, medium),
            stack(groups, members, rows, narrow),
            stack(groups, members, rows, narrow),
            stack(members, rows, narrow),
            stack(members, rows, medium),
            stack(members, rows, narrow),
            stack(members, rows, medium),
            stack(members, rows, narrow),
            stack(outer, cores, blocks, rows, columns),
            stack(outer, cores, blocks, rows, columns),
            stack(outer, steps, blocks, rows, columns),
            stack(blocks, rows, columns),
            stack(2, width, token_count),
            stack(depth, 2 * sides * token_count),
            pltpu.VMEM((token_count, width), F32),
            stack(2, sides, token_count, columns),
            stack(2, sides, token_count, columns),
            stack(token_count, columns),
            stack(token_count, columns),
            stack(2, sides, token_count, columns),
            stack(2, sides, token_count, depth),
            stack(2, sides, token_count, depth),
            pltpu.SemaphoreType.DMA,
            pltpu.SemaphoreType.DMA,
            sems(4),
            sems(2, members),
            sems(2),
            sems(2, groups),
            sems(2, groups),
            sems(4, 2, sides),
            sems(4, 2, sides),
            pltpu.SemaphoreType.DMA,
            sems(outer),
            sems(2, cores),
            sems(2, outer, cores),
            pltpu.SemaphoreType.DMA,
            sems(outer, steps),
            sems(1),
            sems(3),
            pltpu.SemaphoreType.DMA,
            sems(5),
            pltpu.SemaphoreType.DMA,
            pltpu.SemaphoreType.DMA,
            pltpu.SemaphoreType.DMA,
            pltpu.SemaphoreType.DMA,
        ],
        compiler_params=pltpu.CompilerParams(
            collective_id=0, has_side_effects=True, vmem_limit_bytes=60 * 2**20
        ),
        name="exchange",
    )(path, tokens, cotangent, coarse_w, middle_w, fine_w)


def collect_kernel(
    path_hbm,
    tokens_hbm,
    middle_hbm,
    fine_hbm,
    coarse_hbm,
    tokens_out,
    coarse_out,
    middle_out,
    fine_out,
    path,
    tokens_grad,
    coarse_grad,
    middle_grad,
    fine_grad,
    coarse_parts,
    middle_parts,
    fine_parts,
    middle_sum,
    fine_sum,
    middle_last,
    fine_last,
    load_sem,
    out_sem,
):
    count = middle_parts.shape[0]
    owned = fine_grad.shape[0]
    first_owned = lax.axis_index("grp") * owned
    loads = [
        pltpu.make_async_copy(source, target, load_sem.at[index])
        for index, (source, target) in enumerate(
            (
                (path_hbm, path),
                (middle_hbm, middle_parts),
                (fine_hbm, fine_parts),
                (coarse_hbm, coarse_parts),
                (tokens_hbm, tokens_grad),
            )
        )
    ]
    outs = [
        pltpu.make_async_copy(source, target, out_sem.at[index])
        for index, (source, target) in enumerate(
            (
                (tokens_grad, tokens_out),
                (coarse_grad, coarse_out),
                (middle_grad, middle_out),
                (fine_grad, fine_out),
            )
        )
    ]
    for load in loads:
        load.start()
    for last in (middle_last, fine_last):
        for k in range(last.shape[0]):
            last[k] = count
    middle_grad[...] = jnp.zeros_like(middle_grad)
    middle_sum[count] = jnp.zeros(middle_sum.shape[1:], F32)
    fine_sum[count] = jnp.zeros(fine_sum.shape[1:], F32)
    loads[0].wait()
    loads[1].wait()

    def add_middle(document, carry):
        k = path[document, 0, 1]
        value = middle_parts[document].astype(F32) + middle_sum[middle_last[k]]
        middle_sum[document] = value
        middle_grad[k] = value.astype(BF16)
        middle_last[k] = document
        return carry

    lax.fori_loop(0, count, add_middle, 0)
    outs[2].start()
    fine_grad[...] = jnp.zeros_like(fine_grad)
    loads[2].wait()

    def add_fine(document, carry):
        place = path[document, 0, 2] - first_owned

        @pl.when((place >= 0) & (place < owned))
        def _():
            piece = fine_parts[document].astype(F32) + fine_sum[fine_last[place]]
            fine_sum[document] = piece
            fine_grad[place] = piece.astype(BF16)
            fine_last[place] = document

        return carry

    lax.fori_loop(0, count, add_fine, 0)
    outs[3].start()
    loads[3].wait()
    groups, _, _, columns = coarse_parts.shape
    outer, sides, cores = plan(lax.axis_size("mem"), coarse_grad.shape[1])
    side = lax.rem(lax.axis_index("mem"), sides * cores) // cores
    for s in range(2):
        held = lax.rem(s + (1 - sides % 2) * side, 2)
        value = coarse_parts[held].astype(F32)
        for other in range(2, groups, 2):
            value = value + coarse_parts[held + other].astype(F32)
        coarse_grad[:, :, s * columns : (s + 1) * columns] = value.astype(BF16)
    outs[1].start()
    loads[4].wait()
    outs[0].start()
    for out in outs:
        out.wait()


def collect(paths, tokens_grad, middle_parts, fine_parts, coarse_parts, shapes):
    hbm = pl.BlockSpec(memory_space=pl.ANY)
    count, rows, medium = middle_parts.shape
    narrow = fine_parts.shape[2]
    outs = (tokens_grad.shape,) + shapes
    return pl.pallas_call(
        collect_kernel,
        out_shape=tuple(jax.ShapeDtypeStruct(shape, BF16) for shape in outs),
        in_specs=[hbm] * 5,
        out_specs=(hbm,) * 4,
        scratch_shapes=[pltpu.SMEM(paths.shape, jnp.int32)]
        + [pltpu.VMEM(shape, BF16) for shape in outs]
        + [
            pltpu.VMEM(coarse_parts.shape, BF16),
            pltpu.VMEM(middle_parts.shape, BF16),
            pltpu.VMEM(fine_parts.shape, BF16),
            pltpu.VMEM((count + 1, rows, medium), F32),
            pltpu.VMEM((count + 1, rows, narrow), F32),
            pltpu.SMEM((shapes[1][0],), jnp.int32),
            pltpu.SMEM((shapes[2][0],), jnp.int32),
            pltpu.SemaphoreType.DMA((5,)),
            pltpu.SemaphoreType.DMA((4,)),
        ],
        compiler_params=pltpu.CompilerParams(vmem_limit_bytes=60 * 2**20),
        name="collect",
    )(paths, tokens_grad, middle_parts, fine_parts, coarse_parts)


def on_device(tokens, cotangent, path, coarse_weights, middle_weights, fine_weights):
    members = lax.axis_size("mem")
    groups = lax.axis_size("grp")
    paths, tokens_grad, middle_parts, fine_parts, coarse_parts = exchange(
        path, tokens, cotangent, coarse_weights, middle_weights, fine_weights, groups, members
    )
    flat = lambda parts: parts.reshape((groups * members,) + parts.shape[2:])
    return collect(
        paths,
        tokens_grad,
        flat(middle_parts),
        flat(fine_parts),
        coarse_parts,
        (coarse_weights.shape, middle_weights.shape, fine_weights.shape),
    )


def solution(mesh):
    return jax.shard_map(
        on_device,
        mesh=mesh,
        in_specs=(
            P(("grp", "mem"), None),
            P(("grp", "mem"), None),
            P(("grp", "mem"), None),
            P(None, "mem", None),
            P(None, "mem", None),
            P("grp", "mem", None),
        ),
        out_specs=(
            P(("grp", "mem"), None),
            P(None, "mem", None),
            P(None, "mem", None),
            P("grp", "mem", None),
        ),
        check_vma=False,
    )
```
